256 devices in a mesh: groups: 2 (over z), seq: 16 (over y, core), dp: 8 (over x).
Axes of the slice: x: 8, y: 8, z: 2, core: 2. Of those that a mesh axis runs over, the one named last changes fastest.
The devices are a block of a 8x8x16 slice.
Arguments:
- resid: bfloat16 [16, 1024, 2048], P(('groups', 'dp'), 'seq'), parts along dimension 0, may hold values from -6 to 6
- queries_keys: bfloat16 [2, 16, 1024, 2048], P(None, ('groups', 'dp'), 'seq'), parts along dimension 1, may hold values from -20 to 20
- values: bfloat16 [16, 1024, 2048], P(('groups', 'dp'), 'seq'), parts along dimension 0, may hold values from -6 to 6
- doc_ids: int32 [16, 1024], P(('groups', 'dp')), parts along dimension 0, may hold values from 0 to 5, never falling along the last dimension, each value on 1 to 512 neighbouring positions
- out_weight: bfloat16 [2048, 2048], P(None, 'dp'), may hold values from -0.125 to 0.125
- norm_gain: float32 [2048], replicated, may hold values from 0.5 to 1.5
- expert_ids: int32 [16, 1024, 4], P(('groups', 'dp'), 'seq'), parts along dimension 0, may hold values from 0 to 31, all different within a row; in each aligned block of 64 rows (0 to 63, 64 to 127, ..., all dimensions but the last counted through in order) at most 10 rows name the same one
- gate_vals: float32 [16, 1024, 4], P(('groups', 'dp'), 'seq'), parts along dimension 0, may hold values from 0.05 to 0.6
- expert_gate: bfloat16 [128, 2048, 352], P(('seq', 'dp')), may hold values from -0.125 to 0.125
- expert_up: bfloat16 [128, 2048, 352], P(('seq', 'dp')), may hold values from -0.125 to 0.125
- expert_down: bfloat16 [128, 352, 2048], P(('seq', 'dp')), may hold values from -0.15625 to 0.15625
- shared_gate: bfloat16 [2048, 2816], P(None, 'dp'), may hold values from -0.125 to 0.125
- shared_up: bfloat16 [2048, 2816], P(None, 'dp'), may hold values from -0.125 to 0.125
- shared_down: bfloat16 [2816, 2048], P('dp'), may hold values from -0.109375 to 0.109375
- shared_score: bfloat16 [2048], replicated, may hold values from -0.125 to 0.125
Outputs:
- layer_out: bfloat16 [16, 1024, 2048], P(('groups', 'dp'), 'seq'), parts along dimension 0
The draws below stay inside these ranges and needn't reach their ends.
There are 2 independent parts, one for each index of `groups`. The reference program is written for one: setup_inputs(seed, part) draws one part's arguments, and reference() takes and returns one part's arrays. A program takes and returns all parts, laid end to end along the dimension named above; an argument that names none is the same for every part. Nothing has to cross between parts.
Inputs may be any that keep to these rules, and one draw needn't show every extreme that they name: `doc_ids`: document numbers never fall along a sequence; each document holds 1 to 512 positions. `expert_ids`: each token names 4 different experts; among the rows of one device no expert is named more than 10 times.
All inputs are finite; a program needn't handle non-finite values.
Results may differ from the reference program's by a relative error of at most 0.01.
Values may be sent and summed in bfloat16 or wider, within the bound.
A program may use at most 128 MiB of HBM per device.

```python
import math
import jax
import jax.numpy as jnp
import numpy as np
from jax import lax

HEADS = 16
HD = 128
D = 2048
EXPERTS = 32
TOPK = 4
FF_E = 1408
SPLIT = 4
PIECES = 128
PIECE_FF = 352
SH_FF = 2816
TOK_DEV = 64
CAP = 10
LENGTH = 1024
SEQS = 8
N_DP = 8


def draw_queries_keys(key, part):
    baseline = jnp.clip(jax.random.normal(key, (2, SEQS, LENGTH, D), jnp.float32), -6.0, 6.0)
    return baseline.astype(jnp.bfloat16)


def block_levels(rng, extent, pieces, smallest, largest):
    factor_of, own = 1.0, jax.random.fold_in(rng, 6)
    for dim, shards_of in pieces:
        heights = jnp.exp(jax.random.uniform(jax.random.fold_in(own, dim), (shards_of,), jnp.float32, smallest / len(pieces), largest / len(pieces)))
        factor_of = factor_of * jnp.repeat(heights, extent[dim] // shards_of).reshape([-1 if axis == dim else 1 for axis in range(len(extent))])
    return factor_of


def length_profile(number_of, total, reach, skew):
    loads = [(1 << 20) // math.isqrt(grade ** skew) + 1 for grade in range(2, number_of + 1)]
    rest, counts = total - reach - (number_of - 1), [1] * (number_of - 1)
    while rest > 0:
        candidates = [i for i in range(number_of - 1) if counts[i] < reach]
        mass, left = sum([loads[i] for i in candidates]), rest
        for i in candidates:
            addition = min(reach - counts[i], max(1, left * loads[i] // mass), rest)
            counts[i] = counts[i] + addition
            rest = rest - addition
    return np.array([reach] + counts)


def uneven_parts(rng, number_of, total, limit, slope):
    if number_of == 2:
        one = jax.random.randint(rng, (), max(1, total - limit), min(limit, total - 1) + 1)
        return jnp.stack([one, total - one])
    lengths = jnp.asarray(length_profile(number_of, total, limit, slope), jnp.int32)
    couples = (number_of - 1) // 2
    giver, taker = lengths[1:1 + 2 * couples:2], lengths[2:2 + 2 * couples:2]
    margin = jnp.minimum(giver - 1, limit - taker)
    moved = jax.random.randint(jax.random.fold_in(rng, 1), (couples,), 0, 1 << 20) % (margin + 1)
    lengths = lengths.at[1:1 + 2 * couples:2].set(giver - moved).at[2:2 + 2 * couples:2].set(taker + moved)
    return lengths[jax.random.permutation(jax.random.fold_in(rng, 2), number_of)]


def assign_block(own_key, own, number, rows, count, top, bound, skew):
    ranking = jax.random.permutation(own_key, count)
    heavy_load, common = shares(count, rows * top, bound, skew, True), shares(count, rows * top, bound, skew, False)
    places = jnp.arange(count)

    def named(lengths, turn):
        used = int((lengths > 0).sum())
        fixed = max(1, used // 4)
        moved = fixed + (places - fixed + turn * (used - fixed)) % max(1, count - fixed)
        return jnp.zeros((count,), jnp.int32).at[ranking[jnp.where(places < fixed, places, moved)]].set(jnp.asarray(lengths, jnp.int32))

    lengths = jnp.where(number % 4 == 0, named(heavy_load, number // 4), named(common, number - number // 4 - 1))
    mixed = jax.random.permutation(jax.random.fold_in(own, 3), count)
    giver, sink = mixed[0:count // 2 * 2:2], mixed[1:count // 2 * 2:2]
    room = jnp.minimum(lengths[giver] - 1, bound - lengths[sink]) // 2
    room = jnp.where((giver == ranking[0]) | (sink == ranking[0]) | (lengths[sink] == 0), 0, jnp.maximum(room, 0))
    moved = jax.random.randint(jax.random.fold_in(own, 4), (count // 2,), 0, 1 << 20) % (room + 1)
    lengths = lengths.at[giver].add(-moved).at[sink].add(moved)
    labels = jnp.searchsorted(jnp.cumsum(lengths), jnp.arange(rows * top), side="right").astype(jnp.int32)
    grid = labels.reshape(top, rows).T
    grid = grid[jax.random.permutation(jax.random.fold_in(own, 1), rows)]
    turn = jax.random.randint(jax.random.fold_in(own, 2), (rows, 1), 0, top)
    return jnp.take_along_axis(grid, (jnp.arange(top)[None, :] + turn) % top, axis=1)


def shares(number_of, total, bound, lean, full):
    weights = [(1 << 20) // math.isqrt(grade ** lean) + 1 for grade in range(1, number_of + 1)]
    largest = bound if full else min(bound, max(-(-total // number_of), total * weights[0] // sum(weights)))
    least = 1 if total - largest >= number_of - 1 else 0
    counts, rest = [largest] + [least] * (number_of - 1), total - largest - least * (number_of - 1)
    while rest > 0:
        free = [i for i in range(1, number_of) if counts[i] < largest] or [i for i in range(1, number_of) if counts[i] < bound]
        whole, budget = sum([weights[i] for i in free]), rest
        for i in free:
            more = min(bound - counts[i], max(1, budget * weights[i] // whole), rest)
            counts[i] = counts[i] + more
            rest = rest - more
    return np.array(counts)


def bell_draw(own_key, shape, scale, most, pieces=(), kind=jnp.bfloat16):
    gain = block_levels(own_key, shape, pieces, -0.22, 0.18) if pieces else 1.0
    values = jax.random.normal(own_key, shape, jnp.float32) * scale * gain
    return jnp.minimum(jnp.maximum(values, -most), most).astype(kind)


def setup_inputs(seed: int = 0, part: int = 0) -> dict:
    key_of = jax.random.split(jax.random.key(seed), 16)
    part_splits = jax.random.split(jax.random.fold_in(key_of[15], part), 16)
    resid = bell_draw(part_splits[0], (SEQS, LENGTH, D), 1.0, 6.0, ((0, 8), (1, 16)))
    queries_keys = draw_queries_keys(jax.random.fold_in(jax.random.fold_in(key_of[15], part), 71), part)
    values = bell_draw(part_splits[2], (SEQS, LENGTH, D), 1.0, 6.0, ((0, 8), (1, 16)))
    doc_ids = jax.vmap(lambda own: jnp.searchsorted(jnp.cumsum(uneven_parts(own, 6, LENGTH, LENGTH // 2, 1)), jnp.arange(LENGTH), side="right"))(jax.random.split(part_splits[3], SEQS)).reshape((SEQS, LENGTH)).astype(jnp.int32)
    out_weight = bell_draw(key_of[4], (D, D), D ** -0.5, 0.125, ((1, 8),))
    norm_gain = jnp.clip(1.0 + 0.1 * jax.random.normal(key_of[5], (D,), jnp.float32), 0.5, 1.5)
    expert_ids_keys = jax.random.split(jax.random.fold_in(part_splits[6], 1), SEQS * LENGTH // TOK_DEV)
    expert_ids_turns = jax.random.permutation(jax.random.fold_in(part_splits[6], 3), SEQS * LENGTH // TOK_DEV)
    expert_ids = jax.vmap(lambda own, number: assign_block(jax.random.fold_in(part_splits[6], 2), own, number, TOK_DEV, EXPERTS, TOPK, CAP, 2))(expert_ids_keys, expert_ids_turns).reshape((SEQS, LENGTH, TOPK))
    gate_vals = jnp.clip(jnp.exp(math.log(0.6) - 2.4849067 * jax.random.uniform(part_splits[7], (SEQS, LENGTH, TOPK), jnp.float32) ** block_levels(part_splits[7], (SEQS, LENGTH, TOPK), ((0, 8), (1, 16)), -0.2, 0.2)), 0.05, 0.6)
    expert_gate = bell_draw(key_of[8], (PIECES, D, PIECE_FF), D ** -0.5, 0.125, ((0, 128),))
    expert_up = bell_draw(key_of[9], (PIECES, D, PIECE_FF), D ** -0.5, 0.125, ((0, 128),))
    expert_down = bell_draw(key_of[10], (PIECES, PIECE_FF, D), FF_E ** -0.5, 0.15625, ((0, 128),))
    shared_gate = bell_draw(key_of[11], (D, SH_FF), D ** -0.5, 0.125, ((1, 8),))
    shared_up = bell_draw(key_of[12], (D, SH_FF), D ** -0.5, 0.125, ((1, 8),))
    shared_down = bell_draw(key_of[13], (SH_FF, D), SH_FF ** -0.5, 0.109375, ((0, 8),))
    shared_score = bell_draw(key_of[14], (D,), D ** -0.5, 0.125)
    return dict(resid=resid, queries_keys=queries_keys, values=values, doc_ids=doc_ids, out_weight=out_weight, norm_gain=norm_gain, expert_ids=expert_ids, gate_vals=gate_vals, expert_gate=expert_gate, expert_up=expert_up, expert_down=expert_down, shared_gate=shared_gate, shared_up=shared_up, shared_down=shared_down, shared_score=shared_score)


norm_eps = 1e-06

def slot_numbers(routes):
    flat_routes = routes.reshape(routes.shape[:-2] + (-1,))
    matches = (flat_routes[..., None] == jnp.arange(EXPERTS, dtype=jnp.int32)).astype(jnp.int32)
    ranked = lax.optimization_barrier(jnp.sum(matches * (jnp.cumsum(matches, axis=-2) - 1), axis=-1))
    return (flat_routes * CAP + ranked).reshape(routes.shape).astype(jnp.int32)

def reference(resid, queries_keys, values, doc_ids, out_weight, norm_gain, expert_ids, gate_vals, expert_gate, expert_up, expert_down, shared_gate, shared_up, shared_down, shared_score):
    score_scale = 1.0 / math.sqrt(HD)
    positions = jnp.arange(LENGTH, dtype=jnp.int32)
    causal = positions[:, None] >= positions[None, :]

    def attend_sequence(inputs):
        pair_rows, value_rows, documents = inputs
        queries = pair_rows[0].astype(jnp.float32).reshape(LENGTH, HEADS, HD)
        key_rows = pair_rows[1].astype(jnp.float32).reshape(LENGTH, HEADS, HD)
        value_heads = value_rows.astype(jnp.float32).reshape(LENGTH, HEADS, HD)
        scores = jnp.einsum('qhd,khd->hqk', queries, key_rows) * score_scale
        allowed = causal & (documents[:, None] == documents[None, :])
        scores = jnp.where(allowed[None], scores, -1e+30)
        row_max = lax.optimization_barrier(jnp.max(scores, axis=-1, keepdims=True))
        lifted = jnp.exp(scores - row_max)
        weights = (lifted / lax.optimization_barrier(jnp.sum(lifted, axis=-1, keepdims=True))).astype(jnp.bfloat16)
        attended = jnp.einsum('hqk,khd->qhd', weights.astype(jnp.float32), value_heads).astype(jnp.bfloat16)
        return jnp.dot(attended.reshape(LENGTH, D), out_weight, preferred_element_type=jnp.float32).astype(jnp.bfloat16)
    projected = lax.map(attend_sequence, (jnp.moveaxis(queries_keys, 1, 0), values, doc_ids))
    residual = (resid.astype(jnp.float32) + projected.astype(jnp.float32)).astype(jnp.bfloat16)
    stream = residual.astype(jnp.float32)
    normed = (stream * lax.rsqrt(lax.optimization_barrier(jnp.mean(stream * stream, axis=-1, keepdims=True)) + norm_eps) * norm_gain).astype(jnp.bfloat16)
    shared_width = SH_FF // N_DP
    down_blocks = shared_down.astype(jnp.float32).reshape(N_DP, shared_width, D)

    def shared_sequence(row_block):
        gate_act = jnp.dot(row_block, shared_gate, preferred_element_type=jnp.float32)
        up_act = jnp.dot(row_block, shared_up, preferred_element_type=jnp.float32)
        hidden = (jax.nn.silu(gate_act) * up_act).astype(jnp.bfloat16)
        partial_sums = jnp.einsum('lnf,nfd->nld', hidden.astype(jnp.float32).reshape(-1, N_DP, shared_width), down_blocks)
        partial_sums = lax.optimization_barrier(partial_sums.astype(jnp.bfloat16)).astype(jnp.float32)
        return lax.optimization_barrier(jnp.sum(partial_sums, axis=0))
    shared_out = lax.map(shared_sequence, normed).reshape(-1, D)
    flat_rows = normed.reshape(-1, D)
    token_count = flat_rows.shape[0]
    share_weight = jax.nn.sigmoid(jnp.dot(flat_rows, shared_score, preferred_element_type=jnp.float32))
    blocks = token_count // TOK_DEV
    routes = expert_ids.reshape(blocks, TOK_DEV, TOPK).astype(jnp.int32)
    slot_ids = slot_numbers(routes)
    ranked = slot_ids - routes * CAP
    block_ids = jnp.arange(blocks, dtype=jnp.int32)[:, None, None]
    token_ids = block_ids * TOK_DEV + jnp.arange(TOK_DEV, dtype=jnp.int32)[None, :, None] + jnp.zeros_like(routes)
    row_slots = (block_ids * CAP + ranked).astype(jnp.int32)
    row_table = jnp.full((EXPERTS, blocks * CAP), token_count, jnp.int32).at[routes, row_slots].set(token_ids.astype(jnp.int32))
    gate_table = jnp.zeros((EXPERTS, blocks * CAP), jnp.float32).at[routes, row_slots].set(gate_vals.reshape(blocks, TOK_DEV, TOPK).astype(jnp.float32))
    padded = jnp.concatenate([flat_rows, jnp.zeros((1, D), jnp.bfloat16)], axis=0)
    gate_pieces = expert_gate.reshape(EXPERTS, SPLIT, D, PIECE_FF)
    up_pieces = expert_up.reshape(EXPERTS, SPLIT, D, PIECE_FF)
    down_pieces = expert_down.reshape(EXPERTS, SPLIT, PIECE_FF, D)

    def one_expert(running, inputs):
        index_rows, weight_rows, gate_matrix, up_matrix, down_matrix = inputs
        picked = padded[index_rows].astype(jnp.float32)
        gate_act = jnp.einsum('rd,sdf->srf', picked, gate_matrix.astype(jnp.float32))
        up_act = jnp.einsum('rd,sdf->srf', picked, up_matrix.astype(jnp.float32))
        hidden = (jax.nn.silu(gate_act) * up_act).astype(jnp.bfloat16)
        partial_sums = jnp.einsum('srf,sfd->srd', hidden.astype(jnp.float32), down_matrix.astype(jnp.float32))
        partial_sums = lax.optimization_barrier(partial_sums.astype(jnp.bfloat16)).astype(jnp.float32)
        output = lax.optimization_barrier(jnp.sum(partial_sums, axis=0))
        running = running.at[index_rows].add(weight_rows[:, None] * output)
        return (running, None)
    routed, unused = lax.scan(one_expert, jnp.zeros((token_count + 1, D), jnp.float32), (row_table, gate_table, gate_pieces, up_pieces, down_pieces))
    routed = routed[:token_count]
    layer_out = residual.reshape(-1, D).astype(jnp.float32) + routed + share_weight[:, None] * shared_out
    return layer_out.astype(jnp.bfloat16).reshape(SEQS, LENGTH, D)
```

```python
import functools
import math

import jax
import jax.numpy as jnp
from jax import lax
from jax.experimental import pallas as pl
from jax.experimental.pallas import tpu as pltpu
from jax.sharding import PartitionSpec as P

HD = 128
EXPERTS = 32
TOPK = 4
SPLIT = 4
CAP = 10
GROUP = 2

norm_eps = 1e-06
MESH = pl.DeviceIdType.MESH
F32 = jnp.float32
BF16 = jnp.bfloat16


def ring_delta(j):
    return ((j + 1) // 2) * (2 * (j % 2) - 1)


def expert_kernel(
    ns,
    rows,
    send_ref,
    gate_hbm,
    up_hbm,
    down_hbm,
    ret_ref,
    wg,
    wu,
    wd,
    own_in,
    pair_in,
    pair_out,
    pair_part,
    own_part,
    back,
    w_sem,
    local_sem,
    sy_sem,
    ry_sem,
    sx_sem,
    rx_sem,
    sp_sem,
    rp_sem,
    sr_sem,
    rr_sem,
):
    s = lax.axis_index("seq")
    d = lax.axis_index("dp")
    par = lax.rem(d, 2)
    partner = d + 1 - 2 * par
    half = send_ref.shape[1]
    group_rows = GROUP * rows
    groups = ns // GROUP

    w_copies = [
        pltpu.make_async_copy(src.at[0], dst, w_sem.at[i])
        for i, (src, dst) in enumerate(((gate_hbm, wg), (up_hbm, wu), (down_hbm, wd)))
    ]
    for c in w_copies:
        c.start()

    barrier = pltpu.get_barrier_semaphore()

    @pl.loop(1, ns)
    def _(k):
        pl.semaphore_signal(
            barrier, inc=1, device_id={"seq": lax.rem(s + k, ns)}, device_id_type=MESH
        )

    pl.semaphore_signal(barrier, inc=1, device_id={"dp": partner}, device_id_type=MESH)
    pl.semaphore_wait(barrier, ns)

    def block(ref, j):
        return ref.at[pl.ds(pl.multiple_of(j * rows, 16), rows)]

    def span(g):
        return pl.ds(pl.multiple_of(g * group_rows, 16), group_rows)

    def out_copy(j):
        to = lax.rem(s - ring_delta(j) + ns, ns)
        return pltpu.make_async_remote_copy(
            block(send_ref, to), block(own_in, j), sy_sem.at[j], ry_sem.at[j],
            device_id={"seq": to}, device_id_type=MESH,
        )

    def swap_copy(g):
        return pltpu.make_async_remote_copy(
            own_in.at[span(g)], pair_in.at[span(g)], sx_sem.at[g], rx_sem.at[g],
            device_id={"dp": partner}, device_id_type=MESH,
        )

    def part_copy(g):
        return pltpu.make_async_remote_copy(
            pair_out.at[span(g)], pair_part.at[span(g)], sp_sem.at[g], rp_sem.at[g],
            device_id={"dp": partner}, device_id_type=MESH,
        )

    def back_copy(j):
        to = lax.rem(s + ring_delta(j) + ns, ns)
        return pltpu.make_async_remote_copy(
            block(back, j), block(ret_ref, s), sr_sem.at[j], rr_sem.at[j],
            device_id={"seq": to}, device_id_type=MESH,
        )

    @pl.loop(1, ns)
    def _(j):
        out_copy(j).start()

    mine = pltpu.make_async_copy(block(send_ref, s), block(own_in, 0), local_sem.at[0])
    mine.start()
    mine.wait()
    for c in w_copies:
        c.wait()

    own_cols = pl.ds(pl.multiple_of(par * half, half), half)
    pair_cols = pl.ds(pl.multiple_of((1 - par) * half, half), half)

    @pl.loop(0, groups + 2)
    def _(step):
        @pl.when(step < groups)
        def _():
            for i in range(GROUP):
                j = step * GROUP + i

                @pl.when(j > 0)
                def _():
                    out_copy(j).wait_recv()

            swap_copy(step).start()

        @pl.when(step >= 2)
        def _():
            g = step - 2
            part_copy(g).wait_recv()
            back[span(g), :] = (own_part[span(g), :] + pair_part[span(g), :].astype(F32)).astype(
                BF16
            )

        @pl.when((step >= 1) & (step <= groups))
        def _():
            g = step - 1
            swap_copy(g).wait_recv()
            a = own_in[span(g), :]
            b = pair_in[span(g), :]

            def both(w):
                return jnp.dot(a, w[own_cols, :], preferred_element_type=F32) + jnp.dot(
                    b, w[pair_cols, :], preferred_element_type=F32
                )

            gate_act = both(wg)
            hidden = (gate_act / (1.0 + jnp.exp(-gate_act)) * both(wu)).astype(BF16)
            pair_out[span(g), :] = jnp.dot(
                hidden, wd[:, pair_cols], preferred_element_type=F32
            ).astype(BF16)
            own_part[span(g), :] = jnp.dot(hidden, wd[:, own_cols], preferred_element_type=F32)
            part_copy(g).start()

        @pl.when(step >= 2)
        def _():
            for i in range(GROUP):
                j = (step - 2) * GROUP + i

                @pl.when(j > 0)
                def _():
                    back_copy(j).start()

    home = pltpu.make_async_copy(block(back, 0), block(ret_ref, s), local_sem.at[0])
    home.start()

    @pl.loop(1, ns)
    def _(j):
        out_copy(j).wait_send()
        back_copy(j).wait_send()
        frm = lax.rem(s - ring_delta(j) + ns, ns)
        pltpu.make_async_remote_copy(
            block(back, j), block(ret_ref, frm), sr_sem.at[j], rr_sem.at[j],
            device_id={"seq": frm}, device_id_type=MESH,
        ).wait_recv()

    @pl.loop(0, groups)
    def _(g):
        swap_copy(g).wait_send()
        part_copy(g).wait_send()

    home.wait()


def run_experts(send, expert_gate, expert_up, expert_down, ns):
    total, half = send.shape
    rows = total // ns
    groups = ns // GROUP
    dma = pltpu.SemaphoreType.DMA
    hidden = expert_gate.shape[-1]
    vmem = pl.BlockSpec(memory_space=pltpu.VMEM)
    anyspace = pl.BlockSpec(memory_space=pl.ANY)
    return pl.pallas_call(
        functools.partial(expert_kernel, ns, rows),
        out_shape=jax.ShapeDtypeStruct((total, half), BF16),
        in_specs=[vmem, anyspace, anyspace, anyspace],
        out_specs=vmem,
        scratch_shapes=[
            pltpu.VMEM((2 * half, hidden), BF16),
            pltpu.VMEM((2 * half, hidden), BF16),
            pltpu.VMEM((hidden, 2 * half), BF16),
            pltpu.VMEM((total, half), BF16),
            pltpu.VMEM((total, half), BF16),
            pltpu.VMEM((total, half), BF16),
            pltpu.VMEM((total, half), BF16),
            pltpu.VMEM((total, half), F32),
            pltpu.VMEM((total, half), BF16),
            dma((3,)),
            dma((1,)),
            dma((ns,)),
            dma((ns,)),
            dma((groups,)),
            dma((groups,)),
            dma((groups,)),
            dma((groups,)),
            dma((ns,)),
            dma((ns,)),
        ],
        compiler_params=pltpu.CompilerParams(
            collective_id=1, has_side_effects=True, vmem_limit_bytes=60 * 1024 * 1024
        ),
        cost_estimate=pl.CostEstimate(
            flops=12 * total * half * hidden, bytes_accessed=8 * total * half, transcendentals=0
        ),
        name="experts",
    )(send, expert_gate, expert_up, expert_down)


def ring_gather(nd, axis, src_ref, all_ref, send_sem, recv_sem, on_block):
    d = lax.axis_index(axis)
    rows = src_ref.shape[0]
    part = rows // 2
    last = nd // 2

    def place(index, sub):
        return all_ref.at[pl.ds(pl.multiple_of(index * rows + sub * part, 16), part)]

    def hop(way, t, sub):
        sign = 1 - 2 * way
        index = lax.rem(d - sign * (t - 1) + nd, nd)
        src = src_ref.at[pl.ds(sub * part, part)] if t == 1 else place(index, sub)
        return pltpu.make_async_remote_copy(
            src, place(index, sub), send_sem.at[way, t - 1, sub], recv_sem.at[way, t - 1, sub],
            device_id={axis: lax.rem(d + sign + nd, nd)}, device_id_type=MESH,
        )

    def used(way, t, sub):
        return t < last or (t == last and sub == way)

    for sub in range(2):
        for way in range(2):
            if used(way, 1, sub):
                hop(way, 1, sub).start()
    on_block(d, None)
    for t in range(1, last + 1):
        for sub in range(2):
            for way in range(2):
                if used(way, t, sub):
                    hop(way, t, sub).wait_recv()
                    if used(way, t + 1, sub):
                        hop(way, t + 1, sub).start()
        if t < last:
            on_block(lax.rem(d - t + nd, nd), t)
            on_block(lax.rem(d + t, nd), t)
        else:
            on_block(lax.rem(d + t, nd), t)
    for t in range(1, last + 1):
        for sub in range(2):
            for way in range(2):
                if used(way, t, sub):
                    hop(way, t, sub).wait_send()


def greet(axis, size):
    me = lax.axis_index(axis)
    barrier = pltpu.get_barrier_semaphore()

    @pl.loop(1, size)
    def _(k):
        pl.semaphore_signal(
            barrier, inc=1, device_id={axis: lax.rem(me + k, size)}, device_id_type=MESH
        )

    pl.semaphore_wait(barrier, size - 1)


def attend_kernel(
    ns, qk_ref, v_ref, drow_ref, dcol_ref, out_ref, qh, kh, vh, att, si_sem, ri_sem, so_sem, ro_sem,
    local_sem,
):
    s = lax.axis_index("seq")
    rows = v_ref.shape[0]
    length = rows * ns
    greet("seq", ns)

    def own_rows(ref, t):
        return ref.at[pl.ds(pl.multiple_of(t * rows, 16), rows)]

    def cols(t):
        return pl.ds(pl.multiple_of(t * HD, HD), HD)

    def pieces(t):
        return (
            (qk_ref.at[0, :, cols(t)], qh),
            (qk_ref.at[1, :, cols(t)], kh),
            (v_ref.at[:, cols(t)], vh),
        )

    def in_copies(j):
        to = lax.rem(s - ring_delta(j) + ns, ns)
        return [
            pltpu.make_async_remote_copy(
                src, own_rows(dst, s), si_sem.at[c, j], ri_sem.at[c, j],
                device_id={"seq": to}, device_id_type=MESH,
            )
            for c, (src, dst) in enumerate(pieces(to))
        ]

    def in_waits(j):
        frm = lax.rem(s + ring_delta(j) + ns, ns)
        return [
            pltpu.make_async_remote_copy(
                src, own_rows(dst, frm), si_sem.at[c, j], ri_sem.at[c, j],
                device_id={"seq": frm}, device_id_type=MESH,
            )
            for c, (src, dst) in enumerate(pieces(frm))
        ]

    @pl.loop(1, ns)
    def _(j):
        for c in in_copies(j):
            c.start()

    local = [
        pltpu.make_async_copy(src, own_rows(dst, s), local_sem.at[c])
        for c, (src, dst) in enumerate(pieces(s))
    ]
    for c in local:
        c.start()
    for c in local:
        c.wait()

    @pl.loop(1, ns)
    def _(j):
        for c in in_waits(j):
            c.wait_recv()

    scale = 1.0 / math.sqrt(HD)
    step = 4 * rows
    for i in range(length // step):
        upto = (i + 1) * step
        span = pl.ds(i * step, step)
        scores = lax.dot_general(
            qh[span, :], kh[0:upto, :], (((1,), (1,)), ((), ())), preferred_element_type=F32
        ) * scale
        at = lax.broadcasted_iota(jnp.int32, (step, upto), 0) + i * step
        key_at = lax.broadcasted_iota(jnp.int32, (step, upto), 1)
        mine = jnp.concatenate([dcol_ref[span, :]] * (upto // HD), axis=1)
        allowed = (key_at <= at) & (mine == drow_ref[:, 0:upto])
        scores = jnp.where(allowed, scores, -1e30)
        lifted = jnp.exp(scores - jnp.max(scores, axis=-1, keepdims=True))
        weights = (lifted / jnp.sum(lifted, axis=-1, keepdims=True)).astype(BF16)
        att[span, :] = jnp.dot(weights, vh[0:upto, :], preferred_element_type=F32).astype(BF16)
        for t in range(4 * i, 4 * i + 4):

            @pl.when(s != t)
            def _():
                pltpu.make_async_remote_copy(
                    att.at[pl.ds(t * rows, rows)], out_ref.at[:, cols(s)], so_sem.at[t],
                    ro_sem.at[s], device_id={"seq": t}, device_id_type=MESH,
                ).start()

    home = pltpu.make_async_copy(own_rows(att, s), out_ref.at[:, cols(s)], local_sem.at[0])
    home.start()

    @pl.loop(1, ns)
    def _(j):
        for c in in_copies(j):
            c.wait_send()
        other = lax.rem(s + j, ns)
        done = pltpu.make_async_remote_copy(
            own_rows(att, other), out_ref.at[:, cols(other)], so_sem.at[other], ro_sem.at[other],
            device_id={"seq": other}, device_id_type=MESH,
        )
        done.wait_send()
        done.wait_recv()

    home.wait()


def run_attention(qk, v, documents, ns):
    rows, width = v.shape
    length = rows * ns
    dma = pltpu.SemaphoreType.DMA
    vmem = pl.BlockSpec(memory_space=pltpu.VMEM)
    return pl.pallas_call(
        functools.partial(attend_kernel, ns),
        out_shape=jax.ShapeDtypeStruct((rows, width), BF16),
        in_specs=[vmem] * 4,
        out_specs=vmem,
        scratch_shapes=[pltpu.VMEM((length, HD), BF16)] * 4
        + [dma((3, ns)), dma((3, ns)), dma((ns,)), dma((ns,)), dma((3,))],
        compiler_params=pltpu.CompilerParams(
            collective_id=2, has_side_effects=True, vmem_limit_bytes=48 * 1024 * 1024
        ),
        cost_estimate=pl.CostEstimate(
            flops=4 * length * length * HD, bytes_accessed=8 * rows * width, transcendentals=0
        ),
        name="attend",
    )(qk, v, documents[None, :], jnp.broadcast_to(documents[:, None], (length, HD)))


def middle_kernel(
    nd, att_ref, w_ref, resid_ref, gain_ref, residual_ref, all_ref, att_all, column, projected,
    normed, s1_sem, r1_sem, s2_sem, r2_sem, sp_sem, rp_sem,
):
    d = lax.axis_index("dp")
    rows = att_ref.shape[0]
    block = w_ref.shape[1]
    greet("dp", nd)

    def at(index):
        return pl.ds(pl.multiple_of(index * rows, 16), rows)

    def column_copy(to, frm):
        return pltpu.make_async_remote_copy(
            column.at[at(to)],
            projected.at[:, pl.ds(pl.multiple_of(frm * block, block), block)],
            sp_sem.at[to], rp_sem.at[frm], device_id={"dp": to}, device_id_type=MESH,
        )

    def project(index, step):
        src = att_ref[...] if step is None else att_all[at(index), :]
        out = jnp.dot(src, w_ref[...], preferred_element_type=F32).astype(BF16)
        if step is None:
            projected[:, pl.ds(pl.multiple_of(d * block, block), block)] = out
        else:
            column[at(index), :] = out
            column_copy(index, d).start()

    ring_gather(nd, "dp", att_ref, att_all, s1_sem, r1_sem, project)

    @pl.loop(1, nd)
    def _(k):
        other = lax.rem(d + k, nd)
        column_copy(other, other).wait_recv()
        column_copy(other, other).wait_send()

    residual = (resid_ref[...].astype(F32) + projected[...].astype(F32)).astype(BF16)
    residual_ref[...] = residual
    stream = residual.astype(F32)
    out = (
        stream
        * lax.rsqrt(jnp.mean(stream * stream, axis=-1, keepdims=True) + norm_eps)
        * gain_ref[...]
    ).astype(BF16)
    normed[...] = out
    all_ref[at(d), :] = out
    ring_gather(nd, "dp", normed, all_ref, s2_sem, r2_sem, lambda index, step: None)


def run_middle(own_attended, out_weight, resid, norm_gain, nd):
    rows, width = own_attended.shape
    dma = pltpu.SemaphoreType.DMA
    vmem = pl.BlockSpec(memory_space=pltpu.VMEM)
    ring = dma((2, nd // 2, 2))
    return pl.pallas_call(
        functools.partial(middle_kernel, nd),
        out_shape=(
            jax.ShapeDtypeStruct((rows, width), BF16),
            jax.ShapeDtypeStruct((nd * rows, width), BF16),
        ),
        in_specs=[vmem] * 4,
        out_specs=(vmem, vmem),
        scratch_shapes=[
            pltpu.VMEM((nd * rows, width), BF16),
            pltpu.VMEM((nd * rows, out_weight.shape[1]), BF16),
            pltpu.VMEM((rows, width), BF16),
            pltpu.VMEM((rows, width), BF16),
            ring, ring, ring, ring, dma((nd,)), dma((nd,)),
        ],
        compiler_params=pltpu.CompilerParams(
            collective_id=3, has_side_effects=True, vmem_limit_bytes=48 * 1024 * 1024
        ),
        cost_estimate=pl.CostEstimate(
            flops=2 * nd * rows * width * out_weight.shape[1],
            bytes_accessed=4 * nd * rows * width, transcendentals=0,
        ),
        name="middle",
    )(own_attended, out_weight, resid, norm_gain[None, :])


def sum_kernel(nd, part_ref, out_ref, landed, passed, send_sem, recv_sem):
    d = lax.axis_index("dp")
    rows = out_ref.shape[0]
    part = rows // 2
    last = nd // 2
    greet("dp", nd)

    def own(index, sub):
        return pl.ds(pl.multiple_of(index * rows + sub * part, 16), part)

    def used(way, t, sub):
        return t < last or (t == last and sub == way)

    def hop(way, t, sub, src):
        sign = 1 - 2 * way
        return pltpu.make_async_remote_copy(
            src, landed.at[way, t - 1, sub], send_sem.at[way, t - 1, sub],
            recv_sem.at[way, t - 1, sub],
            device_id={"dp": lax.rem(d + sign + nd, nd)}, device_id_type=MESH,
        )

    def target(way, t):
        return lax.rem(d + (1 - 2 * way) * t + nd, nd)

    def first(way, sub):
        return last if sub == way else last - 1

    for way in range(2):
        for sub in range(2):
            t = first(way, sub)
            hop(way, t, sub, part_ref.at[own(target(way, t), sub)]).start()
    for t in range(last - 1, 0, -1):
        for sub in range(2):
            for way in range(2):
                if t == first(way, sub):
                    continue
                got = hop(way, t + 1, sub, passed.at[way, t - 1, sub])
                got.wait_recv()
                passed[way, t - 1, sub] = (
                    landed[way, t, sub].astype(F32)
                    + part_ref[own(target(way, t), sub), :].astype(F32)
                ).astype(BF16)
                hop(way, t, sub, passed.at[way, t - 1, sub]).start()
    for sub in range(2):
        for way in range(2):
            hop(way, 1, sub, passed.at[way, 0, sub]).wait_recv()
        out_ref[pl.ds(sub * part, part), :] = (
            part_ref[own(d, sub), :].astype(F32)
            + landed[0, 0, sub].astype(F32)
            + landed[1, 0, sub].astype(F32)
        )
    for way in range(2):
        for sub in range(2):
            for t in range(1, last + 1):
                if used(way, t, sub):
                    hop(way, t, sub, passed.at[way, t - 1, sub]).wait_send()


def run_sum(part, nd):
    total, width = part.shape
    rows = total // nd
    dma = pltpu.SemaphoreType.DMA
    vmem = pl.BlockSpec(memory_space=pltpu.VMEM)
    ring = dma((2, nd // 2, 2))
    return pl.pallas_call(
        functools.partial(sum_kernel, nd),
        out_shape=jax.ShapeDtypeStruct((rows, width), F32),
        in_specs=[vmem],
        out_specs=vmem,
        scratch_shapes=[
            pltpu.VMEM((2, nd // 2, 2, rows // 2, width), BF16),
            pltpu.VMEM((2, nd // 2, 2, rows // 2, width), BF16),
            ring, ring,
        ],
        compiler_params=pltpu.CompilerParams(
            collective_id=4, has_side_effects=True, vmem_limit_bytes=32 * 1024 * 1024
        ),
        cost_estimate=pl.CostEstimate(
            flops=2 * total * width, bytes_accessed=4 * total * width, transcendentals=0
        ),
        name="ring_sum",
    )(part)


def body(
    resid,
    queries_keys,
    values,
    doc_ids,
    out_weight,
    norm_gain,
    expert_ids,
    gate_vals,
    expert_gate,
    expert_up,
    expert_down,
    shared_gate,
    shared_up,
    shared_down,
    shared_score,
):
    ns = lax.axis_size("seq")
    nd = lax.axis_size("dp")
    tokens = resid.shape[1]
    width = resid.shape[2]
    d = lax.axis_index("dp")
    documents = doc_ids[0]

    all_ids = lax.all_gather(expert_ids[0], "dp", axis=0, tiled=True)
    all_gates = lax.all_gather(gate_vals[0], "dp", axis=0, tiled=True)
    per_seq = nd // SPLIT
    routes = all_ids.reshape(nd, tokens * TOPK)
    matches = (routes[..., None] == jnp.arange(EXPERTS, dtype=jnp.int32)).astype(jnp.int32)
    ranked = jnp.sum(matches * (jnp.cumsum(matches, axis=1) - 1), axis=-1)
    blocks = jnp.arange(nd, dtype=jnp.int32)[:, None]
    slots = jnp.where(
        routes % per_seq == d // SPLIT,
        (routes // per_seq) * (nd * CAP) + blocks * CAP + ranked,
        -1,
    ).reshape(nd * tokens, TOPK)
    slot_range = jnp.arange(ns * nd * CAP, dtype=jnp.int32)

    own_attended = run_attention(
        queries_keys.reshape(2, tokens, width), values[0], documents, ns
    )
    residual, normed_all = run_middle(own_attended, out_weight, resid[0], norm_gain, nd)

    half = width // 2
    par = d % 2
    picked = jnp.sum(
        (slots[None, :, :] == slot_range[:, None, None]).astype(jnp.int32), axis=-1
    ).astype(BF16)
    side = lax.dynamic_slice_in_dim(normed_all, par * half, half, axis=1)
    send = jnp.dot(picked, side, preferred_element_type=F32).astype(BF16)
    returned = run_experts(send, expert_gate, expert_up, expert_down, ns)

    gate_act = jnp.dot(normed_all, shared_gate, preferred_element_type=F32)
    up_act = jnp.dot(normed_all, shared_up, preferred_element_type=F32)
    hidden = (jax.nn.silu(gate_act) * up_act).astype(BF16)
    shared_part = jnp.dot(hidden, shared_down, preferred_element_type=F32)
    share_weight = jax.nn.sigmoid(jnp.dot(normed_all, shared_score, preferred_element_type=F32))

    gate_rows = jnp.sum(
        jnp.where(slots[:, :, None] == slot_range[None, None, :], all_gates[:, :, None], 0.0),
        axis=1,
    ).astype(BF16)
    routed = jnp.dot(gate_rows, returned, preferred_element_type=F32)
    routed_wide = jnp.concatenate(
        [jnp.where(par == 0, routed, 0.0), jnp.where(par == 1, routed, 0.0)], axis=1
    )
    part = (share_weight[:, None] * shared_part + routed_wide).astype(BF16)
    total = run_sum(part, nd)
    return (residual.astype(F32) + total).astype(BF16)[None]


def solution(mesh):
    placed = (
        P(("groups", "dp"), "seq", None),
        P(None, ("groups", "dp"), "seq", None),
        P(("groups", "dp"), "seq", None),
        P(("groups", "dp"), None),
        P(None, "dp"),
        P(),
        P(("groups", "dp"), "seq", None),
        P(("groups", "dp"), "seq", None),
        P(("seq", "dp"), None, None),
        P(("seq", "dp"), None, None),
        P(("seq", "dp"), None, None),
        P(None, "dp"),
        P(None, "dp"),
        P("dp", None),
        P(),
    )
    return jax.shard_map(
        body,
        mesh=mesh,
        in_specs=placed,
        out_specs=P(("groups", "dp"), "seq", None),
        check_vma=False,
    )
```

```python
import functools
import math

import jax
import jax.numpy as jnp
from jax import lax
from jax.experimental import pallas as pl
from jax.experimental.pallas import tpu as pltpu
from jax.sharding import PartitionSpec as P

HD = 128
TOPK = 4
SPLIT = 4
CAP = 10
GROUP = 2

norm_eps = 1e-06
MESH = pl.DeviceIdType.MESH
F32 = jnp.float32
BF16 = jnp.bfloat16


def ring_delta(j):
    return ((j + 1) // 2) * (2 * (j % 2) - 1)


def ring_gather(nd, axis, src_ref, all_ref, send_sem, recv_sem, on_block):
    d = lax.axis_index(axis)
    rows = src_ref.shape[0]
    part = rows // 2
    last = nd // 2

    def place(index, sub):
        return all_ref.at[pl.ds(pl.multiple_of(index * rows + sub * part, 16), part)]

    def hop(way, t, sub):
        sign = 1 - 2 * way
        index = lax.rem(d - sign * (t - 1) + nd, nd)
        src = src_ref.at[pl.ds(sub * part, part)] if t == 1 else place(index, sub)
        return pltpu.make_async_remote_copy(
            src, place(index, sub), send_sem.at[way, t - 1, sub], recv_sem.at[way, t - 1, sub],
            device_id={axis: lax.rem(d + sign + nd, nd)}, device_id_type=MESH,
        )

    def used(way, t, sub):
        return t < last or (t == last and sub == way)

    for sub in range(2):
        for way in range(2):
            if used(way, 1, sub):
                hop(way, 1, sub).start()
    on_block(d, None)
    for t in range(1, last + 1):
        for sub in range(2):
            for way in range(2):
                if used(way, t, sub):
                    hop(way, t, sub).wait_recv()
                    if used(way, t + 1, sub):
                        hop(way, t + 1, sub).start()
        if t < last:
            on_block(lax.rem(d - t + nd, nd), t)
            on_block(lax.rem(d + t, nd), t)
        else:
            on_block(lax.rem(d + t, nd), t)
    for t in range(1, last + 1):
        for sub in range(2):
            for way in range(2):
                if used(way, t, sub):
                    hop(way, t, sub).wait_send()


def greet(axes):
    barrier = pltpu.get_barrier_semaphore()
    for axis, size in axes.items():
        me = lax.axis_index(axis)

        @pl.loop(1, size)
        def _(k):
            pl.semaphore_signal(
                barrier, inc=1, device_id={axis: lax.rem(me + k, size)}, device_id_type=MESH
            )

    pl.semaphore_wait(barrier, sum(axes.values()) - len(axes))


def attend_kernel(
    ns, nd, qk_ref, v_ref, drow_ref, dcol_ref, info_ref, out_ref, routes_ref, qh, kh, vh, att, si_sem,
    ri_sem, so_sem, ro_sem, sd_sem, rd_sem, local_sem,
):
    s = lax.axis_index("seq")
    d = lax.axis_index("dp")
    rows = v_ref.shape[0]
    length = rows * ns
    greet({"seq": ns, "dp": nd})

    def info_copy(to, slot):
        return pltpu.make_async_remote_copy(
            info_ref, routes_ref.at[slot], sd_sem.at[to], rd_sem.at[slot],
            device_id={"dp": to}, device_id_type=MESH,
        )

    def own_rows(ref, t):
        return ref.at[pl.ds(pl.multiple_of(t * rows, 16), rows)]

    def cols(t):
        return pl.ds(pl.multiple_of(t * HD, HD), HD)

    def pieces(t):
        return (
            (qk_ref.at[0, :, cols(t)], qh),
            (qk_ref.at[1, :, cols(t)], kh),
            (v_ref.at[:, cols(t)], vh),
        )

    def in_copies(j):
        to = lax.rem(s - ring_delta(j) + ns, ns)
        return [
            pltpu.make_async_remote_copy(
                src, own_rows(dst, s), si_sem.at[c, j], ri_sem.at[c, j],
                device_id={"seq": to}, device_id_type=MESH,
            )
            for c, (src, dst) in enumerate(pieces(to))
        ]

    def in_waits(j):
        frm = lax.rem(s + ring_delta(j) + ns, ns)
        return [
            pltpu.make_async_remote_copy(
                src, own_rows(dst, frm), si_sem.at[c, j], ri_sem.at[c, j],
                device_id={"seq": frm}, device_id_type=MESH,
            )
            for c, (src, dst) in enumerate(pieces(frm))
        ]

    @pl.loop(1, ns)
    def _(j):
        for c in in_copies(j):
            c.start()

    @pl.loop(1, nd)
    def _(k):
        info_copy(lax.rem(d + k, nd), d).start()

    routes_ref[d] = info_ref[...]
    local = [
        pltpu.make_async_copy(src, own_rows(dst, s), local_sem.at[c])
        for c, (src, dst) in enumerate(pieces(s))
    ]
    for c in local:
        c.start()
    for c in local:
        c.wait()

    @pl.loop(1, ns)
    def _(j):
        for c in in_waits(j):
            c.wait_recv()

    scale = 1.0 / math.sqrt(HD)
    step = 4 * rows
    for i in range(length // step):
        upto = (i + 1) * step
        span = pl.ds(i * step, step)
        scores = lax.dot_general(
            qh[span, :], kh[0:upto, :], (((1,), (1,)), ((), ())), preferred_element_type=F32
        ) * scale
        at = lax.broadcasted_iota(jnp.int32, (step, upto), 0) + i * step
        key_at = lax.broadcasted_iota(jnp.int32, (step, upto), 1)
        mine = jnp.concatenate([dcol_ref[span, :]] * (upto // HD), axis=1)
        allowed = (key_at <= at) & (mine == drow_ref[:, 0:upto])
        scores = jnp.where(allowed, scores, -1e30)
        lifted = jnp.exp(scores - jnp.max(scores, axis=-1, keepdims=True))
        weights = (lifted / jnp.sum(lifted, axis=-1, keepdims=True)).astype(BF16)
        att[span, :] = jnp.dot(weights, vh[0:upto, :], preferred_element_type=F32).astype(BF16)
        for t in range(4 * i, 4 * i + 4):

            @pl.when(s != t)
            def _():
                pltpu.make_async_remote_copy(
                    att.at[pl.ds(t * rows, rows)], out_ref.at[:, cols(s)], so_sem.at[t],
                    ro_sem.at[s], device_id={"seq": t}, device_id_type=MESH,
                ).start()

    home = pltpu.make_async_copy(own_rows(att, s), out_ref.at[:, cols(s)], local_sem.at[0])
    home.start()

    @pl.loop(1, ns)
    def _(j):
        for c in in_copies(j):
            c.wait_send()
        other = lax.rem(s + j, ns)
        done = pltpu.make_async_remote_copy(
            own_rows(att, other), out_ref.at[:, cols(other)], so_sem.at[other], ro_sem.at[other],
            device_id={"seq": other}, device_id_type=MESH,
        )
        done.wait_send()
        done.wait_recv()

    @pl.loop(1, nd)
    def _(k):
        other = lax.rem(d + k, nd)
        info_copy(other, other).wait_send()
        info_copy(other, other).wait_recv()

    home.wait()


def run_attention(qk, v, documents, info, ns, nd):
    rows, width = v.shape
    length = rows * ns
    dma = pltpu.SemaphoreType.DMA
    vmem = pl.BlockSpec(memory_space=pltpu.VMEM)
    return pl.pallas_call(
        functools.partial(attend_kernel, ns, nd),
        out_shape=(
            jax.ShapeDtypeStruct((rows, width), BF16),
            jax.ShapeDtypeStruct((nd,) + info.shape, F32),
        ),
        in_specs=[vmem] * 5,
        out_specs=(vmem, vmem),
        scratch_shapes=[pltpu.VMEM((length, HD), BF16)] * 4
        + [dma((3, ns)), dma((3, ns)), dma((ns,)), dma((ns,)), dma((nd,)), dma((nd,)), dma((3,))],
        compiler_params=pltpu.CompilerParams(
            collective_id=2, has_side_effects=True, vmem_limit_bytes=48 * 1024 * 1024
        ),
        cost_estimate=pl.CostEstimate(
            flops=4 * length * length * HD, bytes_accessed=8 * rows * width, transcendentals=0
        ),
        name="attend",
    )(qk, v, documents[None, :], jnp.broadcast_to(documents[:, None], (length, HD)), info)


def middle_kernel(
    nd, att_ref, w_ref, resid_ref, gain_ref, residual_ref, all_ref, att_all, column, projected,
    normed, s1_sem, r1_sem, s2_sem, r2_sem, sp_sem, rp_sem,
):
    d = lax.axis_index("dp")
    rows = att_ref.shape[0]
    block = w_ref.shape[1]
    greet({"dp": nd})

    def at(index):
        return pl.ds(pl.multiple_of(index * rows, 16), rows)

    def column_copy(to, frm):
        return pltpu.make_async_remote_copy(
            column.at[at(to)],
            projected.at[:, pl.ds(pl.multiple_of(frm * block, block), block)],
            sp_sem.at[to], rp_sem.at[frm], device_id={"dp": to}, device_id_type=MESH,
        )

    def project(index, step):
        src = att_ref[...] if step is None else att_all[at(index), :]
        out = jnp.dot(src, w_ref[...], preferred_element_type=F32).astype(BF16)
        if step is None:
            projected[:, pl.ds(pl.multiple_of(d * block, block), block)] = out
        else:
            column[at(index), :] = out
            column_copy(index, d).start()

    ring_gather(nd, "dp", att_ref, att_all, s1_sem, r1_sem, project)

    @pl.loop(1, nd)
    def _(k):
        other = lax.rem(d + k, nd)
        column_copy(other, other).wait_recv()
        column_copy(other, other).wait_send()

    residual = (resid_ref[...].astype(F32) + projected[...].astype(F32)).astype(BF16)
    residual_ref[...] = residual
    stream = residual.astype(F32)
    out = (
        stream
        * lax.rsqrt(jnp.mean(stream * stream, axis=-1, keepdims=True) + norm_eps)
        * gain_ref[...]
    ).astype(BF16)
    normed[...] = out
    all_ref[at(d), :] = out
    ring_gather(nd, "dp", normed, all_ref, s2_sem, r2_sem, lambda index, step: None)


def run_middle(own_attended, out_weight, resid, norm_gain, nd):
    rows, width = own_attended.shape
    dma = pltpu.SemaphoreType.DMA
    vmem = pl.BlockSpec(memory_space=pltpu.VMEM)
    ring = dma((2, nd // 2, 2))
    return pl.pallas_call(
        functools.partial(middle_kernel, nd),
        out_shape=(
            jax.ShapeDtypeStruct((rows, width), BF16),
            jax.ShapeDtypeStruct((nd * rows, width), BF16),
        ),
        in_specs=[vmem] * 4,
        out_specs=(vmem, vmem),
        scratch_shapes=[
            pltpu.VMEM((nd * rows, width), BF16),
            pltpu.VMEM((nd * rows, out_weight.shape[1]), BF16),
            pltpu.VMEM((rows, width), BF16),
            pltpu.VMEM((rows, width), BF16),
            ring, ring, ring, ring, dma((nd,)), dma((nd,)),
        ],
        compiler_params=pltpu.CompilerParams(
            collective_id=3, has_side_effects=True, vmem_limit_bytes=48 * 1024 * 1024
        ),
        cost_estimate=pl.CostEstimate(
            flops=2 * nd * rows * width * out_weight.shape[1],
            bytes_accessed=4 * nd * rows * width, transcendentals=0,
        ),
        name="middle",
    )(own_attended, out_weight, resid, norm_gain[None, :])


def finish_kernel(
    ns, nd, all_ref, routes_ref, residual_ref, score_ref, eg_hbm, eu_hbm, ed_hbm, sg_hbm, su_hbm,
    sd_hbm, out_ref, wg, wu, wd, vg, vu, vd, code, gates, ranks, send, own_in, pair_in, pair_out,
    pair_part, own_part, back, ret, total, landed, passed, w_sem, sy_sem, ry_sem, sx_sem, rx_sem,
    sp_sem, rp_sem, sr_sem, rr_sem, s2_sem, r2_sem,
):
    s = lax.axis_index("seq")
    d = lax.axis_index("dp")
    par = lax.rem(d, 2)
    partner = d + 1 - 2 * par
    tokens, width = all_ref.shape
    half = width // 2
    rows = nd * CAP
    own_tokens = tokens // nd
    group_rows = GROUP * rows
    groups = ns // GROUP
    per_seq = nd // SPLIT
    first_expert = d // SPLIT

    w_copies = [
        pltpu.make_async_copy(src, dst, w_sem.at[i])
        for i, (src, dst) in enumerate(
            (
                (eg_hbm.at[0], wg), (eu_hbm.at[0], wu), (ed_hbm.at[0], wd),
                (sg_hbm, vg), (su_hbm, vu), (sd_hbm, vd),
            )
        )
    ]
    for c in w_copies:
        c.start()
    greet({"seq": ns, "dp": nd})

    own_cols = pl.ds(pl.multiple_of(par * half, half), half)
    pair_cols = pl.ds(pl.multiple_of((1 - par) * half, half), half)

    def block(ref, j):
        return ref.at[pl.ds(pl.multiple_of(j * rows, 16), rows)]

    def span(g):
        return pl.ds(pl.multiple_of(g * group_rows, 16), group_rows)

    def out_copy(j):
        return pltpu.make_async_remote_copy(
            block(send, j), block(own_in, j), sy_sem.at[j], ry_sem.at[j],
            device_id={"seq": lax.rem(s - ring_delta(j) + ns, ns)}, device_id_type=MESH,
        )

    def swap_copy(g):
        return pltpu.make_async_remote_copy(
            own_in.at[span(g)], pair_in.at[span(g)], sx_sem.at[g], rx_sem.at[g],
            device_id={"dp": partner}, device_id_type=MESH,
        )

    def part_copy(g):
        return pltpu.make_async_remote_copy(
            pair_out.at[span(g)], pair_part.at[span(g)], sp_sem.at[g], rp_sem.at[g],
            device_id={"dp": partner}, device_id_type=MESH,
        )

    def back_copy(j):
        return pltpu.make_async_remote_copy(
            block(back, j), block(ret, j), sr_sem.at[j], rr_sem.at[j],
            device_id={"seq": lax.rem(s + ring_delta(j) + ns, ns)}, device_id_type=MESH,
        )

    lanes = 2 * own_tokens
    for m in range(nd // 2):
        tile = routes_ref[2 * m] + routes_ref[2 * m + 1]
        code[:, m * lanes : (m + 1) * lanes] = tile[:TOPK]
        gates[:, m * lanes : (m + 1) * lanes] = tile[TOPK:]
    slot = lax.broadcasted_iota(jnp.int32, (rows, tokens), 0).astype(F32)
    token = lax.broadcasted_iota(jnp.int32, (rows, tokens), 1).astype(F32)
    slot_block = jnp.floor((slot + 0.5) * (1.0 / CAP))
    token_block = jnp.floor((token + 0.5) * (1.0 / own_tokens))
    ranks[...] = jnp.where(slot_block == token_block, slot - slot_block * CAP, -1e6)

    def chosen(j):
        to = lax.rem(s - ring_delta(j) + ns, ns)
        base = ((to * per_seq + first_expert) * CAP).astype(F32)
        return [code[k : k + 1, :] - base == ranks[...] for k in range(TOPK)]

    def pick(j):
        hits = chosen(j)
        hit = functools.reduce(jnp.logical_or, hits)
        onehot = jnp.where(hit, 1.0, 0.0).astype(BF16)
        return jnp.dot(onehot, all_ref[:, own_cols], preferred_element_type=F32).astype(BF16)

    own_in[0:rows, :] = pick(0)

    @pl.loop(1, ns + 1)
    def _(j):
        @pl.when(j < ns)
        def _():
            send[pl.ds(pl.multiple_of(j * rows, 16), rows), :] = pick(j)

        @pl.when(j > 1)
        def _():
            out_copy(j - 1).start()

    for c in w_copies:
        c.wait()

    def nt(a, w):
        return lax.dot_general(a, w, (((1,), (1,)), ((), ())), preferred_element_type=F32)

    chunk = tokens // 4

    @pl.loop(0, groups + 5)
    def _(step):
        @pl.when(step < groups)
        def _():
            for i in range(GROUP):
                j = step * GROUP + i

                @pl.when(j > 0)
                def _():
                    out_copy(j).wait_recv()

            swap_copy(step).start()

        @pl.when((step >= 2) & (step < groups + 2))
        def _():
            g = step - 2
            part_copy(g).wait_recv()
            back[span(g), :] = (own_part[span(g), :] + pair_part[span(g), :].astype(F32)).astype(
                BF16
            )

        @pl.when((step >= 1) & (step <= groups))
        def _():
            g = step - 1
            swap_copy(g).wait_recv()
            a = own_in[span(g), :]
            b = pair_in[span(g), :]
            gate_act = nt(a, wg[:, own_cols]) + nt(b, wg[:, pair_cols])
            up_act = nt(a, wu[:, own_cols]) + nt(b, wu[:, pair_cols])
            hidden = (gate_act / (1.0 + jnp.exp(-gate_act)) * up_act).astype(BF16)
            pair_out[span(g), :] = jnp.dot(
                hidden, wd[:, pair_cols], preferred_element_type=F32
            ).astype(BF16)
            own_part[span(g), :] = jnp.dot(hidden, wd[:, own_cols], preferred_element_type=F32)
            part_copy(g).start()

        @pl.when((step >= 2) & (step < groups + 2))
        def _():
            for i in range(GROUP):
                j = (step - 2) * GROUP + i

                @pl.when(j > 0)
                def _():
                    back_copy(j).start()

                @pl.when(j == 0)
                def _():
                    ret[0:rows, :] = back[0:rows, :]

        @pl.when((step >= 1) & (step <= 4))
        def _():
            at = pl.ds(pl.multiple_of((step - 1) * chunk, chunk), chunk)
            a = all_ref[at, :]
            gate_act = nt(a, vg[...])
            hidden = (gate_act / (1.0 + jnp.exp(-gate_act)) * nt(a, vu[...])).astype(BF16)
            weight = jnp.sum(
                a.astype(F32) * score_ref[...].astype(F32), axis=-1, keepdims=True
            )
            weight = 1.0 / (1.0 + jnp.exp(-weight))
            total[at, :] = jnp.dot(hidden, vd[...], preferred_element_type=F32) * weight

        @pl.when(step >= 5)
        def _():
            g = step - 5
            weights = []
            for i in range(GROUP):
                j = g * GROUP + i

                @pl.when(j > 0)
                def _():
                    back_copy(j).wait_recv()

                hits = chosen(j)
                weights.append(
                    functools.reduce(
                        jnp.add,
                        [jnp.where(hits[k], gates[k : k + 1, :], 0.0) for k in range(TOPK)],
                    )
                )
            mix = jnp.concatenate(weights, axis=0).astype(BF16)
            total[:, own_cols] += lax.dot_general(
                mix, ret[span(g), :], (((0,), (0,)), ((), ())), preferred_element_type=F32
            )

    piece = own_tokens // 2
    last = nd // 2

    def own(index, sub):
        return pl.ds(pl.multiple_of(index * own_tokens + sub * piece, 16), piece)

    def used(way, t, sub):
        return t < last or (t == last and sub == way)

    def hop(way, t, sub):
        sign = 1 - 2 * way
        return pltpu.make_async_remote_copy(
            passed.at[way, t - 1, sub], landed.at[way, t - 1, sub], s2_sem.at[way, t - 1, sub],
            r2_sem.at[way, t - 1, sub],
            device_id={"dp": lax.rem(d + sign + nd, nd)}, device_id_type=MESH,
        )

    def target(way, t):
        return lax.rem(d + (1 - 2 * way) * t + nd, nd)

    for t in range(last, 0, -1):
        for sub in range(2):
            for way in range(2):
                if not used(way, t, sub):
                    continue
                term = total[own(target(way, t), sub), :]
                if used(way, t + 1, sub):
                    hop(way, t + 1, sub).wait_recv()
                    term = term + landed[way, t, sub].astype(F32)
                passed[way, t - 1, sub] = term.astype(BF16)
                hop(way, t, sub).start()
    for sub in range(2):
        for way in range(2):
            hop(way, 1, sub).wait_recv()
        at = pl.ds(sub * piece, piece)
        out_ref[at, :] = (
            residual_ref[at, :].astype(F32)
            + total[own(d, sub), :]
            + landed[0, 0, sub].astype(F32)
            + landed[1, 0, sub].astype(F32)
        ).astype(BF16)

    for way in range(2):
        for sub in range(2):
            for t in range(1, last + 1):
                if used(way, t, sub):
                    hop(way, t, sub).wait_send()

    @pl.loop(1, ns)
    def _(j):
        out_copy(j).wait_send()
        back_copy(j).wait_send()

    @pl.loop(0, groups)
    def _(g):
        swap_copy(g).wait_send()
        part_copy(g).wait_send()


def run_finish(normed_all, routes, residual, score, expert_weights, shared_weights, ns, nd):
    tokens, width = normed_all.shape
    half = width // 2
    rows = nd * CAP
    slots = ns * rows
    groups = ns // GROUP
    dma = pltpu.SemaphoreType.DMA
    hidden = expert_weights[0].shape[1]
    shared_hidden = shared_weights[0].shape[0]
    vmem = pl.BlockSpec(memory_space=pltpu.VMEM)
    anyspace = pl.BlockSpec(memory_space=pl.ANY)
    own_tokens = tokens // nd
    hops = pltpu.VMEM((2, nd // 2, 2, own_tokens // 2, width), BF16)
    ring = dma((2, nd // 2, 2))
    lane_rows = pltpu.VMEM((slots, half), BF16)
    return pl.pallas_call(
        functools.partial(finish_kernel, ns, nd),
        out_shape=jax.ShapeDtypeStruct(residual.shape, BF16),
        in_specs=[vmem] * 4 + [anyspace] * 6,
        out_specs=vmem,
        scratch_shapes=[pltpu.VMEM((hidden, width), BF16)] * 3
        + [pltpu.VMEM((shared_hidden, width), BF16)] * 3
        + [
            pltpu.VMEM((TOPK, tokens), F32),
            pltpu.VMEM((TOPK, tokens), F32),
            pltpu.VMEM((rows, tokens), F32),
            lane_rows, lane_rows, lane_rows, lane_rows, lane_rows,
            pltpu.VMEM((slots, half), F32),
            lane_rows, lane_rows,
            pltpu.VMEM((tokens, width), F32),
            hops, hops,
            dma((6,)), dma((ns,)), dma((ns,)), dma((groups,)), dma((groups,)), dma((groups,)),
            dma((groups,)), dma((ns,)), dma((ns,)), ring, ring,
        ],
        compiler_params=pltpu.CompilerParams(
            collective_id=1, has_side_effects=True, vmem_limit_bytes=63 * 1024 * 1024
        ),
        cost_estimate=pl.CostEstimate(
            flops=12 * slots * half * hidden, bytes_accessed=8 * slots * half, transcendentals=0
        ),
        name="finish",
    )(normed_all, routes, residual, score, *expert_weights, *shared_weights)


def body(
    resid,
    queries_keys,
    values,
    doc_ids,
    out_weight,
    norm_gain,
    expert_ids,
    gate_vals,
    expert_gate,
    expert_up,
    expert_down,
    shared_gate,
    shared_up,
    shared_down,
    shared_score,
):
    ns = lax.axis_size("seq")
    nd = lax.axis_size("dp")
    tokens = resid.shape[1]
    width = resid.shape[2]
    d = lax.axis_index("dp")
    documents = doc_ids[0]

    routes = expert_ids[0].T
    earlier = jnp.arange(tokens)[None, :] < jnp.arange(tokens)[:, None]
    same = routes[:, :, None, None] == routes[None, None, :, :]
    ranked = jnp.sum((same & earlier[None, :, None, :]).astype(jnp.int32), axis=(2, 3))
    info = jnp.concatenate([(routes * CAP + ranked).astype(F32), gate_vals[0].T], axis=0)
    blank = jnp.zeros_like(info)
    info = jnp.where(
        d % 2 == 0,
        jnp.concatenate([info, blank], axis=1),
        jnp.concatenate([blank, info], axis=1),
    )

    own_attended, all_routes = run_attention(
        queries_keys.reshape(2, tokens, width), values[0], documents, info, ns, nd
    )
    residual, normed_all = run_middle(own_attended, out_weight, resid[0], norm_gain, nd)
    out = run_finish(
        normed_all,
        all_routes,
        residual,
        shared_score[None, :],
        (expert_gate.transpose(0, 2, 1), expert_up.transpose(0, 2, 1), expert_down),
        (shared_gate.T, shared_up.T, shared_down),
        ns,
        nd,
    )
    return out[None]


def solution(mesh):
    placed = (
        P(("groups", "dp"), "seq", None),
        P(None, ("groups", "dp"), "seq", None),
        P(("groups", "dp"), "seq", None),
        P(("groups", "dp"), None),
        P(None, "dp"),
        P(),
        P(("groups", "dp"), "seq", None),
        P(("groups", "dp"), "seq", None),
        P(("seq", "dp"), None, None),
        P(("seq", "dp"), None, None),
        P(("seq", "dp"), None, None),
        P(None, "dp"),
        P(None, "dp"),
        P("dp", None),
        P(),
    )
    return jax.shard_map(
        body,
        mesh=mesh,
        in_specs=placed,
        out_specs=P(("groups", "dp"), "seq", None),
        check_vma=False,
    )
```

```python
import functools
import math

import jax
import jax.numpy as jnp
from jax import lax
from jax.experimental import pallas as pl
from jax.experimental.pallas import tpu as pltpu
from jax.sharding import PartitionSpec as P

HD = 128
TOPK = 4
SPLIT = 4
CAP = 10
GROUP = 2
CORES = 2

norm_eps = 1e-06
MESH = pl.DeviceIdType.MESH
F32 = jnp.float32
BF16 = jnp.bfloat16


def ring_delta(j):
    return ((j + 1) // 2) * (2 * (j % 2) - 1)


class Ring:
    def __init__(self, nd, axis, source, place, send_sem, recv_sem):
        self.nd, self.axis, self.last = nd, axis, nd // 2
        self.source, self.place = source, place
        self.send_sem, self.recv_sem = send_sem, recv_sem
        self.me = lax.axis_index(axis)

    def behind(self, t, way):
        return lax.rem(self.me - (1 - 2 * way) * t + self.nd, self.nd)

    def hop(self, way, t, sub):
        index = self.behind(t - 1, way)
        src = self.source(sub) if t == 1 else self.place(index, sub)
        return pltpu.make_async_remote_copy(
            src, self.place(index, sub), self.send_sem.at[way, t - 1, sub],
            self.recv_sem.at[way, t - 1, sub],
            device_id={self.axis: self.behind(-1, way)}, device_id_type=MESH,
        )

    def hops(self, t):
        return [
            (way, t, sub)
            for sub in range(2)
            for way in range(2)
            if t < self.last or (t == self.last and sub == way)
        ]

    def start(self):
        for h in self.hops(1):
            self.hop(*h).start()

    def advance(self, t):
        following = self.hops(t + 1)
        for way, _, sub in self.hops(t):
            self.hop(way, t, sub).wait_recv()
            if (way, t + 1, sub) in following:
                self.hop(way, t + 1, sub).start()

    def arrived(self, t):
        return [self.behind(t, 0), self.behind(t, 1)] if t < self.last else [self.behind(t, 0)]

    def finish(self):
        for t in range(1, self.last + 1):
            for h in self.hops(t):
                self.hop(*h).wait_send()


def greet(axes):
    barrier = pltpu.get_barrier_semaphore()
    for axis, size in axes.items():
        me = lax.axis_index(axis)

        @pl.loop(1, size)
        def _(k):
            pl.semaphore_signal(
                barrier, inc=1, device_id={axis: lax.rem(me + k, size)}, device_id_type=MESH
            )

    pl.semaphore_wait(barrier, sum(axes.values()) - len(axes))


def front_kernel(
    ns, nd, qk_ref, v_ref, drow_ref, dcol_ref, info_ref, w_hbm, resid_ref, gain_ref, residual_ref,
    all_ref, routes_ref, qh, kh, vh, att, mixed, wall, own_sum, send_sum, got_sum, normed, si_sem,
    ri_sem, so_sem, ro_sem, sd_sem, rd_sem, sp_sem, rp_sem, sw_sem, rw_sem, sg_sem, rg_sem, w_sem,
    local_sem,
):
    s = lax.axis_index("seq")
    d = lax.axis_index("dp")
    rows, width = v_ref.shape
    length = rows * ns
    core = lax.rem(s, CORES)
    chips = ns // CORES
    depth = width // CORES
    block = width // nd
    chip_rows = rows * CORES

    w_own = pltpu.make_async_copy(
        w_hbm.at[pl.ds(pl.multiple_of(core * depth, 16), depth)], wall.at[d], w_sem.at[0]
    )
    w_own.start()
    greet({"seq": ns, "dp": nd})

    def own_rows(ref, t):
        return ref.at[pl.ds(pl.multiple_of(t * rows, 16), rows)]

    def cols(t):
        return pl.ds(pl.multiple_of(t * HD, HD), HD)

    def info_copy(to, slot):
        return pltpu.make_async_remote_copy(
            info_ref, routes_ref.at[slot], sd_sem.at[to], rd_sem.at[slot],
            device_id={"dp": to}, device_id_type=MESH,
        )

    def pieces(t):
        return (
            (qk_ref.at[0, :, cols(t)], qh),
            (qk_ref.at[1, :, cols(t)], kh),
            (v_ref.at[:, cols(t)], vh),
        )

    def in_copies(j, to, slot):
        return [
            pltpu.make_async_remote_copy(
                src, own_rows(dst, slot), si_sem.at[c, j], ri_sem.at[c, j],
                device_id={"seq": to}, device_id_type=MESH,
            )
            for c, (src, dst) in enumerate(pieces(to))
        ]

    def sent(j):
        return in_copies(j, lax.rem(s - ring_delta(j) + ns, ns), s)

    def received(j):
        frm = lax.rem(s + ring_delta(j) + ns, ns)
        return in_copies(j, frm, frm)

    @pl.loop(1, ns)
    def _(j):
        for c in sent(j):
            c.start()

    @pl.loop(1, nd)
    def _(k):
        info_copy(lax.rem(d + k, nd), d).start()

    w_part = depth // 2
    weights = Ring(
        nd, "dp",
        lambda sub: wall.at[d, pl.ds(sub * w_part, w_part)],
        lambda index, sub: wall.at[index, pl.ds(sub * w_part, w_part)],
        sw_sem, rw_sem,
    )
    w_own.wait()
    weights.start()

    routes_ref[d] = info_ref[...]
    local = [
        pltpu.make_async_copy(src, own_rows(dst, s), local_sem.at[c])
        for c, (src, dst) in enumerate(pieces(s))
    ]
    for c in local:
        c.start()
    for c in local:
        c.wait()

    @pl.loop(1, ns // 2)
    def _(j):
        for c in received(j):
            c.wait_recv()

    weights.advance(1)

    @pl.loop(ns // 2, ns)
    def _(j):
        for c in received(j):
            c.wait_recv()

    per_core = ns // CORES
    mate = s + 1 - 2 * core

    def owner(chip):
        return chip * CORES + s // per_core

    def out_copy(chip, head):
        return pltpu.make_async_remote_copy(
            att.at[pl.ds(pl.multiple_of(chip * chip_rows, 16), chip_rows)],
            mixed.at[:, cols(lax.rem(head, per_core))], so_sem.at[chip],
            ro_sem.at[lax.rem(head, per_core)],
            device_id={"seq": owner(chip)}, device_id_type=MESH,
        )

    scale = 1.0 / math.sqrt(HD)
    step = 2 * chip_rows
    for i in range(length // step):
        upto = (i + 1) * step
        span = pl.ds(i * step, step)
        scores = lax.dot_general(
            qh[span, :], kh[0:upto, :], (((1,), (1,)), ((), ())), preferred_element_type=F32
        ) * scale
        at = lax.broadcasted_iota(jnp.int32, (step, upto), 0) + i * step
        key_at = lax.broadcasted_iota(jnp.int32, (step, upto), 1)
        mine = jnp.concatenate([dcol_ref[span, :]] * (upto // HD), axis=1)
        allowed = (key_at <= at) & (mine == drow_ref[:, 0:upto])
        scores = jnp.where(allowed, scores, -1e30)
        lifted = jnp.exp(scores - jnp.max(scores, axis=-1, keepdims=True))
        probs = (lifted / jnp.sum(lifted, axis=-1, keepdims=True)).astype(BF16)
        att[span, :] = jnp.dot(probs, vh[0:upto, :], preferred_element_type=F32).astype(BF16)
        for chip in (2 * i, 2 * i + 1):

            @pl.when(owner(chip) != s)
            def _():
                out_copy(chip, s).start()

            @pl.when(owner(chip) == s)
            def _():
                mixed[:, cols(lax.rem(s, per_core))] = att[
                    pl.ds(chip * chip_rows, chip_rows), :
                ]

        if i == 1:
            weights.advance(2)

    @pl.loop(0, per_core)
    def _(h):
        @pl.when(core * per_core + h != s)
        def _():
            out_copy(0, h).wait_recv()

    def sum_copy(index):
        at = pl.ds(pl.multiple_of(index * block, block), block)
        return pltpu.make_async_remote_copy(
            send_sum.at[:, at], got_sum.at[:, at], sp_sem.at[index], rp_sem.at[index],
            device_id={"seq": mate}, device_id_type=MESH,
        )

    def project(index):
        at = pl.ds(pl.multiple_of(index * block, block), block)
        theirs = mixed[pl.ds(pl.multiple_of((1 - core) * rows, 16), rows), :]
        mine = mixed[pl.ds(pl.multiple_of(core * rows, 16), rows), :]
        send_sum[:, at] = jnp.dot(theirs, wall[index], preferred_element_type=F32)
        own_sum[:, at] = jnp.dot(mine, wall[index], preferred_element_type=F32)
        sum_copy(index).start()

    project(d)
    for t in range(1, nd // 2 + 1):
        if t >= 3:
            weights.advance(t)
        for index in weights.arrived(t):
            project(index)

    @pl.loop(0, nd)
    def _(index):
        sum_copy(index).wait_recv()

    projected = (own_sum[...] + got_sum[...]).astype(BF16)
    residual = (resid_ref[...].astype(F32) + projected.astype(F32)).astype(BF16)
    residual_ref[...] = residual
    stream = residual.astype(F32)
    out = (
        stream
        * lax.rsqrt(jnp.mean(stream * stream, axis=-1, keepdims=True) + norm_eps)
        * gain_ref[...]
    ).astype(BF16)
    normed[...] = out
    own_rows(all_ref, d)[...] = out
    part = rows // 2
    gather = Ring(
        nd, "dp",
        lambda sub: normed.at[pl.ds(sub * part, part)],
        lambda index, sub: all_ref.at[pl.ds(pl.multiple_of(index * rows + sub * part, 16), part)],
        sg_sem, rg_sem,
    )
    gather.start()
    for t in range(1, nd // 2 + 1):
        gather.advance(t)
    gather.finish()
    weights.finish()

    @pl.loop(1, ns)
    def _(j):
        for c in sent(j):
            c.wait_send()

    @pl.loop(0, chips)
    def _(chip):
        @pl.when(owner(chip) != s)
        def _():
            out_copy(chip, s).wait_send()

    @pl.loop(0, nd)
    def _(index):
        sum_copy(index).wait_send()

    @pl.loop(1, nd)
    def _(k):
        other = lax.rem(d + k, nd)
        info_copy(other, other).wait_send()
        info_copy(other, other).wait_recv()


def run_front(qk, v, documents, info, out_weight, resid, norm_gain, ns, nd):
    rows, width = v.shape
    length = rows * ns
    dma = pltpu.SemaphoreType.DMA
    vmem = pl.BlockSpec(memory_space=pltpu.VMEM)
    anyspace = pl.BlockSpec(memory_space=pl.ANY)
    ring = dma((2, nd // 2, 2))
    sums = pltpu.VMEM((rows, width), F32)
    return pl.pallas_call(
        functools.partial(front_kernel, ns, nd),
        out_shape=(
            jax.ShapeDtypeStruct((rows, width), BF16),
            jax.ShapeDtypeStruct((nd * rows, width), BF16),
            jax.ShapeDtypeStruct((nd,) + info.shape, F32),
        ),
        in_specs=[vmem] * 5 + [anyspace] + [vmem] * 2,
        out_specs=(vmem,) * 3,
        scratch_shapes=[pltpu.VMEM((length, HD), BF16)] * 4
        + [
            pltpu.VMEM((rows * CORES, width // CORES), BF16),
            pltpu.VMEM((nd, width // CORES, out_weight.shape[1]), BF16),
            sums, sums, sums,
            pltpu.VMEM((rows, width), BF16),
            dma((3, ns)), dma((3, ns)), dma((ns // CORES,)), dma((ns // CORES,)),
            dma((nd,)), dma((nd,)), dma((nd,)), dma((nd,)),
            ring, ring, ring, ring, dma((1,)), dma((3,)),
        ],
        compiler_params=pltpu.CompilerParams(
            collective_id=2, has_side_effects=True, vmem_limit_bytes=48 * 1024 * 1024
        ),
        cost_estimate=pl.CostEstimate(
            flops=4 * length * length * HD, bytes_accessed=8 * rows * width, transcendentals=0
        ),
        name="front",
    )(
        qk, v, documents[None, :], jnp.broadcast_to(documents[:, None], (length, HD)), info,
        out_weight, resid, norm_gain[None, :],
    )


def finish_kernel(
    ns, nd, all_ref, routes_ref, residual_ref, score_ref, eg_hbm, eu_hbm, ed_hbm, sg_hbm, su_hbm,
    sd_hbm, out_ref, wg, wu, wd, vg, vu, vd, code, gates, ranks, send, own_in, pair_in, pair_out,
    pair_part, own_part, back, ret, total, landed, passed, w_sem, sy_sem, ry_sem, sx_sem, rx_sem,
    sp_sem, rp_sem, sr_sem, rr_sem, s2_sem, r2_sem,
):
    s = lax.axis_index("seq")
    d = lax.axis_index("dp")
    par = lax.rem(d, 2)
    partner = d + 1 - 2 * par
    tokens, width = all_ref.shape
    half = width // 2
    rows = nd * CAP
    own_tokens = tokens // nd
    group_rows = GROUP * rows
    groups = ns // GROUP
    per_seq = nd // SPLIT
    first_expert = d // SPLIT

    w_copies = [
        pltpu.make_async_copy(src, dst, w_sem.at[i])
        for i, (src, dst) in enumerate(
            (
                (eg_hbm.at[0], wg), (eu_hbm.at[0], wu), (ed_hbm.at[0], wd),
                (sg_hbm, vg), (su_hbm, vu), (sd_hbm, vd),
            )
        )
    ]
    for c in w_copies:
        c.start()
    greet({"seq": ns, "dp": nd})

    own_cols = pl.ds(pl.multiple_of(par * half, half), half)
    pair_cols = pl.ds(pl.multiple_of((1 - par) * half, half), half)

    def block(ref, j):
        return ref.at[pl.ds(pl.multiple_of(j * rows, 16), rows)]

    def span(g):
        return pl.ds(pl.multiple_of(g * group_rows, 16), group_rows)

    def out_copy(j):
        return pltpu.make_async_remote_copy(
            block(send, j), block(own_in, j), sy_sem.at[j], ry_sem.at[j],
            device_id={"seq": lax.rem(s - ring_delta(j) + ns, ns)}, device_id_type=MESH,
        )

    def swap_copy(g):
        return pltpu.make_async_remote_copy(
            own_in.at[span(g)], pair_in.at[span(g)], sx_sem.at[g], rx_sem.at[g],
            device_id={"dp": partner}, device_id_type=MESH,
        )

    def part_copy(g):
        return pltpu.make_async_remote_copy(
            pair_out.at[span(g)], pair_part.at[span(g)], sp_sem.at[g], rp_sem.at[g],
            device_id={"dp": partner}, device_id_type=MESH,
        )

    def back_copy(j):
        return pltpu.make_async_remote_copy(
            block(back, j), block(ret, j), sr_sem.at[j], rr_sem.at[j],
            device_id={"seq": lax.rem(s + ring_delta(j) + ns, ns)}, device_id_type=MESH,
        )

    lanes = 2 * own_tokens
    for m in range(nd // 2):
        tile = routes_ref[2 * m] + routes_ref[2 * m + 1]
        code[:, m * lanes : (m + 1) * lanes] = tile[:TOPK]
        gates[:, m * lanes : (m + 1) * lanes] = tile[TOPK:]
    slot = lax.broadcasted_iota(jnp.int32, (rows, tokens), 0).astype(F32)
    token = lax.broadcasted_iota(jnp.int32, (rows, tokens), 1).astype(F32)
    slot_block = jnp.floor((slot + 0.5) * (1.0 / CAP))
    token_block = jnp.floor((token + 0.5) * (1.0 / own_tokens))
    ranks[...] = jnp.where(slot_block == token_block, slot - slot_block * CAP, -1e6)

    def chosen(j):
        to = lax.rem(s - ring_delta(j) + ns, ns)
        base = ((to * per_seq + first_expert) * CAP).astype(F32)
        return [code[k : k + 1, :] - base == ranks[...] for k in range(TOPK)]

    def pick(j):
        hits = chosen(j)
        hit = functools.reduce(jnp.logical_or, hits)
        onehot = jnp.where(hit, 1.0, 0.0).astype(BF16)
        return jnp.dot(onehot, all_ref[:, own_cols], preferred_element_type=F32).astype(BF16)

    own_in[0:rows, :] = pick(0)

    @pl.loop(1, ns + 1)
    def _(j):
        @pl.when(j < ns)
        def _():
            send[pl.ds(pl.multiple_of(j * rows, 16), rows), :] = pick(j)

        @pl.when(j > 1)
        def _():
            out_copy(j - 1).start()

    for c in w_copies:
        c.wait()

    def nt(a, w):
        return lax.dot_general(a, w, (((1,), (1,)), ((), ())), preferred_element_type=F32)

    chunk = tokens // 4

    @pl.loop(0, groups + 5)
    def _(step):
        @pl.when(step < groups)
        def _():
            for i in range(GROUP):
                j = step * GROUP + i

                @pl.when(j > 0)
                def _():
                    out_copy(j).wait_recv()

            swap_copy(step).start()

        @pl.when((step >= 2) & (step < groups + 2))
        def _():
            g = step - 2
            part_copy(g).wait_recv()
            back[span(g), :] = (own_part[span(g), :] + pair_part[span(g), :].astype(F32)).astype(
                BF16
            )

        @pl.when((step >= 1) & (step <= groups))
        def _():
            g = step - 1
            swap_copy(g).wait_recv()
            a = own_in[span(g), :]
            b = pair_in[span(g), :]
            gate_act = nt(a, wg[:, own_cols]) + nt(b, wg[:, pair_cols])
            up_act = nt(a, wu[:, own_cols]) + nt(b, wu[:, pair_cols])
            hidden = (gate_act / (1.0 + jnp.exp(-gate_act)) * up_act).astype(BF16)
            pair_out[span(g), :] = jnp.dot(
                hidden, wd[:, pair_cols], preferred_element_type=F32
            ).astype(BF16)
            own_part[span(g), :] = jnp.dot(hidden, wd[:, own_cols], preferred_element_type=F32)
            part_copy(g).start()

        @pl.when((step >= 2) & (step < groups + 2))
        def _():
            for i in range(GROUP):
                j = (step - 2) * GROUP + i

                @pl.when(j > 0)
                def _():
                    back_copy(j).start()

                @pl.when(j == 0)
                def _():
                    ret[0:rows, :] = back[0:rows, :]

        @pl.when((step >= 1) & (step <= 4))
        def _():
            at = pl.ds(pl.multiple_of((step - 1) * chunk, chunk), chunk)
            a = all_ref[at, :]
            gate_act = nt(a, vg[...])
            hidden = (gate_act / (1.0 + jnp.exp(-gate_act)) * nt(a, vu[...])).astype(BF16)
            weight = jnp.sum(
                a.astype(F32) * score_ref[...].astype(F32), axis=-1, keepdims=True
            )
            weight = 1.0 / (1.0 + jnp.exp(-weight))
            total[at, :] = jnp.dot(hidden, vd[...], preferred_element_type=F32) * weight

        @pl.when(step >= 5)
        def _():
            g = step - 5
            weights = []
            for i in range(GROUP):
                j = g * GROUP + i

                @pl.when(j > 0)
                def _():
                    back_copy(j).wait_recv()

                hits = chosen(j)
                weights.append(
                    functools.reduce(
                        jnp.add,
                        [jnp.where(hits[k], gates[k : k + 1, :], 0.0) for k in range(TOPK)],
                    )
                )
            mix = jnp.concatenate(weights, axis=0).astype(BF16)
            total[:, own_cols] += lax.dot_general(
                mix, ret[span(g), :], (((0,), (0,)), ((), ())), preferred_element_type=F32
            )

    piece = own_tokens // 2
    last = nd // 2

    def own(index, sub):
        return pl.ds(pl.multiple_of(index * own_tokens + sub * piece, 16), piece)

    def used(way, t, sub):
        return t < last or (t == last and sub == way)

    def hop(way, t, sub):
        sign = 1 - 2 * way
        return pltpu.make_async_remote_copy(
            passed.at[way, t - 1, sub], landed.at[way, t - 1, sub], s2_sem.at[way, t - 1, sub],
            r2_sem.at[way, t - 1, sub],
            device_id={"dp": lax.rem(d + sign + nd, nd)}, device_id_type=MESH,
        )

    def target(way, t):
        return lax.rem(d + (1 - 2 * way) * t + nd, nd)

    for t in range(last, 0, -1):
        for sub in range(2):
            for way in range(2):
                if not used(way, t, sub):
                    continue
                term = total[own(target(way, t), sub), :]
                if used(way, t + 1, sub):
                    hop(way, t + 1, sub).wait_recv()
                    term = term + landed[way, t, sub].astype(F32)
                passed[way, t - 1, sub] = term.astype(BF16)
                hop(way, t, sub).start()
    for sub in range(2):
        for way in range(2):
            hop(way, 1, sub).wait_recv()
        at = pl.ds(sub * piece, piece)
        out_ref[at, :] = (
            residual_ref[at, :].astype(F32)
            + total[own(d, sub), :]
            + landed[0, 0, sub].astype(F32)
            + landed[1, 0, sub].astype(F32)
        ).astype(BF16)

    for way in range(2):
        for sub in range(2):
            for t in range(1, last + 1):
                if used(way, t, sub):
                    hop(way, t, sub).wait_send()

    @pl.loop(1, ns)
    def _(j):
        out_copy(j).wait_send()
        back_copy(j).wait_send()

    @pl.loop(0, groups)
    def _(g):
        swap_copy(g).wait_send()
        part_copy(g).wait_send()


def run_finish(normed_all, routes, residual, score, expert_weights, shared_weights, ns, nd):
    tokens, width = normed_all.shape
    half = width // 2
    rows = nd * CAP
    slots = ns * rows
    groups = ns // GROUP
    dma = pltpu.SemaphoreType.DMA
    hidden = expert_weights[0].shape[1]
    shared_hidden = shared_weights[0].shape[0]
    vmem = pl.BlockSpec(memory_space=pltpu.VMEM)
    anyspace = pl.BlockSpec(memory_space=pl.ANY)
    own_tokens = tokens // nd
    hops = pltpu.VMEM((2, nd // 2, 2, own_tokens // 2, width), BF16)
    ring = dma((2, nd // 2, 2))
    lane_rows = pltpu.VMEM((slots, half), BF16)
    return pl.pallas_call(
        functools.partial(finish_kernel, ns, nd),
        out_shape=jax.ShapeDtypeStruct(residual.shape, BF16),
        in_specs=[vmem] * 4 + [anyspace] * 6,
        out_specs=vmem,
        scratch_shapes=[pltpu.VMEM((hidden, width), BF16)] * 3
        + [pltpu.VMEM((shared_hidden, width), BF16)] * 3
        + [
            pltpu.VMEM((TOPK, tokens), F32),
            pltpu.VMEM((TOPK, tokens), F32),
            pltpu.VMEM((rows, tokens), F32),
            lane_rows, lane_rows, lane_rows, lane_rows, lane_rows,
            pltpu.VMEM((slots, half), F32),
            lane_rows, lane_rows,
            pltpu.VMEM((tokens, width), F32),
            hops, hops,
            dma((6,)), dma((ns,)), dma((ns,)), dma((groups,)), dma((groups,)), dma((groups,)),
            dma((groups,)), dma((ns,)), dma((ns,)), ring, ring,
        ],
        compiler_params=pltpu.CompilerParams(
            collective_id=1, has_side_effects=True, vmem_limit_bytes=63 * 1024 * 1024
        ),
        cost_estimate=pl.CostEstimate(
            flops=12 * slots * half * hidden, bytes_accessed=8 * slots * half, transcendentals=0
        ),
        name="finish",
    )(normed_all, routes, residual, score, *expert_weights, *shared_weights)


def body(
    resid,
    queries_keys,
    values,
    doc_ids,
    out_weight,
    norm_gain,
    expert_ids,
    gate_vals,
    expert_gate,
    expert_up,
    expert_down,
    shared_gate,
    shared_up,
    shared_down,
    shared_score,
):
    ns = lax.axis_size("seq")
    nd = lax.axis_size("dp")
    tokens = resid.shape[1]
    width = resid.shape[2]
    d = lax.axis_index("dp")
    documents = doc_ids[0]

    routes = expert_ids[0].T
    earlier = jnp.arange(tokens)[None, :] < jnp.arange(tokens)[:, None]
    same = routes[:, :, None, None] == routes[None, None, :, :]
    ranked = jnp.sum((same & earlier[None, :, None, :]).astype(jnp.int32), axis=(2, 3))
    info = jnp.concatenate([(routes * CAP + ranked).astype(F32), gate_vals[0].T], axis=0)
    blank = jnp.zeros_like(info)
    info = jnp.where(
        d % 2 == 0,
        jnp.concatenate([info, blank], axis=1),
        jnp.concatenate([blank, info], axis=1),
    )

    residual, normed_all, all_routes = run_front(
        queries_keys.reshape(2, tokens, width), values[0], documents, info, out_weight, resid[0],
        norm_gain, ns, nd,
    )
    out = run_finish(
        normed_all,
        all_routes,
        residual,
        shared_score[None, :],
        (expert_gate.transpose(0, 2, 1), expert_up.transpose(0, 2, 1), expert_down),
        (shared_gate.T, shared_up.T, shared_down),
        ns,
        nd,
    )
    return out[None]


def solution(mesh):
    placed = (
        P(("groups", "dp"), "seq", None),
        P(None, ("groups", "dp"), "seq", None),
        P(("groups", "dp"), "seq", None),
        P(("groups", "dp"), None),
        P(None, "dp"),
        P(),
        P(("groups", "dp"), "seq", None),
        P(("groups", "dp"), "seq", None),
        P(("seq", "dp"), None, None),
        P(("seq", "dp"), None, None),
        P(("seq", "dp"), None, None),
        P(None, "dp"),
        P(None, "dp"),
        P("dp", None),
        P(),
    )
    return jax.shard_map(
        body,
        mesh=mesh,
        in_specs=placed,
        out_specs=P(("groups", "dp"), "seq", None),
        check_vma=False,
    )
```

```python
import functools
import math

import jax
import jax.numpy as jnp
from jax import lax
from jax.experimental import pallas as pl
from jax.experimental.pallas import tpu as pltpu
from jax.sharding import PartitionSpec as P

HD = 128
TOPK = 4
SPLIT = 4
CAP = 10
GROUP = 2
CORES = 2

norm_eps = 1e-06
MESH = pl.DeviceIdType.MESH
F32 = jnp.float32
BF16 = jnp.bfloat16


def ring_delta(j):
    return ((j + 1) // 2) * (2 * (j % 2) - 1)


class Ring:
    def __init__(self, nd, axis, source, place, send_sem, recv_sem):
        self.nd, self.axis, self.last = nd, axis, nd // 2
        self.source, self.place = source, place
        self.send_sem, self.recv_sem = send_sem, recv_sem
        self.me = lax.axis_index(axis)

    def behind(self, t, way):
        return lax.rem(self.me - (1 - 2 * way) * t + self.nd, self.nd)

    def hop(self, way, t, sub):
        index = self.behind(t - 1, way)
        src = self.source(sub) if t == 1 else self.place(index, sub)
        return pltpu.make_async_remote_copy(
            src, self.place(index, sub), self.send_sem.at[way, t - 1, sub],
            self.recv_sem.at[way, t - 1, sub],
            device_id={self.axis: self.behind(-1, way)}, device_id_type=MESH,
        )

    def hops(self, t):
        return [
            (way, t, sub)
            for sub in range(2)
            for way in range(2)
            if t < self.last or (t == self.last and sub == way)
        ]

    def start(self):
        for h in self.hops(1):
            self.hop(*h).start()

    def advance(self, t):
        following = self.hops(t + 1)
        for way, _, sub in self.hops(t):
            self.hop(way, t, sub).wait_recv()
            if (way, t + 1, sub) in following:
                self.hop(way, t + 1, sub).start()

    def arrived(self, t):
        return [self.behind(t, 0), self.behind(t, 1)] if t < self.last else [self.behind(t, 0)]

    def finish(self):
        for t in range(1, self.last + 1):
            for h in self.hops(t):
                self.hop(*h).wait_send()


def greet(axes):
    barrier = pltpu.get_barrier_semaphore()
    for axis, size in axes.items():
        me = lax.axis_index(axis)

        @pl.loop(1, size)
        def _(k):
            pl.semaphore_signal(
                barrier, inc=1, device_id={axis: lax.rem(me + k, size)}, device_id_type=MESH
            )

    pl.semaphore_wait(barrier, sum(axes.values()) - len(axes))


def layer_kernel(
    ns, nd, docs_ref, info_ref, vecs_ref, qk_hbm, v_hbm, resid_hbm, w_hbm, eg_hbm, eu_hbm, ed_hbm,
    sg_hbm, su_hbm, sd_hbm, out_ref,
    qk, v, resid, wg, wu, wd, vg, vu, vd, dcol, info, routes, qh, kh, vh, att, mixed, wall, own_sum,
    send_sum, got_sum, residual, normed, every, picks, mixes, send, own_in, pair_in, act, pair_out,
    pair_part, own_part, back, ret, total, landed, passed,
    w_sem, local_sem, si_sem, ri_sem, so_sem, ro_sem, sd_sem, rd_sem, sp_sem, rp_sem, sw_sem, rw_sem,
    sg_sem, rg_sem, sy_sem, ry_sem, sx_sem, rx_sem, sq_sem, rq_sem, sr_sem, rr_sem, s2_sem, r2_sem,
):
    s = lax.axis_index("seq")
    d = lax.axis_index("dp")
    rows, width = v.shape
    length = rows * ns
    tokens = rows * nd
    core = lax.rem(s, CORES)
    chips = ns // CORES
    depth = width // CORES
    block = width // nd
    chip_rows = rows * CORES
    half = width // 2
    quarter = half // 2
    lanes = 2 * rows

    first = [
        pltpu.make_async_copy(src, dst, w_sem.at[i])
        for i, (src, dst) in enumerate(
            (
                (qk_hbm, qk), (v_hbm, v),
                (w_hbm.at[pl.ds(pl.multiple_of(core * depth, 16), depth)], wall.at[d]),
                (resid_hbm, resid),
            )
        )
    ]
    later = [
        pltpu.make_async_copy(src, dst, w_sem.at[4 + i])
        for i, (src, dst) in enumerate(
            (
                (sg_hbm, vg), (su_hbm, vu), (sd_hbm, vd),
                (eg_hbm.at[0], wg), (eu_hbm.at[0], wu), (ed_hbm.at[0], wd),
            )
        )
    ]
    for c in first:
        c.start()

    experts = ns * nd // SPLIT
    lane = lax.broadcasted_iota(jnp.int32, (1, lanes), 1)
    valid = (lane >= lax.rem(d, 2) * rows) & (lane < (lax.rem(d, 2) + 1) * rows)
    expert = lax.broadcasted_iota(jnp.int32, (experts, lanes), 0).astype(F32)
    chosen_ids = [jnp.where(valid, info_ref[k : k + 1, :], -1.0) for k in range(TOPK)]
    named = [ids == expert for ids in chosen_ids]
    earlier = lax.broadcasted_iota(jnp.int32, (lanes, lanes), 0) < lax.broadcasted_iota(
        jnp.int32, (lanes, lanes), 1
    )
    counts = jnp.dot(
        jnp.where(functools.reduce(jnp.logical_or, named), 1.0, 0.0).astype(BF16),
        jnp.where(earlier, 1.0, 0.0).astype(BF16),
        preferred_element_type=F32,
    )
    for k in range(TOPK):
        rank = jnp.sum(jnp.where(named[k], counts, 0.0), axis=0, keepdims=True)
        info[k : k + 1, :] = jnp.where(valid, chosen_ids[k] * CAP + rank, 0.0)
    info[TOPK:, :] = info_ref[TOPK:, :]
    routes[d] = info[...]
    docs = docs_ref[...].astype(F32)
    for i in range(length // HD):
        tile = jnp.broadcast_to(docs[:, i * HD : (i + 1) * HD], (HD, HD))
        dcol[i * HD : (i + 1) * HD, :] = tile.T

    greet({"seq": ns, "dp": nd})
    first[0].wait()
    first[1].wait()

    def own_rows(ref, t):
        return ref.at[pl.ds(pl.multiple_of(t * rows, 16), rows)]

    def cols(t):
        return pl.ds(pl.multiple_of(t * HD, HD), HD)

    def info_copy(to, slot):
        return pltpu.make_async_remote_copy(
            info, routes.at[slot], sd_sem.at[to], rd_sem.at[slot],
            device_id={"dp": to}, device_id_type=MESH,
        )

    def pieces(t):
        return (
            (qk.at[0, :, cols(t)], qh),
            (qk.at[1, :, cols(t)], kh),
            (v.at[:, cols(t)], vh),
        )

    def in_copies(j, to, slot):
        return [
            pltpu.make_async_remote_copy(
                src, own_rows(dst, slot), si_sem.at[c, j], ri_sem.at[c, j],
                device_id={"seq": to}, device_id_type=MESH,
            )
            for c, (src, dst) in enumerate(pieces(to))
        ]

    def toward(j):
        return lax.rem(s - ring_delta(j) + ns, ns)

    def origin(j):
        return lax.rem(s + ring_delta(j) + ns, ns)

    @pl.loop(1, ns)
    def _(j):
        for c in in_copies(j, toward(j), s):
            c.start()

    w_part = depth // 2
    weights = Ring(
        nd, "dp",
        lambda sub: wall.at[d, pl.ds(sub * w_part, w_part)],
        lambda index, sub: wall.at[index, pl.ds(sub * w_part, w_part)],
        sw_sem, rw_sem,
    )
    first[2].wait()
    weights.start()

    @pl.loop(1, nd)
    def _(k):
        info_copy(lax.rem(d + k, nd), d).start()

    for c in later:
        c.start()
    local = [
        pltpu.make_async_copy(src, own_rows(dst, s), local_sem.at[c])
        for c, (src, dst) in enumerate(pieces(s))
    ]
    for c in local:
        c.start()
    for c in local:
        c.wait()

    def receive(j):
        frm = origin(j)
        for c in in_copies(j, frm, frm):
            c.wait_recv()

    @pl.loop(1, ns // 2)
    def _(j):
        receive(j)

    weights.advance(1)

    @pl.loop(ns // 2, ns)
    def _(j):
        receive(j)

    per_core = ns // CORES
    mate = s + 1 - 2 * core

    def owner(chip):
        return chip * CORES + s // per_core

    def out_copy(chip, head):
        return pltpu.make_async_remote_copy(
            att.at[pl.ds(pl.multiple_of(chip * chip_rows, 16), chip_rows)],
            mixed.at[:, cols(lax.rem(head, per_core))], so_sem.at[chip],
            ro_sem.at[lax.rem(head, per_core)],
            device_id={"seq": owner(chip)}, device_id_type=MESH,
        )

    scale = 1.0 / math.sqrt(HD)
    step_rows = 2 * chip_rows
    for i in range(length // step_rows):
        upto = (i + 1) * step_rows
        span = pl.ds(i * step_rows, step_rows)
        scores = lax.dot_general(
            qh[span, :], kh[0:upto, :], (((1,), (1,)), ((), ())), preferred_element_type=F32
        ) * scale
        at = lax.broadcasted_iota(jnp.int32, (step_rows, upto), 0) + i * step_rows
        key_at = lax.broadcasted_iota(jnp.int32, (step_rows, upto), 1)
        mine = jnp.concatenate([dcol[span, :]] * (upto // HD), axis=1)
        allowed = (key_at <= at) & (mine == docs[:, 0:upto])
        scores = jnp.where(allowed, scores, -1e30)
        lifted = jnp.exp(scores - jnp.max(scores, axis=-1, keepdims=True))
        probs = (lifted / jnp.sum(lifted, axis=-1, keepdims=True)).astype(BF16)
        att[span, :] = jnp.dot(probs, vh[0:upto, :], preferred_element_type=F32).astype(BF16)
        for chip in (2 * i, 2 * i + 1):

            @pl.when(owner(chip) != s)
            def _():
                out_copy(chip, s).start()

            @pl.when(owner(chip) == s)
            def _():
                mixed[:, cols(lax.rem(s, per_core))] = att[
                    pl.ds(chip * chip_rows, chip_rows), :
                ]

        if i == 1:
            weights.advance(2)

    slots = nd * CAP
    per_seq = nd // SPLIT
    first_expert = d // SPLIT

    @pl.loop(1, nd)
    def _(k):
        other = lax.rem(d + k, nd)
        info_copy(other, other).wait_send()
        info_copy(other, other).wait_recv()

    tiles = [routes[2 * m] + routes[2 * m + 1] for m in range(nd // 2)]
    code = jnp.concatenate([tile[:TOPK] for tile in tiles], axis=1)
    gates = jnp.concatenate([tile[TOPK:] for tile in tiles], axis=1)
    slot = lax.broadcasted_iota(jnp.int32, (slots, tokens), 0).astype(F32)
    token = lax.broadcasted_iota(jnp.int32, (slots, tokens), 1).astype(F32)
    slot_block = jnp.floor((slot + 0.5) * (1.0 / CAP))
    token_block = jnp.floor((token + 0.5) * (1.0 / rows))
    ranks = jnp.where(slot_block == token_block, slot - slot_block * CAP, -1e6)

    def seat(j):
        return pl.ds(pl.multiple_of(j * slots, 16), slots)

    @pl.loop(0, ns)
    def _(j):
        base = ((toward(j) * per_seq + first_expert) * CAP).astype(F32)
        hits = [code[k : k + 1, :] - base == ranks for k in range(TOPK)]
        hit = functools.reduce(jnp.logical_or, hits)
        picks[seat(j), :] = jnp.where(hit, 1.0, 0.0).astype(BF16)
        mixes[seat(j), :] = functools.reduce(
            jnp.add, [jnp.where(hits[k], gates[k : k + 1, :], 0.0) for k in range(TOPK)]
        ).astype(BF16)

    weights.advance(3)

    @pl.loop(0, per_core)
    def _(h):
        @pl.when(core * per_core + h != s)
        def _():
            out_copy(0, h).wait_recv()

    def sum_copy(index):
        at = pl.ds(pl.multiple_of(index * block, block), block)
        return pltpu.make_async_remote_copy(
            send_sum.at[:, at], got_sum.at[:, at], sp_sem.at[index], rp_sem.at[index],
            device_id={"seq": mate}, device_id_type=MESH,
        )

    def project(index):
        at = pl.ds(pl.multiple_of(index * block, block), block)
        theirs = mixed[pl.ds(pl.multiple_of((1 - core) * rows, 16), rows), :]
        mine = mixed[pl.ds(pl.multiple_of(core * rows, 16), rows), :]
        send_sum[:, at] = jnp.dot(theirs, wall[index], preferred_element_type=F32)
        own_sum[:, at] = jnp.dot(mine, wall[index], preferred_element_type=F32)
        sum_copy(index).start()

    project(d)
    for t in range(1, nd // 2 + 1):
        if t >= 4:
            weights.advance(t)
        for index in weights.arrived(t):
            project(index)

    @pl.loop(0, nd)
    def _(index):
        sum_copy(index).wait_recv()

    first[3].wait()
    projected = (own_sum[...] + got_sum[...]).astype(BF16)
    summed = (resid[...].astype(F32) + projected.astype(F32)).astype(BF16)
    residual[...] = summed
    stream = summed.astype(F32)
    scaled = (
        stream
        * lax.rsqrt(jnp.mean(stream * stream, axis=-1, keepdims=True) + norm_eps)
        * vecs_ref[0:1, :]
    ).astype(BF16)

    def place_of(chunk, side):
        return side * half + chunk * quarter

    mine_at = pl.ds(pl.multiple_of(d * rows, 16), rows)
    for chunk in range(2):
        for side in range(2):
            at = place_of(chunk, side)
            normed[chunk, side] = scaled[:, at : at + quarter]
            every[chunk, side, mine_at, :] = scaled[:, at : at + quarter]
    part = rows // 2

    def gather(chunk):
        return Ring(
            nd, "dp",
            lambda sub: normed.at[chunk, :, pl.ds(sub * part, part)],
            lambda index, sub: every.at[
                chunk, :, pl.ds(pl.multiple_of(index * rows + sub * part, 16), part)
            ],
            sg_sem.at[chunk], rg_sem.at[chunk],
        )

    rings = [gather(0), gather(1)]

    par = lax.rem(d, 2)
    partner = d + 1 - 2 * par
    group_slots = GROUP * slots
    groups = ns // GROUP

    def span_of(g):
        return pl.ds(pl.multiple_of(g * group_slots, 16), group_slots)

    def go_copy(chunk, j):
        return pltpu.make_async_remote_copy(
            send.at[chunk, seat(j)], own_in.at[chunk, seat(j)], sy_sem.at[chunk, j],
            ry_sem.at[chunk, j], device_id={"seq": toward(j)}, device_id_type=MESH,
        )

    def swap_copy(chunk, g):
        return pltpu.make_async_remote_copy(
            own_in.at[chunk, span_of(g)], pair_in.at[chunk, span_of(g)], sx_sem.at[chunk, g],
            rx_sem.at[chunk, g], device_id={"dp": partner}, device_id_type=MESH,
        )

    def part_copy(chunk, g):
        return pltpu.make_async_remote_copy(
            pair_out.at[chunk, span_of(g)], pair_part.at[chunk, span_of(g)], sq_sem.at[chunk, g],
            rq_sem.at[chunk, g], device_id={"dp": partner}, device_id_type=MESH,
        )

    def back_copy(chunk, j):
        return pltpu.make_async_remote_copy(
            back.at[chunk, seat(j)], ret.at[chunk, seat(j)], sr_sem.at[chunk, j],
            rr_sem.at[chunk, j], device_id={"seq": origin(j)}, device_id_type=MESH,
        )

    def columns(chunk, side):
        return pl.ds(pl.multiple_of(side * half + chunk * quarter, quarter), quarter)

    batch = ns // 4

    def pick(chunk, q):
        at = pl.ds(q * batch * slots, batch * slots)
        got = jnp.dot(
            picks[at, :], every[chunk, par], preferred_element_type=F32
        ).astype(BF16)
        send[chunk, at, :] = got
        if q == 0:
            own_in[chunk, 0:slots, :] = got[0:slots]

    def go(chunk, q):
        @pl.loop(max(1, q * batch), (q + 1) * batch)
        def _(j):
            go_copy(chunk, j).start()

    rings[0].start()
    rings[0].advance(1)
    rings[0].advance(2)
    rings[1].start()
    rings[0].advance(3)
    rings[0].advance(4)
    for q in range(4):
        pick(0, q)
        if q:
            go(0, q - 1)
        rings[1].advance(q + 1)
    go(0, 3)
    for q in range(4):
        pick(1, q)
        if q:
            go(1, q - 1)
    go(1, 3)
    for c in later:
        c.wait()

    def nt(a, w):
        return lax.dot_general(a, w, (((1,), (1,)), ((), ())), preferred_element_type=F32)

    def silu(a):
        return a / (1.0 + jnp.exp(-a))

    def arrive(chunk, g):
        for i in range(GROUP):
            j = g * GROUP + i

            @pl.when(j > 0)
            def _():
                go_copy(chunk, j).wait_recv()

        swap_copy(chunk, g).start()

    quads = [(chunk, side) for chunk in range(2) for side in range(2)]
    share = tokens // 4

    @pl.loop(0, groups)
    def _(g):
        arrive(0, g)

        @pl.when((g >= 1) & (g <= 4))
        def _():
            at = pl.ds(pl.multiple_of((g - 1) * share, share), share)
            gate_act = jnp.zeros((share, vg.shape[0]), F32)
            up_act = jnp.zeros((share, vg.shape[0]), F32)
            weight = jnp.zeros((share, 1), F32)
            for chunk, side in quads:
                a = every[chunk, side, at, :]
                where = pl.ds(place_of(chunk, side), quarter)
                gate_act += nt(a, vg[:, where])
                up_act += nt(a, vu[:, where])
                weight += jnp.sum(
                    a.astype(F32) * vecs_ref[1:2, where], axis=-1, keepdims=True
                )
            hidden = (silu(gate_act) * up_act).astype(BF16)
            weight = 1.0 / (1.0 + jnp.exp(-weight))
            for chunk, side in quads:
                total[chunk, side, at, :] = weight * jnp.dot(
                    hidden, vd[:, pl.ds(place_of(chunk, side), quarter)],
                    preferred_element_type=F32,
                )

    def down(chunk, g):
        hidden = act[span_of(g), :]
        pair_out[chunk, span_of(g), :] = jnp.dot(
            hidden, wd[:, columns(chunk, 1 - par)], preferred_element_type=F32
        ).astype(BF16)
        own_part[span_of(g), :] = jnp.dot(
            hidden, wd[:, columns(chunk, par)], preferred_element_type=F32
        )
        part_copy(chunk, g).start()

    def join(chunk, g):
        part_copy(chunk, g).wait_recv()
        back[chunk, span_of(g), :] = (
            own_part[span_of(g), :] + pair_part[chunk, span_of(g), :].astype(F32)
        ).astype(BF16)

    def leave(chunk, g):
        for i in range(GROUP):
            j = g * GROUP + i

            @pl.when(j > 0)
            def _():
                back_copy(chunk, j).start()

            @pl.when(j == 0)
            def _():
                ret[chunk, 0:slots, :] = back[chunk, 0:slots, :]

    def combine(chunk, g):
        for i in range(GROUP):
            j = g * GROUP + i

            @pl.when(j > 0)
            def _():
                back_copy(chunk, j).wait_recv()

        total[chunk, par] += lax.dot_general(
            mixes[span_of(g), :], ret[chunk, span_of(g), :], (((0,), (0,)), ((), ())),
            preferred_element_type=F32,
        )

    @pl.loop(0, groups + 2)
    def _(step):
        @pl.when(step < groups)
        def _():
            arrive(1, step)

        @pl.when(step >= 2)
        def _():
            join(0, step - 2)

        @pl.when((step >= 1) & (step <= groups))
        def _():
            g = step - 1
            gate_act = jnp.zeros((group_slots, wg.shape[0]), F32)
            up_act = jnp.zeros((group_slots, wg.shape[0]), F32)
            for chunk in range(2):
                swap_copy(chunk, g).wait_recv()
                for rows_in, side in ((own_in, par), (pair_in, 1 - par)):
                    a = rows_in[chunk, span_of(g), :]
                    gate_act += nt(a, wg[:, columns(chunk, side)])
                    up_act += nt(a, wu[:, columns(chunk, side)])
            act[span_of(g), :] = (silu(gate_act) * up_act).astype(BF16)
            down(0, g)

        @pl.when(step >= 2)
        def _():
            leave(0, step - 2)

    @pl.loop(0, groups)
    def _(g):
        down(1, g)

    @pl.loop(0, groups)
    def _(g):
        join(1, g)
        combine(0, g)
        leave(1, g)

    last = nd // 2

    def own(index, sub):
        return pl.ds(pl.multiple_of(index * rows + sub * part, 16), part)

    def used(way, t, sub):
        return t < last or (t == last and sub == way)

    def hop(chunk, way, t, sub):
        sign = 1 - 2 * way
        return pltpu.make_async_remote_copy(
            passed.at[chunk, way, t - 1, sub], landed.at[chunk, way, t - 1, sub],
            s2_sem.at[chunk, way, t - 1, sub], r2_sem.at[chunk, way, t - 1, sub],
            device_id={"dp": lax.rem(d + sign + nd, nd)}, device_id_type=MESH,
        )

    def target(way, t):
        return lax.rem(d + (1 - 2 * way) * t + nd, nd)

    def reduce_chunk(chunk):
        for t in range(last, 0, -1):
            for sub in range(2):
                for way in range(2):
                    if not used(way, t, sub):
                        continue
                    term = total[chunk, :, own(target(way, t), sub), :]
                    if used(way, t + 1, sub):
                        hop(chunk, way, t + 1, sub).wait_recv()
                        term = term + landed[chunk, way, t, sub].astype(F32)
                    passed[chunk, way, t - 1, sub] = term.astype(BF16)
                    hop(chunk, way, t, sub).start()

    def settle(chunk):
        for sub in range(2):
            for way in range(2):
                hop(chunk, way, 1, sub).wait_recv()
            at = pl.ds(sub * part, part)
            sums = (
                total[chunk, :, own(d, sub), :]
                + landed[chunk, 0, 0, sub].astype(F32)
                + landed[chunk, 1, 0, sub].astype(F32)
            )
            for side in range(2):
                where = pl.ds(place_of(chunk, side), quarter)
                out_ref[at, where] = residual[at, where].astype(F32) + sums[side]

    reduce_chunk(0)

    @pl.loop(0, groups)
    def _(g):
        combine(1, g)

    reduce_chunk(1)
    settle(0)
    settle(1)

    for chunk in range(2):
        for way in range(2):
            for sub in range(2):
                for t in range(1, last + 1):
                    if used(way, t, sub):
                        hop(chunk, way, t, sub).wait_send()
        rings[chunk].finish()

        @pl.loop(1, ns)
        def _(j):
            go_copy(chunk, j).wait_send()
            back_copy(chunk, j).wait_send()

        @pl.loop(0, groups)
        def _(g):
            swap_copy(chunk, g).wait_send()
            part_copy(chunk, g).wait_send()

    weights.finish()

    @pl.loop(1, ns)
    def _(j):
        for c in in_copies(j, toward(j), s):
            c.wait_send()

    @pl.loop(0, chips)
    def _(chip):
        @pl.when(owner(chip) != s)
        def _():
            out_copy(chip, s).wait_send()

    @pl.loop(0, nd)
    def _(index):
        sum_copy(index).wait_send()


def run_layer(docs, info, vecs, qk, v, resid, out_weight, expert_weights, shared_weights, ns, nd):
    rows, width = v.shape
    length = rows * ns
    tokens = rows * nd
    half = width // 2
    quarter = half // 2
    slots = ns * nd * CAP
    groups = ns // GROUP
    hidden = expert_weights[0].shape[1]
    shared_hidden = shared_weights[0].shape[0]
    dma = pltpu.SemaphoreType.DMA
    vmem = pl.BlockSpec(memory_space=pltpu.VMEM)
    anyspace = pl.BlockSpec(memory_space=pl.ANY)

    def buf(*shape):
        return pltpu.VMEM(shape, BF16)

    def wide(*shape):
        return pltpu.VMEM(shape, F32)

    ring = dma((2, nd // 2, 2))
    rings = dma((2, 2, nd // 2, 2))
    per_seat = dma((2, ns))
    per_group = dma((2, groups))
    return pl.pallas_call(
        functools.partial(layer_kernel, ns, nd),
        out_shape=jax.ShapeDtypeStruct((rows, width), F32),
        in_specs=[vmem] * 3 + [anyspace] * 10,
        out_specs=vmem,
        scratch_shapes=[buf(2, rows, width), buf(rows, width), buf(rows, width)]
        + [buf(hidden, width)] * 3
        + [buf(shared_hidden, width)] * 3
        + [wide(length, HD), wide(*info.shape), wide(nd, *info.shape)]
        + [buf(length, HD)] * 4
        + [
            buf(rows * CORES, width // CORES),
            buf(nd, width // CORES, out_weight.shape[1]),
            wide(rows, width), wide(rows, width), wide(rows, width),
            buf(rows, width),
            buf(2, 2, rows, quarter),
            buf(2, 2, tokens, quarter),
            buf(slots, tokens), buf(slots, tokens),
            buf(2, slots, quarter), buf(2, slots, quarter), buf(2, slots, quarter),
            buf(slots, hidden),
            buf(2, slots, quarter), buf(2, slots, quarter),
            wide(slots, quarter),
            buf(2, slots, quarter), buf(2, slots, quarter),
            wide(2, 2, tokens, quarter),
            buf(2, 2, nd // 2, 2, 2, rows // 2, quarter),
            buf(2, 2, nd // 2, 2, 2, rows // 2, quarter),
            dma((10,)), dma((3,)), dma((3, ns)), dma((3, ns)), dma((ns // CORES,)),
            dma((ns // CORES,)), dma((nd,)), dma((nd,)), dma((nd,)), dma((nd,)),
            ring, ring, rings, rings,
            per_seat, per_seat, per_group, per_group, per_group, per_group, per_seat, per_seat,
            rings, rings,
        ],
        compiler_params=pltpu.CompilerParams(
            collective_id=1, has_side_effects=True, vmem_limit_bytes=67043328
        ),
        cost_estimate=pl.CostEstimate(
            flops=12 * slots * half * hidden, bytes_accessed=8 * slots * half, transcendentals=0
        ),
        name="layer",
    )(docs, info, vecs, qk, v, resid, out_weight, *expert_weights, *shared_weights)


def body(
    resid,
    queries_keys,
    values,
    doc_ids,
    out_weight,
    norm_gain,
    expert_ids,
    gate_vals,
    expert_gate,
    expert_up,
    expert_down,
    shared_gate,
    shared_up,
    shared_down,
    shared_score,
):
    ns = lax.axis_size("seq")
    nd = lax.axis_size("dp")
    tokens = resid.shape[1]
    width = resid.shape[2]
    d = lax.axis_index("dp")
    info = jnp.concatenate([expert_ids[0].T.astype(F32), gate_vals[0].T], axis=0)
    blank = jnp.zeros_like(info)
    info = jnp.where(
        d % 2 == 0,
        jnp.concatenate([info, blank], axis=1),
        jnp.concatenate([blank, info], axis=1),
    )
    out = run_layer(
        doc_ids,
        info,
        jnp.stack([norm_gain, shared_score.astype(F32)]),
        queries_keys.reshape(2, tokens, width),
        values[0],
        resid[0],
        out_weight,
        (expert_gate.transpose(0, 2, 1), expert_up.transpose(0, 2, 1), expert_down),
        (shared_gate.T, shared_up.T, shared_down),
        ns,
        nd,
    )
    return out.astype(BF16)[None]


def solution(mesh):
    placed = (
        P(("groups", "dp"), "seq", None),
        P(None, ("groups", "dp"), "seq", None),
        P(("groups", "dp"), "seq", None),
        P(("groups", "dp"), None),
        P(None, "dp"),
        P(),
        P(("groups", "dp"), "seq", None),
        P(("groups", "dp"), "seq", None),
        P(("seq", "dp"), None, None),
        P(("seq", "dp"), None, None),
        P(("seq", "dp"), None, None),
        P(None, "dp"),
        P(None, "dp"),
        P("dp", None),
        P(),
    )
    return jax.shard_map(
        body,
        mesh=mesh,
        in_specs=placed,
        out_specs=P(("groups", "dp"), "seq", None),
        check_vma=False,
    )
```

```python
import functools
import math

import jax
import jax.numpy as jnp
from jax import lax
from jax.experimental import pallas as pl
from jax.experimental.pallas import tpu as pltpu
from jax.sharding import PartitionSpec as P

HD = 128
TOPK = 4
SPLIT = 4
CAP = 10
GROUP = 2
CORES = 2
DIRECT = 1

norm_eps = 1e-06
MESH = pl.DeviceIdType.MESH
F32 = jnp.float32
BF16 = jnp.bfloat16


def ring_delta(j):
    return ((j + 1) // 2) * (2 * (j % 2) - 1)


class Ring:
    def __init__(self, nd, axis, source, place, send_sem, recv_sem):
        self.nd, self.axis, self.last = nd, axis, nd // 2
        self.source, self.place = source, place
        self.send_sem, self.recv_sem = send_sem, recv_sem
        self.me = lax.axis_index(axis)

    def behind(self, t, way):
        return lax.rem(self.me - (1 - 2 * way) * t + self.nd, self.nd)

    def hop(self, way, t, sub):
        index = self.behind(t - 1, way)
        src = self.source(sub) if t == 1 else self.place(index, sub)
        return pltpu.make_async_remote_copy(
            src, self.place(index, sub), self.send_sem.at[way, t - 1, sub],
            self.recv_sem.at[way, t - 1, sub],
            device_id={self.axis: self.behind(-1, way)}, device_id_type=MESH,
        )

    def hops(self, t):
        return [
            (way, t, sub)
            for sub in range(2)
            for way in range(2)
            if t < self.last or (t == self.last and sub == way)
        ]

    def start(self):
        for h in self.hops(1):
            self.hop(*h).start()

    def advance(self, t):
        following = self.hops(t + 1)
        for way, _, sub in self.hops(t):
            self.hop(way, t, sub).wait_recv()
            if (way, t + 1, sub) in following:
                self.hop(way, t + 1, sub).start()

    def arrived(self, t):
        return [self.behind(t, 0), self.behind(t, 1)] if t < self.last else [self.behind(t, 0)]

    def finish(self):
        for t in range(1, self.last + 1):
            for h in self.hops(t):
                self.hop(*h).wait_send()


def greet(axes):
    barrier = pltpu.get_barrier_semaphore()
    for axis, size in axes.items():
        me = lax.axis_index(axis)

        @pl.loop(1, size)
        def _(k):
            pl.semaphore_signal(
                barrier, inc=1, device_id={axis: lax.rem(me + k, size)}, device_id_type=MESH
            )

    pl.semaphore_wait(barrier, sum(axes.values()) - len(axes))


def layer_kernel(
    ns, nd, docs_ref, ids_ref, gates_ref, gain_ref, score_ref, qk_hbm, v_hbm, resid_hbm, w_hbm, eg_hbm, eu_hbm, ed_hbm,
    sg_hbm, su_hbm, sd_hbm, out_ref,
    qk, v, resid, wg, wu, wd, vg, vu, vd, vecs, dcol, spread, info, routes, qh, kh, vh, att, mixed, wall, own_sum,
    send_sum, got_sum, residual, normed, every, picks, mixes, send, own_in, pair_in, act, pair_out,
    pair_part, own_part, back, ret, send_pair, ret_pair, total, landed, passed,
    w_sem, local_sem, si_sem, ri_sem, so_sem, ro_sem, sd_sem, rd_sem, sp_sem, rp_sem, sw_sem, rw_sem,
    sg_sem, rg_sem, sy_sem, ry_sem, sx_sem, rx_sem, sq_sem, rq_sem, sr_sem, rr_sem, sf_sem, rf_sem, sb_sem, rb_sem,
    s2_sem, r2_sem,
):
    s = lax.axis_index("seq")
    d = lax.axis_index("dp")
    rows, width = v.shape
    length = rows * ns
    tokens = rows * nd
    core = lax.rem(s, CORES)
    chips = ns // CORES
    depth = width // CORES
    block = width // nd
    chip_rows = rows * CORES
    half = width // 2
    quarter = half // 2
    lanes = 2 * rows

    first = [
        pltpu.make_async_copy(src, dst, w_sem.at[i])
        for i, (src, dst) in enumerate(
            (
                (qk_hbm, qk), (v_hbm, v),
                (w_hbm.at[pl.ds(pl.multiple_of(core * depth, 16), depth)], wall.at[d]),
                (resid_hbm, resid),
            )
        )
    ]
    later = [
        pltpu.make_async_copy(src, dst, w_sem.at[4 + i])
        for i, (src, dst) in enumerate(
            (
                (sg_hbm, vg), (su_hbm, vu), (sd_hbm, vd),
                (eg_hbm.at[0], wg), (eu_hbm.at[0], wu), (ed_hbm.at[0], wd),
            )
        )
    ]
    for c in first:
        c.start()

    experts = ns * nd // SPLIT
    lane = lax.broadcasted_iota(jnp.int32, (1, lanes), 1)
    valid = (lane >= lax.rem(d, 2) * rows) & (lane < (lax.rem(d, 2) + 1) * rows)
    expert = lax.broadcasted_iota(jnp.int32, (experts, lanes), 0).astype(F32)
    spread[...] = jnp.zeros_like(spread)
    spread[0:TOPK, 0:rows] = ids_ref[...].astype(F32)
    spread[TOPK:, 0:rows] = gates_ref[...]
    odd = lax.rem(d, 2).astype(F32)
    both = spread[...] * (1.0 - odd) + pltpu.roll(spread[...], rows, 1) * odd
    chosen_ids = [jnp.where(valid, both[k : k + 1, :], -1.0) for k in range(TOPK)]
    named = [ids == expert for ids in chosen_ids]
    earlier = lax.broadcasted_iota(jnp.int32, (lanes, lanes), 0) < lax.broadcasted_iota(
        jnp.int32, (lanes, lanes), 1
    )
    counts = jnp.dot(
        jnp.where(functools.reduce(jnp.logical_or, named), 1.0, 0.0).astype(BF16),
        jnp.where(earlier, 1.0, 0.0).astype(BF16),
        preferred_element_type=F32,
    )
    for k in range(TOPK):
        rank = jnp.sum(jnp.where(named[k], counts, 0.0), axis=0, keepdims=True)
        info[k : k + 1, :] = jnp.where(valid, chosen_ids[k] * CAP + rank, 0.0)
    info[TOPK:, :] = both[TOPK:, :]
    score = score_ref[...].astype(F32)
    for i in range(width // HD):
        vecs[0:1, i * HD : (i + 1) * HD] = gain_ref[i : i + 1, :]
        vecs[1:2, i * HD : (i + 1) * HD] = score[i : i + 1, :]
    routes[d] = info[...]
    docs = docs_ref[...].astype(F32)
    for i in range(length // HD):
        tile = jnp.broadcast_to(docs[:, i * HD : (i + 1) * HD], (HD, HD))
        dcol[i * HD : (i + 1) * HD, :] = tile.T

    greet({"seq": ns, "dp": nd})
    first[0].wait()
    first[1].wait()

    def own_rows(ref, t):
        return ref.at[pl.ds(pl.multiple_of(t * rows, 16), rows)]

    def cols(t):
        return pl.ds(pl.multiple_of(t * HD, HD), HD)

    def info_copy(to, slot):
        return pltpu.make_async_remote_copy(
            info, routes.at[slot], sd_sem.at[to], rd_sem.at[slot],
            device_id={"dp": to}, device_id_type=MESH,
        )

    def pieces(t):
        return (
            (qk.at[0, :, cols(t)], qh),
            (qk.at[1, :, cols(t)], kh),
            (v.at[:, cols(t)], vh),
        )

    def in_copies(j, to, slot):
        return [
            pltpu.make_async_remote_copy(
                src, own_rows(dst, slot), si_sem.at[c, j], ri_sem.at[c, j],
                device_id={"seq": to}, device_id_type=MESH,
            )
            for c, (src, dst) in enumerate(pieces(to))
        ]

    def peer(j, sign):
        chip = lax.rem(s // CORES + sign * ring_delta(j // CORES) + chips, chips)
        return chip * CORES + lax.rem(core + j, CORES)

    def toward(j):
        return peer(j, -1)

    def origin(j):
        return peer(j, 1)

    @pl.loop(1, ns)
    def _(j):
        for c in in_copies(j, toward(j), s):
            c.start()

    w_part = depth // 2
    weights = Ring(
        nd, "dp",
        lambda sub: wall.at[d, pl.ds(sub * w_part, w_part)],
        lambda index, sub: wall.at[index, pl.ds(sub * w_part, w_part)],
        sw_sem, rw_sem,
    )
    first[2].wait()
    weights.start()

    @pl.loop(1, nd)
    def _(k):
        info_copy(lax.rem(d + k, nd), d).start()

    for c in later:
        c.start()
    local = [
        pltpu.make_async_copy(src, own_rows(dst, s), local_sem.at[c])
        for c, (src, dst) in enumerate(pieces(s))
    ]
    for c in local:
        c.start()
    for c in local:
        c.wait()

    def receive(j):
        frm = origin(j)
        for c in in_copies(j, frm, frm):
            c.wait_recv()

    @pl.loop(1, ns // 2)
    def _(j):
        receive(j)

    weights.advance(1)

    @pl.loop(ns // 2, ns)
    def _(j):
        receive(j)

    per_core = ns // CORES
    mate = s + 1 - 2 * core

    def owner(chip):
        return chip * CORES + s // per_core

    def out_copy(chip, head):
        return pltpu.make_async_remote_copy(
            att.at[pl.ds(pl.multiple_of(chip * chip_rows, 16), chip_rows)],
            mixed.at[:, cols(lax.rem(head, per_core))], so_sem.at[chip],
            ro_sem.at[lax.rem(head, per_core)],
            device_id={"seq": owner(chip)}, device_id_type=MESH,
        )

    scale = 1.0 / math.sqrt(HD)
    step_rows = 2 * chip_rows
    for i in range(length // step_rows):
        upto = (i + 1) * step_rows
        span = pl.ds(i * step_rows, step_rows)
        scores = lax.dot_general(
            qh[span, :], kh[0:upto, :], (((1,), (1,)), ((), ())), preferred_element_type=F32
        ) * scale
        at = lax.broadcasted_iota(jnp.int32, (step_rows, upto), 0) + i * step_rows
        key_at = lax.broadcasted_iota(jnp.int32, (step_rows, upto), 1)
        mine = jnp.concatenate([dcol[span, :]] * (upto // HD), axis=1)
        allowed = (key_at <= at) & (mine == docs[:, 0:upto])
        scores = jnp.where(allowed, scores, -1e30)
        lifted = jnp.exp(scores - jnp.max(scores, axis=-1, keepdims=True))
        probs = (lifted / jnp.sum(lifted, axis=-1, keepdims=True)).astype(BF16)
        att[span, :] = jnp.dot(probs, vh[0:upto, :], preferred_element_type=F32).astype(BF16)
        for chip in (2 * i, 2 * i + 1):

            @pl.when(owner(chip) != s)
            def _():
                out_copy(chip, s).start()

            @pl.when(owner(chip) == s)
            def _():
                mixed[:, cols(lax.rem(s, per_core))] = att[
                    pl.ds(chip * chip_rows, chip_rows), :
                ]

        if i == 1:
            weights.advance(2)

    slots = nd * CAP
    per_seq = nd // SPLIT
    first_expert = d // SPLIT

    @pl.loop(1, nd)
    def _(k):
        other = lax.rem(d + k, nd)
        info_copy(other, other).wait_send()
        info_copy(other, other).wait_recv()

    tiles = [routes[2 * m] + routes[2 * m + 1] for m in range(nd // 2)]
    code = jnp.concatenate([tile[:TOPK] for tile in tiles], axis=1)
    gates = jnp.concatenate([tile[TOPK:] for tile in tiles], axis=1)
    slot = lax.broadcasted_iota(jnp.int32, (slots, tokens), 0).astype(F32)
    token = lax.broadcasted_iota(jnp.int32, (slots, tokens), 1).astype(F32)
    slot_block = jnp.floor((slot + 0.5) * (1.0 / CAP))
    token_block = jnp.floor((token + 0.5) * (1.0 / rows))
    ranks = jnp.where(slot_block == token_block, slot - slot_block * CAP, -1e6)

    def seat(j):
        return pl.ds(pl.multiple_of(j * slots, 16), slots)

    @pl.loop(0, ns)
    def _(j):
        base = ((toward(j) * per_seq + first_expert) * CAP).astype(F32)
        hits = [code[k : k + 1, :] - base == ranks for k in range(TOPK)]
        hit = functools.reduce(jnp.logical_or, hits)
        picks[seat(j), :] = jnp.where(hit, 1.0, 0.0).astype(BF16)
        mixes[seat(j), :] = functools.reduce(
            jnp.add, [jnp.where(hits[k], gates[k : k + 1, :], 0.0) for k in range(TOPK)]
        ).astype(BF16)

    weights.advance(3)

    @pl.loop(0, per_core)
    def _(h):
        @pl.when(core * per_core + h != s)
        def _():
            out_copy(0, h).wait_recv()

    def sum_copy(index):
        at = pl.ds(pl.multiple_of(index * block, block), block)
        return pltpu.make_async_remote_copy(
            send_sum.at[:, at], got_sum.at[:, at], sp_sem.at[index], rp_sem.at[index],
            device_id={"seq": mate}, device_id_type=MESH,
        )

    def project(index):
        at = pl.ds(pl.multiple_of(index * block, block), block)
        theirs = mixed[pl.ds(pl.multiple_of((1 - core) * rows, 16), rows), :]
        mine = mixed[pl.ds(pl.multiple_of(core * rows, 16), rows), :]
        send_sum[:, at] = jnp.dot(theirs, wall[index], preferred_element_type=F32)
        own_sum[:, at] = jnp.dot(mine, wall[index], preferred_element_type=F32)
        sum_copy(index).start()

    project(d)
    for t in range(1, nd // 2 + 1):
        if t >= 4:
            weights.advance(t)
        for index in weights.arrived(t):
            project(index)

    @pl.loop(0, nd)
    def _(index):
        sum_copy(index).wait_recv()

    first[3].wait()
    projected = (own_sum[...] + got_sum[...]).astype(BF16)
    summed = (resid[...].astype(F32) + projected.astype(F32)).astype(BF16)
    residual[...] = summed
    stream = summed.astype(F32)
    scaled = (
        stream
        * lax.rsqrt(jnp.mean(stream * stream, axis=-1, keepdims=True) + norm_eps)
        * vecs[0:1, :]
    ).astype(BF16)

    def place_of(chunk, side):
        return side * half + chunk * quarter

    mine_at = pl.ds(pl.multiple_of(d * rows, 16), rows)
    for chunk in range(2):
        for side in range(2):
            at = place_of(chunk, side)
            normed[chunk, side] = scaled[:, at : at + quarter]
            every[chunk, side, mine_at, :] = scaled[:, at : at + quarter]
    part = rows // 2

    def gather(chunk):
        return Ring(
            nd, "dp",
            lambda sub: normed.at[chunk, :, pl.ds(sub * part, part)],
            lambda index, sub: every.at[
                chunk, :, pl.ds(pl.multiple_of(index * rows + sub * part, 16), part)
            ],
            sg_sem.at[chunk], rg_sem.at[chunk],
        )

    rings = [gather(0), gather(1)]

    par = lax.rem(d, 2)
    partner = d + 1 - 2 * par
    group_slots = GROUP * slots
    groups = ns // GROUP

    def span_of(g):
        return pl.ds(pl.multiple_of(g * group_slots, 16), group_slots)

    def go_copy(chunk, j):
        return pltpu.make_async_remote_copy(
            send.at[chunk, seat(j)], own_in.at[chunk, seat(j)], sy_sem.at[chunk, j],
            ry_sem.at[chunk, j], device_id={"seq": toward(j)}, device_id_type=MESH,
        )

    def swap_copy(chunk, g):
        return pltpu.make_async_remote_copy(
            own_in.at[chunk, span_of(g)], pair_in.at[chunk, span_of(g)], sx_sem.at[chunk, g],
            rx_sem.at[chunk, g], device_id={"dp": partner}, device_id_type=MESH,
        )

    def part_copy(chunk, g):
        return pltpu.make_async_remote_copy(
            pair_out.at[chunk, span_of(g)], pair_part.at[chunk, span_of(g)], sq_sem.at[chunk, g],
            rq_sem.at[chunk, g], device_id={"dp": partner}, device_id_type=MESH,
        )

    def back_copy(chunk, j):
        return pltpu.make_async_remote_copy(
            back.at[chunk, seat(j)], ret.at[chunk, seat(j)], sr_sem.at[chunk, j],
            rr_sem.at[chunk, j], device_id={"seq": origin(j)}, device_id_type=MESH,
        )

    def go_pair(chunk, j):
        return pltpu.make_async_remote_copy(
            send_pair.at[chunk, seat(j)], pair_in.at[chunk, seat(j)], sf_sem.at[chunk, j],
            rf_sem.at[chunk, j], device_id={"seq": toward(j)}, device_id_type=MESH,
        )

    def back_pair(chunk, j):
        return pltpu.make_async_remote_copy(
            pair_out.at[chunk, seat(j)], ret_pair.at[chunk, seat(j)], sb_sem.at[chunk, j],
            rb_sem.at[chunk, j], device_id={"seq": origin(j)}, device_id_type=MESH,
        )

    near_seats = DIRECT * GROUP

    def columns(chunk, side):
        return pl.ds(pl.multiple_of(side * half + chunk * quarter, quarter), quarter)

    batch = ns // 4

    def pick(chunk, q):
        at = pl.ds(q * batch * slots, batch * slots)
        got = jnp.dot(
            picks[at, :], every[chunk, par], preferred_element_type=F32
        ).astype(BF16)
        send[chunk, at, :] = got
        if q == 0:
            own_in[chunk, 0:slots, :] = got[0:slots]
            near = pl.ds(0, near_seats * slots)
            got = jnp.dot(
                picks[near, :], every[chunk, 1 - par], preferred_element_type=F32
            ).astype(BF16)
            send_pair[chunk, near, :] = got
            pair_in[chunk, 0:slots, :] = got[0:slots]

    def go(chunk, q):
        @pl.loop(max(1, q * batch), (q + 1) * batch)
        def _(j):
            go_copy(chunk, j).start()

        if q == 0:

            @pl.loop(1, near_seats)
            def _(j):
                go_pair(chunk, j).start()

    rings[0].start()
    rings[0].advance(1)
    rings[0].advance(2)
    rings[1].start()
    rings[0].advance(3)
    rings[0].advance(4)
    for q in range(4):
        pick(0, q)
        if q:
            go(0, q - 1)
    go(0, 3)
    for t in range(1, nd // 2 + 1):
        rings[1].advance(t)
    for q in range(4):
        pick(1, q)
        if q:
            go(1, q - 1)
    go(1, 3)
    for c in later:
        c.wait()

    def nt(a, w):
        return lax.dot_general(a, w, (((1,), (1,)), ((), ())), preferred_element_type=F32)

    def silu(a):
        return a / (1.0 + jnp.exp(-a))

    def arrive(chunk, g):
        for i in range(GROUP):
            j = g * GROUP + i

            @pl.when(j > 0)
            def _():
                go_copy(chunk, j).wait_recv()

            @pl.when((j > 0) & (g < DIRECT))
            def _():
                go_pair(chunk, j).wait_recv()

        @pl.when(g >= DIRECT)
        def _():
            swap_copy(chunk, g).start()

    quads = [(chunk, side) for chunk in range(2) for side in range(2)]
    share = tokens // 4

    @pl.loop(0, groups)
    def _(g):
        arrive(0, g)

        @pl.when((g >= 1) & (g <= 4))
        def _():
            at = pl.ds(pl.multiple_of((g - 1) * share, share), share)
            gate_act = jnp.zeros((share, vg.shape[0]), F32)
            up_act = jnp.zeros((share, vg.shape[0]), F32)
            weight = jnp.zeros((share, 1), F32)
            for chunk, side in quads:
                a = every[chunk, side, at, :]
                where = pl.ds(place_of(chunk, side), quarter)
                gate_act += nt(a, vg[:, where])
                up_act += nt(a, vu[:, where])
                weight += jnp.sum(
                    a.astype(F32) * vecs[1:2, where], axis=-1, keepdims=True
                )
            hidden = (silu(gate_act) * up_act).astype(BF16)
            weight = 1.0 / (1.0 + jnp.exp(-weight))
            for chunk, side in quads:
                total[chunk, side, at, :] = weight * jnp.dot(
                    hidden, vd[:, pl.ds(place_of(chunk, side), quarter)],
                    preferred_element_type=F32,
                )

    def down(chunk, g):
        hidden = act[span_of(g), :]
        pair_out[chunk, span_of(g), :] = jnp.dot(
            hidden, wd[:, columns(chunk, 1 - par)], preferred_element_type=F32
        ).astype(BF16)
        own_part[span_of(g), :] = jnp.dot(
            hidden, wd[:, columns(chunk, par)], preferred_element_type=F32
        )

        @pl.when(g >= DIRECT)
        def _():
            part_copy(chunk, g).start()

    def join(chunk, g):
        @pl.when(g >= DIRECT)
        def _():
            part_copy(chunk, g).wait_recv()
            back[chunk, span_of(g), :] = (
                own_part[span_of(g), :] + pair_part[chunk, span_of(g), :].astype(F32)
            ).astype(BF16)

        @pl.when(g < DIRECT)
        def _():
            back[chunk, span_of(g), :] = own_part[span_of(g), :].astype(BF16)

    def leave(chunk, g):
        for i in range(GROUP):
            j = g * GROUP + i

            @pl.when(j > 0)
            def _():
                back_copy(chunk, j).start()

            @pl.when((j > 0) & (g < DIRECT))
            def _():
                back_pair(chunk, j).start()

            @pl.when(j == 0)
            def _():
                ret[chunk, 0:slots, :] = back[chunk, 0:slots, :]
                ret_pair[chunk, 0:slots, :] = pair_out[chunk, 0:slots, :]

    def combine(chunk, g):
        for i in range(GROUP):
            j = g * GROUP + i

            @pl.when(j > 0)
            def _():
                back_copy(chunk, j).wait_recv()

            @pl.when((j > 0) & (g < DIRECT))
            def _():
                back_pair(chunk, j).wait_recv()

        def mix(rows_in):
            return lax.dot_general(
                mixes[span_of(g), :], rows_in[chunk, span_of(g), :], (((0,), (0,)), ((), ())),
                preferred_element_type=F32,
            )

        total[chunk, par] += mix(ret)

        @pl.when(g < DIRECT)
        def _():
            total[chunk, 1 - par] += mix(ret_pair)

    @pl.loop(0, groups + 2)
    def _(step):
        @pl.when(step < groups)
        def _():
            arrive(1, step)

        @pl.when(step >= 2)
        def _():
            join(0, step - 2)

        @pl.when((step >= 1) & (step <= groups))
        def _():
            g = step - 1
            gate_act = jnp.zeros((group_slots, wg.shape[0]), F32)
            up_act = jnp.zeros((group_slots, wg.shape[0]), F32)
            for chunk in range(2):
                @pl.when(g >= DIRECT)
                def _():
                    swap_copy(chunk, g).wait_recv()

                for rows_in, side in ((own_in, par), (pair_in, 1 - par)):
                    a = rows_in[chunk, span_of(g), :]
                    gate_act += nt(a, wg[:, columns(chunk, side)])
                    up_act += nt(a, wu[:, columns(chunk, side)])
            act[span_of(g), :] = (silu(gate_act) * up_act).astype(BF16)
            down(0, g)

        @pl.when(step >= 2)
        def _():
            leave(0, step - 2)

    @pl.loop(0, groups)
    def _(g):
        down(1, g)

    @pl.loop(0, groups)
    def _(g):
        combine(0, g)

    last = nd // 2

    def own(index, sub):
        return pl.ds(pl.multiple_of(index * rows + sub * part, 16), part)

    def used(way, t, sub):
        return t < last or (t == last and sub == way)

    def hop(chunk, way, t, sub):
        sign = 1 - 2 * way
        return pltpu.make_async_remote_copy(
            passed.at[chunk, way, t - 1, sub], landed.at[chunk, way, t - 1, sub],
            s2_sem.at[chunk, way, t - 1, sub], r2_sem.at[chunk, way, t - 1, sub],
            device_id={"dp": lax.rem(d + sign + nd, nd)}, device_id_type=MESH,
        )

    def target(way, t):
        return lax.rem(d + (1 - 2 * way) * t + nd, nd)

    def reduce_step(chunk, t):
        for sub in range(2):
            for way in range(2):
                if not used(way, t, sub):
                    continue
                term = total[chunk, :, own(target(way, t), sub), :]
                if used(way, t + 1, sub):
                    hop(chunk, way, t + 1, sub).wait_recv()
                    term = term + landed[chunk, way, t, sub].astype(F32)
                passed[chunk, way, t - 1, sub] = term.astype(BF16)
                hop(chunk, way, t, sub).start()

    def settle(chunk):
        for sub in range(2):
            for way in range(2):
                hop(chunk, way, 1, sub).wait_recv()
            at = pl.ds(sub * part, part)
            sums = (
                total[chunk, :, own(d, sub), :]
                + landed[chunk, 0, 0, sub].astype(F32)
                + landed[chunk, 1, 0, sub].astype(F32)
            )
            for side in range(2):
                where = pl.ds(place_of(chunk, side), quarter)
                out_ref[at, where] = residual[at, where].astype(F32) + sums[side]

    for t in range(last, 0, -1):
        reduce_step(0, t)

        @pl.loop((last - t) * groups // last, (last - t + 1) * groups // last)
        def _(g):
            join(1, g)
            leave(1, g)

    @pl.loop(0, groups)
    def _(g):
        combine(1, g)

    for t in range(last, 0, -1):
        reduce_step(1, t)
    settle(0)
    settle(1)

    for chunk in range(2):
        for way in range(2):
            for sub in range(2):
                for t in range(1, last + 1):
                    if used(way, t, sub):
                        hop(chunk, way, t, sub).wait_send()
        rings[chunk].finish()

        @pl.loop(1, ns)
        def _(j):
            go_copy(chunk, j).wait_send()
            back_copy(chunk, j).wait_send()

        @pl.loop(1, near_seats)
        def _(j):
            go_pair(chunk, j).wait_send()
            back_pair(chunk, j).wait_send()

        @pl.loop(DIRECT, groups)
        def _(g):
            swap_copy(chunk, g).wait_send()
            part_copy(chunk, g).wait_send()

    weights.finish()

    @pl.loop(1, ns)
    def _(j):
        for c in in_copies(j, toward(j), s):
            c.wait_send()

    @pl.loop(0, chips)
    def _(chip):
        @pl.when(owner(chip) != s)
        def _():
            out_copy(chip, s).wait_send()

    @pl.loop(0, nd)
    def _(index):
        sum_copy(index).wait_send()


def run_layer(docs, ids, gates, gain, score, qk, v, resid, out_weight, expert_weights, shared_weights, ns, nd):
    rows, width = v.shape
    length = rows * ns
    tokens = rows * nd
    half = width // 2
    quarter = half // 2
    slots = ns * nd * CAP
    groups = ns // GROUP
    near = DIRECT * GROUP * nd * CAP
    hidden = expert_weights[0].shape[1]
    shared_hidden = shared_weights[0].shape[0]
    dma = pltpu.SemaphoreType.DMA
    vmem = pl.BlockSpec(memory_space=pltpu.VMEM)
    anyspace = pl.BlockSpec(memory_space=pl.ANY)

    def buf(*shape):
        return pltpu.VMEM(shape, BF16)

    def wide(*shape):
        return pltpu.VMEM(shape, F32)

    ring = dma((2, nd // 2, 2))
    rings = dma((2, 2, nd // 2, 2))
    per_seat = dma((2, ns))
    per_group = dma((2, groups))
    per_near = dma((2, DIRECT * GROUP))
    return pl.pallas_call(
        functools.partial(layer_kernel, ns, nd),
        out_shape=jax.ShapeDtypeStruct((rows, width), F32),
        in_specs=[vmem] * 5 + [anyspace] * 10,
        out_specs=vmem,
        scratch_shapes=[buf(2, rows, width), buf(rows, width), buf(rows, width)]
        + [buf(hidden, width)] * 3
        + [buf(shared_hidden, width)] * 3
        + [wide(2, width), wide(length, HD)]
        + [wide(2 * TOPK, 2 * rows), wide(2 * TOPK, 2 * rows), wide(nd, 2 * TOPK, 2 * rows)]
        + [buf(length, HD)] * 4
        + [
            buf(rows * CORES, width // CORES),
            buf(nd, width // CORES, out_weight.shape[1]),
            wide(rows, width), wide(rows, width), wide(rows, width),
            buf(rows, width),
            buf(2, 2, rows, quarter),
            buf(2, 2, tokens, quarter),
            buf(slots, tokens), buf(slots, tokens),
            buf(2, slots, quarter), buf(2, slots, quarter), buf(2, slots, quarter),
            buf(slots, hidden),
            buf(2, slots, quarter), buf(2, slots, quarter),
            wide(slots, quarter),
            buf(2, slots, quarter), buf(2, slots, quarter),
            buf(2, near, quarter), buf(2, near, quarter),
            wide(2, 2, tokens, quarter),
            buf(2, 2, nd // 2, 2, 2, rows // 2, quarter),
            buf(2, 2, nd // 2, 2, 2, rows // 2, quarter),
            dma((10,)), dma((3,)), dma((3, ns)), dma((3, ns)), dma((ns // CORES,)),
            dma((ns // CORES,)), dma((nd,)), dma((nd,)), dma((nd,)), dma((nd,)),
            ring, ring, rings, rings,
            per_seat, per_seat, per_group, per_group, per_group, per_group, per_seat, per_seat,
            per_near, per_near, per_near, per_near, rings, rings,
        ],
        compiler_params=pltpu.CompilerParams(
            collective_id=1, has_side_effects=True, vmem_limit_bytes=67043328
        ),
        cost_estimate=pl.CostEstimate(
            flops=12 * slots * half * hidden, bytes_accessed=8 * slots * half, transcendentals=0
        ),
        name="layer",
    )(docs, ids, gates, gain, score, qk, v, resid, out_weight, *expert_weights, *shared_weights)


def body(
    resid,
    queries_keys,
    values,
    doc_ids,
    out_weight,
    norm_gain,
    expert_ids,
    gate_vals,
    expert_gate,
    expert_up,
    expert_down,
    shared_gate,
    shared_up,
    shared_down,
    shared_score,
):
    ns = lax.axis_size("seq")
    nd = lax.axis_size("dp")
    tokens = resid.shape[1]
    width = resid.shape[2]
    out = run_layer(
        doc_ids,
        expert_ids[0].T,
        gate_vals[0].T,
        norm_gain.reshape(-1, HD),
        shared_score.reshape(-1, HD),
        queries_keys.reshape(2, tokens, width),
        values[0],
        resid[0],
        out_weight,
        (expert_gate.transpose(0, 2, 1), expert_up.transpose(0, 2, 1), expert_down),
        (shared_gate.T, shared_up.T, shared_down),
        ns,
        nd,
    )
    return out.astype(BF16)[None]


def solution(mesh):
    placed = (
        P(("groups", "dp"), "seq", None),
        P(None, ("groups", "dp"), "seq", None),
        P(("groups", "dp"), "seq", None),
        P(("groups", "dp"), None),
        P(None, "dp"),
        P(),
        P(("groups", "dp"), "seq", None),
        P(("groups", "dp"), "seq", None),
        P(("seq", "dp"), None, None),
        P(("seq", "dp"), None, None),
        P(("seq", "dp"), None, None),
        P(None, "dp"),
        P(None, "dp"),
        P("dp", None),
        P(),
    )
    return jax.shard_map(
        body,
        mesh=mesh,
        in_specs=placed,
        out_specs=P(("groups", "dp"), "seq", None),
        check_vma=False,
    )
```

```python
import functools
import math

import jax
import jax.numpy as jnp
from jax import lax
from jax.experimental import pallas as pl
from jax.experimental.pallas import tpu as pltpu
from jax.sharding import PartitionSpec as P

HD = 128
TOPK = 4
SPLIT = 4
CAP = 10
GROUP = 2
CORES = 2
DIRECT = 1

norm_eps = 1e-06
MESH = pl.DeviceIdType.MESH
F32 = jnp.float32
BF16 = jnp.bfloat16


def ring_delta(j):
    return ((j + 1) // 2) * (2 * (j % 2) - 1)


class Ring:
    def __init__(self, nd, axis, source, place, send_sem, recv_sem):
        self.nd, self.axis, self.last = nd, axis, nd // 2
        self.source, self.place = source, place
        self.send_sem, self.recv_sem = send_sem, recv_sem
        self.me = lax.axis_index(axis)

    def behind(self, t, way):
        return lax.rem(self.me - (1 - 2 * way) * t + self.nd, self.nd)

    def hop(self, way, t, sub):
        index = self.behind(t - 1, way)
        src = self.source(sub) if t == 1 else self.place(index, sub)
        return pltpu.make_async_remote_copy(
            src, self.place(index, sub), self.send_sem.at[way, t - 1, sub],
            self.recv_sem.at[way, t - 1, sub],
            device_id={self.axis: self.behind(-1, way)}, device_id_type=MESH,
        )

    def hops(self, t):
        return [
            (way, t, sub)
            for sub in range(2)
            for way in range(2)
            if t < self.last or (t == self.last and sub == way)
        ]

    def start(self):
        for h in self.hops(1):
            self.hop(*h).start()

    def advance(self, t):
        following = self.hops(t + 1)
        for way, _, sub in self.hops(t):
            self.hop(way, t, sub).wait_recv()
            if (way, t + 1, sub) in following:
                self.hop(way, t + 1, sub).start()

    def arrived(self, t):
        return [self.behind(t, 0), self.behind(t, 1)] if t < self.last else [self.behind(t, 0)]

    def finish(self):
        for t in range(1, self.last + 1):
            for h in self.hops(t):
                self.hop(*h).wait_send()


def greet(axes):
    barrier = pltpu.get_barrier_semaphore()
    for axis, size in axes.items():
        me = lax.axis_index(axis)

        @pl.loop(1, size)
        def _(k):
            pl.semaphore_signal(
                barrier, inc=1, device_id={axis: lax.rem(me + k, size)}, device_id_type=MESH
            )

    pl.semaphore_wait(barrier, sum(axes.values()) - len(axes))


def layer_kernel(
    ns, nd, docs_ref, ids_ref, gates_ref, gain_ref, score_ref, qk_hbm, v_hbm, resid_hbm, w_hbm, eg_hbm, eu_hbm, ed_hbm,
    sg_hbm, su_hbm, sd_hbm, out_ref,
    qk, v, resid, wg, wu, wd, vg, vu, vd, vecs, dcol, spread, info, routes, qh, kh, vh, att, mixed, wall, own_sum,
    send_sum, got_sum, residual, normed, every, picks, mixes, send, own_in, pair_in, act, pair_out,
    pair_part, own_part, back, ret, send_pair, ret_pair, total, landed, passed,
    w_sem, local_sem, si_sem, ri_sem, so_sem, ro_sem, sd_sem, rd_sem, sp_sem, rp_sem, sw_sem, rw_sem,
    sg_sem, rg_sem, sy_sem, ry_sem, sx_sem, rx_sem, sq_sem, rq_sem, sr_sem, rr_sem, sf_sem, rf_sem, sb_sem, rb_sem,
    s2_sem, r2_sem,
):
    s = lax.axis_index("seq")
    d = lax.axis_index("dp")
    rows, width = v.shape
    length = rows * ns
    tokens = rows * nd
    core = lax.rem(s, CORES)
    chips = ns // CORES
    depth = width // CORES
    block = width // nd
    chip_rows = rows * CORES
    half = width // 2
    quarter = half // 2
    lanes = 2 * rows

    first = [
        pltpu.make_async_copy(src, dst, w_sem.at[i])
        for i, (src, dst) in enumerate(
            (
                (qk_hbm, qk), (v_hbm, v),
                (w_hbm.at[pl.ds(pl.multiple_of(core * depth, 16), depth)], wall.at[d]),
                (resid_hbm, resid),
            )
        )
    ]
    later = [
        pltpu.make_async_copy(src, dst, w_sem.at[4 + i])
        for i, (src, dst) in enumerate(
            (
                (sg_hbm, vg), (su_hbm, vu), (sd_hbm, vd),
                (eg_hbm.at[0], wg), (eu_hbm.at[0], wu), (ed_hbm.at[0], wd),
            )
        )
    ]
    for c in first:
        c.start()

    experts = ns * nd // SPLIT
    lane = lax.broadcasted_iota(jnp.int32, (1, lanes), 1)
    valid = (lane >= lax.rem(d, 2) * rows) & (lane < (lax.rem(d, 2) + 1) * rows)
    expert = lax.broadcasted_iota(jnp.int32, (experts, lanes), 0).astype(F32)
    spread[...] = jnp.zeros_like(spread)
    spread[0:TOPK, 0:rows] = ids_ref[...].astype(F32)
    spread[TOPK:, 0:rows] = gates_ref[...]
    odd = lax.rem(d, 2).astype(F32)
    both = spread[...] * (1.0 - odd) + pltpu.roll(spread[...], rows, 1) * odd
    chosen_ids = [jnp.where(valid, both[k : k + 1, :], -1.0) for k in range(TOPK)]
    named = [ids == expert for ids in chosen_ids]
    earlier = lax.broadcasted_iota(jnp.int32, (lanes, lanes), 0) < lax.broadcasted_iota(
        jnp.int32, (lanes, lanes), 1
    )
    counts = jnp.dot(
        jnp.where(functools.reduce(jnp.logical_or, named), 1.0, 0.0).astype(BF16),
        jnp.where(earlier, 1.0, 0.0).astype(BF16),
        preferred_element_type=F32,
    )
    for k in range(TOPK):
        rank = jnp.sum(jnp.where(named[k], counts, 0.0), axis=0, keepdims=True)
        info[k : k + 1, :] = jnp.where(valid, chosen_ids[k] * CAP + rank, 0.0)
    info[TOPK:, :] = both[TOPK:, :]
    score = score_ref[...].astype(F32)
    for i in range(width // HD):
        vecs[0:1, i * HD : (i + 1) * HD] = gain_ref[i : i + 1, :]
        vecs[1:2, i * HD : (i + 1) * HD] = score[i : i + 1, :]
    routes[d] = info[...]
    docs = docs_ref[...].astype(F32)
    for i in range(length // HD):
        tile = jnp.broadcast_to(docs[:, i * HD : (i + 1) * HD], (HD, HD))
        dcol[i * HD : (i + 1) * HD, :] = tile.T

    greet({"seq": ns, "dp": nd})
    first[0].wait()
    first[1].wait()

    def own_rows(ref, t):
        return ref.at[pl.ds(pl.multiple_of(t * rows, 16), rows)]

    def cols(t):
        return pl.ds(pl.multiple_of(t * HD, HD), HD)

    def info_copy(to, slot):
        return pltpu.make_async_remote_copy(
            info, routes.at[slot], sd_sem.at[to], rd_sem.at[slot],
            device_id={"dp": to}, device_id_type=MESH,
        )

    def pieces(t):
        return (
            (qk.at[0, :, cols(t)], qh),
            (qk.at[1, :, cols(t)], kh),
            (v.at[:, cols(t)], vh),
        )

    def in_copies(j, to, slot):
        return [
            pltpu.make_async_remote_copy(
                src, own_rows(dst, slot), si_sem.at[c, j], ri_sem.at[c, j],
                device_id={"seq": to}, device_id_type=MESH,
            )
            for c, (src, dst) in enumerate(pieces(to))
        ]

    def peer(j, sign):
        chip = lax.rem(s // CORES + sign * ring_delta(j // CORES) + chips, chips)
        return chip * CORES + lax.rem(core + j, CORES)

    def toward(j):
        return peer(j, -1)

    def origin(j):
        return peer(j, 1)

    @pl.loop(1, ns)
    def _(j):
        for c in in_copies(j, toward(j), s):
            c.start()

    w_part = depth // 2
    weights = Ring(
        nd, "dp",
        lambda sub: wall.at[d, pl.ds(sub * w_part, w_part)],
        lambda index, sub: wall.at[index, pl.ds(sub * w_part, w_part)],
        sw_sem, rw_sem,
    )
    first[2].wait()
    weights.start()

    @pl.loop(1, nd)
    def _(k):
        info_copy(lax.rem(d + k, nd), d).start()

    for c in later:
        c.start()
    local = [
        pltpu.make_async_copy(src, own_rows(dst, s), local_sem.at[c])
        for c, (src, dst) in enumerate(pieces(s))
    ]
    for c in local:
        c.start()
    for c in local:
        c.wait()

    def receive(j):
        frm = origin(j)
        for c in in_copies(j, frm, frm):
            c.wait_recv()

    @pl.loop(1, ns // 2)
    def _(j):
        receive(j)

    weights.advance(1)

    @pl.loop(ns // 2, ns)
    def _(j):
        receive(j)

    per_core = ns // CORES
    mate = s + 1 - 2 * core

    def owner(chip):
        return chip * CORES + s // per_core

    def out_copy(chip, head):
        return pltpu.make_async_remote_copy(
            att.at[pl.ds(pl.multiple_of(chip * chip_rows, 16), chip_rows)],
            mixed.at[:, cols(lax.rem(head, per_core))], so_sem.at[chip],
            ro_sem.at[lax.rem(head, per_core)],
            device_id={"seq": owner(chip)}, device_id_type=MESH,
        )

    scale = 1.0 / math.sqrt(HD)
    step_rows = 2 * chip_rows
    for i in range(length // step_rows):
        upto = (i + 1) * step_rows
        span = pl.ds(i * step_rows, step_rows)
        scores = lax.dot_general(
            qh[span, :], kh[0:upto, :], (((1,), (1,)), ((), ())), preferred_element_type=F32
        ) * scale
        at = lax.broadcasted_iota(jnp.int32, (step_rows, upto), 0) + i * step_rows
        key_at = lax.broadcasted_iota(jnp.int32, (step_rows, upto), 1)
        mine = jnp.concatenate([dcol[span, :]] * (upto // HD), axis=1)
        allowed = (key_at <= at) & (mine == docs[:, 0:upto])
        scores = jnp.where(allowed, scores, -1e30)
        lifted = jnp.exp(scores - jnp.max(scores, axis=-1, keepdims=True))
        probs = (lifted / jnp.sum(lifted, axis=-1, keepdims=True)).astype(BF16)
        att[span, :] = jnp.dot(probs, vh[0:upto, :], preferred_element_type=F32).astype(BF16)
        for chip in (2 * i, 2 * i + 1):

            @pl.when(owner(chip) != s)
            def _():
                out_copy(chip, s).start()

            @pl.when(owner(chip) == s)
            def _():
                mixed[:, cols(lax.rem(s, per_core))] = att[
                    pl.ds(chip * chip_rows, chip_rows), :
                ]

        if i == 1:
            weights.advance(2)

    slots = nd * CAP
    per_seq = nd // SPLIT
    first_expert = d // SPLIT

    @pl.loop(1, nd)
    def _(k):
        other = lax.rem(d + k, nd)
        info_copy(other, other).wait_send()
        info_copy(other, other).wait_recv()

    tiles = [routes[2 * m] + routes[2 * m + 1] for m in range(nd // 2)]
    code = jnp.concatenate([tile[:TOPK] for tile in tiles], axis=1)
    gates = jnp.concatenate([tile[TOPK:] for tile in tiles], axis=1)
    slot = lax.broadcasted_iota(jnp.int32, (slots, tokens), 0).astype(F32)
    token = lax.broadcasted_iota(jnp.int32, (slots, tokens), 1).astype(F32)
    slot_block = jnp.floor((slot + 0.5) * (1.0 / CAP))
    token_block = jnp.floor((token + 0.5) * (1.0 / rows))
    ranks = jnp.where(slot_block == token_block, slot - slot_block * CAP, -1e6)

    def seat(j):
        return pl.ds(pl.multiple_of(j * slots, 16), slots)

    @pl.loop(0, ns)
    def _(j):
        base = ((toward(j) * per_seq + first_expert) * CAP).astype(F32)
        hits = [code[k : k + 1, :] - base == ranks for k in range(TOPK)]
        hit = functools.reduce(jnp.logical_or, hits)
        picks[seat(j), :] = jnp.where(hit, 1.0, 0.0).astype(BF16)
        mixes[seat(j), :] = functools.reduce(
            jnp.add, [jnp.where(hits[k], gates[k : k + 1, :], 0.0) for k in range(TOPK)]
        ).astype(BF16)

    weights.advance(3)

    @pl.loop(0, per_core)
    def _(h):
        @pl.when(core * per_core + h != s)
        def _():
            out_copy(0, h).wait_recv()

    def sum_copy(index):
        at = pl.ds(pl.multiple_of(index * block, block), block)
        return pltpu.make_async_remote_copy(
            send_sum.at[:, at], got_sum.at[:, at], sp_sem.at[index], rp_sem.at[index],
            device_id={"seq": mate}, device_id_type=MESH,
        )

    def project(index):
        at = pl.ds(pl.multiple_of(index * block, block), block)
        theirs = mixed[pl.ds(pl.multiple_of((1 - core) * rows, 16), rows), :]
        mine = mixed[pl.ds(pl.multiple_of(core * rows, 16), rows), :]
        send_sum[:, at] = jnp.dot(theirs, wall[index], preferred_element_type=F32)
        own_sum[:, at] = jnp.dot(mine, wall[index], preferred_element_type=F32)
        sum_copy(index).start()

    project(d)
    for t in range(1, nd // 2 + 1):
        if t >= 4:
            weights.advance(t)
        for index in weights.arrived(t):
            project(index)

    @pl.loop(0, nd)
    def _(index):
        sum_copy(index).wait_recv()

    first[3].wait()
    projected = (own_sum[...] + got_sum[...]).astype(BF16)
    summed = (resid[...].astype(F32) + projected.astype(F32)).astype(BF16)
    residual[...] = summed
    stream = summed.astype(F32)
    scaled = (
        stream
        * lax.rsqrt(jnp.mean(stream * stream, axis=-1, keepdims=True) + norm_eps)
        * vecs[0:1, :]
    ).astype(BF16)

    def place_of(chunk, side):
        return side * half + chunk * quarter

    mine_at = pl.ds(pl.multiple_of(d * rows, 16), rows)
    for chunk in range(2):
        for side in range(2):
            at = place_of(chunk, side)
            normed[chunk, side] = scaled[:, at : at + quarter]
            every[chunk, side, mine_at, :] = scaled[:, at : at + quarter]
    part = rows // 2

    def gather(chunk):
        return Ring(
            nd, "dp",
            lambda sub: normed.at[chunk, :, pl.ds(sub * part, part)],
            lambda index, sub: every.at[
                chunk, :, pl.ds(pl.multiple_of(index * rows + sub * part, 16), part)
            ],
            sg_sem.at[chunk], rg_sem.at[chunk],
        )

    rings = [gather(0), gather(1)]

    par = lax.rem(d, 2)
    partner = d + 1 - 2 * par
    group_slots = GROUP * slots
    groups = ns // GROUP

    def span_of(g):
        return pl.ds(pl.multiple_of(g * group_slots, 16), group_slots)

    def go_copy(chunk, j):
        return pltpu.make_async_remote_copy(
            send.at[chunk, seat(j)], own_in.at[chunk, seat(j)], sy_sem.at[chunk, j],
            ry_sem.at[chunk, j], device_id={"seq": toward(j)}, device_id_type=MESH,
        )

    def swap_copy(chunk, g):
        return pltpu.make_async_remote_copy(
            own_in.at[chunk, span_of(g)], pair_in.at[chunk, span_of(g)], sx_sem.at[chunk, g],
            rx_sem.at[chunk, g], device_id={"dp": partner}, device_id_type=MESH,
        )

    def part_copy(chunk, g):
        return pltpu.make_async_remote_copy(
            pair_out.at[chunk, span_of(g)], pair_part.at[chunk, span_of(g)], sq_sem.at[chunk, g],
            rq_sem.at[chunk, g], device_id={"dp": partner}, device_id_type=MESH,
        )

    def back_copy(chunk, j):
        return pltpu.make_async_remote_copy(
            back.at[chunk, seat(j)], ret.at[chunk, seat(j)], sr_sem.at[chunk, j],
            rr_sem.at[chunk, j], device_id={"seq": origin(j)}, device_id_type=MESH,
        )

    def go_pair(chunk, j):
        return pltpu.make_async_remote_copy(
            send_pair.at[chunk, seat(j)], pair_in.at[chunk, seat(j)], sf_sem.at[chunk, j],
            rf_sem.at[chunk, j], device_id={"seq": toward(j)}, device_id_type=MESH,
        )

    def back_pair(chunk, j):
        return pltpu.make_async_remote_copy(
            pair_out.at[chunk, seat(j)], ret_pair.at[chunk, seat(j)], sb_sem.at[chunk, j],
            rb_sem.at[chunk, j], device_id={"seq": origin(j)}, device_id_type=MESH,
        )

    near_seats = DIRECT * GROUP

    def columns(chunk, side):
        return pl.ds(pl.multiple_of(side * half + chunk * quarter, quarter), quarter)

    batch = ns // 4

    def pick(chunk, q):
        at = pl.ds(q * batch * slots, batch * slots)
        got = jnp.dot(
            picks[at, :], every[chunk, par], preferred_element_type=F32
        ).astype(BF16)
        send[chunk, at, :] = got
        if q == 0:
            own_in[chunk, 0:slots, :] = got[0:slots]
            near = pl.ds(0, near_seats * slots)
            got = jnp.dot(
                picks[near, :], every[chunk, 1 - par], preferred_element_type=F32
            ).astype(BF16)
            send_pair[chunk, near, :] = got
            pair_in[chunk, 0:slots, :] = got[0:slots]

    def go(chunk, q):
        @pl.loop(max(1, q * batch), (q + 1) * batch)
        def _(j):
            go_copy(chunk, j).start()

        if q == 0:

            @pl.loop(1, near_seats)
            def _(j):
                go_pair(chunk, j).start()

    for ring in rings:
        ring.start()
    for t in range(1, nd // 2):
        for ring in rings:
            ring.advance(t)
    for chunk in range(2):
        rings[chunk].advance(nd // 2)
        for q in range(4):
            pick(chunk, q)
            if q:
                go(chunk, q - 1)
        go(chunk, 3)
    for c in later:
        c.wait()

    def nt(a, w):
        return lax.dot_general(a, w, (((1,), (1,)), ((), ())), preferred_element_type=F32)

    def silu(a):
        return a / (1.0 + jnp.exp(-a))

    def arrive(chunk, g):
        for i in range(GROUP):
            j = g * GROUP + i

            @pl.when(j > 0)
            def _():
                go_copy(chunk, j).wait_recv()

            @pl.when((j > 0) & (g < DIRECT))
            def _():
                go_pair(chunk, j).wait_recv()

        @pl.when(g >= DIRECT)
        def _():
            swap_copy(chunk, g).start()

    quads = [(chunk, side) for chunk in range(2) for side in range(2)]
    share = tokens // 4

    @pl.loop(0, groups)
    def _(g):
        arrive(0, g)

        @pl.when((g >= 1) & (g <= 4))
        def _():
            at = pl.ds(pl.multiple_of((g - 1) * share, share), share)
            gate_act = jnp.zeros((share, vg.shape[0]), F32)
            up_act = jnp.zeros((share, vg.shape[0]), F32)
            weight = jnp.zeros((share, 1), F32)
            for chunk, side in quads:
                a = every[chunk, side, at, :]
                where = pl.ds(place_of(chunk, side), quarter)
                gate_act += nt(a, vg[:, where])
                up_act += nt(a, vu[:, where])
                weight += jnp.sum(
                    a.astype(F32) * vecs[1:2, where], axis=-1, keepdims=True
                )
            hidden = (silu(gate_act) * up_act).astype(BF16)
            weight = 1.0 / (1.0 + jnp.exp(-weight))
            for chunk, side in quads:
                total[chunk, side, at, :] = weight * jnp.dot(
                    hidden, vd[:, pl.ds(place_of(chunk, side), quarter)],
                    preferred_element_type=F32,
                )

    def down(chunk, g):
        hidden = act[span_of(g), :]
        pair_out[chunk, span_of(g), :] = jnp.dot(
            hidden, wd[:, columns(chunk, 1 - par)], preferred_element_type=F32
        ).astype(BF16)
        own_part[span_of(g), :] = jnp.dot(
            hidden, wd[:, columns(chunk, par)], preferred_element_type=F32
        )

        @pl.when(g >= DIRECT)
        def _():
            part_copy(chunk, g).start()

    def join(chunk, g):
        @pl.when(g >= DIRECT)
        def _():
            part_copy(chunk, g).wait_recv()
            back[chunk, span_of(g), :] = (
                own_part[span_of(g), :] + pair_part[chunk, span_of(g), :].astype(F32)
            ).astype(BF16)

        @pl.when(g < DIRECT)
        def _():
            back[chunk, span_of(g), :] = own_part[span_of(g), :].astype(BF16)

    def leave(chunk, g):
        for i in range(GROUP):
            j = g * GROUP + i

            @pl.when(j > 0)
            def _():
                back_copy(chunk, j).start()

            @pl.when((j > 0) & (g < DIRECT))
            def _():
                back_pair(chunk, j).start()

            @pl.when(j == 0)
            def _():
                ret[chunk, 0:slots, :] = back[chunk, 0:slots, :]
                ret_pair[chunk, 0:slots, :] = pair_out[chunk, 0:slots, :]

    def combine(chunk, g):
        for i in range(GROUP):
            j = g * GROUP + i

            @pl.when(j > 0)
            def _():
                back_copy(chunk, j).wait_recv()

            @pl.when((j > 0) & (g < DIRECT))
            def _():
                back_pair(chunk, j).wait_recv()

        def mix(rows_in):
            return lax.dot_general(
                mixes[span_of(g), :], rows_in[chunk, span_of(g), :], (((0,), (0,)), ((), ())),
                preferred_element_type=F32,
            )

        total[chunk, par] += mix(ret)

        @pl.when(g < DIRECT)
        def _():
            total[chunk, 1 - par] += mix(ret_pair)

    @pl.loop(0, groups + 2)
    def _(step):
        @pl.when(step < groups)
        def _():
            arrive(1, step)

        @pl.when(step >= 2)
        def _():
            join(0, step - 2)

        @pl.when((step >= 1) & (step <= groups))
        def _():
            g = step - 1
            gate_act = jnp.zeros((group_slots, wg.shape[0]), F32)
            up_act = jnp.zeros((group_slots, wg.shape[0]), F32)
            for chunk in range(2):
                @pl.when(g >= DIRECT)
                def _():
                    swap_copy(chunk, g).wait_recv()

                for rows_in, side in ((own_in, par), (pair_in, 1 - par)):
                    a = rows_in[chunk, span_of(g), :]
                    gate_act += nt(a, wg[:, columns(chunk, side)])
                    up_act += nt(a, wu[:, columns(chunk, side)])
            act[span_of(g), :] = (silu(gate_act) * up_act).astype(BF16)
            down(0, g)

        @pl.when(step >= 2)
        def _():
            leave(0, step - 2)

    @pl.loop(0, groups)
    def _(g):
        down(1, g)

    @pl.loop(0, groups)
    def _(g):
        join(1, g)
        leave(1, g)
        combine(0, g)

    last = nd // 2

    def own(index, sub):
        return pl.ds(pl.multiple_of(index * rows + sub * part, 16), part)

    def used(way, t, sub):
        return t < last or (t == last and sub == way)

    def hop(chunk, way, t, sub):
        sign = 1 - 2 * way
        return pltpu.make_async_remote_copy(
            passed.at[chunk, way, t - 1, sub], landed.at[chunk, way, t - 1, sub],
            s2_sem.at[chunk, way, t - 1, sub], r2_sem.at[chunk, way, t - 1, sub],
            device_id={"dp": lax.rem(d + sign + nd, nd)}, device_id_type=MESH,
        )

    def target(way, t):
        return lax.rem(d + (1 - 2 * way) * t + nd, nd)

    def reduce_step(chunk, t):
        for sub in range(2):
            for way in range(2):
                if not used(way, t, sub):
                    continue
                term = total[chunk, :, own(target(way, t), sub), :]
                if used(way, t + 1, sub):
                    hop(chunk, way, t + 1, sub).wait_recv()
                    term = term + landed[chunk, way, t, sub].astype(F32)
                passed[chunk, way, t - 1, sub] = term.astype(BF16)
                hop(chunk, way, t, sub).start()

    def settle(chunk):
        for sub in range(2):
            for way in range(2):
                hop(chunk, way, 1, sub).wait_recv()
            at = pl.ds(sub * part, part)
            sums = (
                total[chunk, :, own(d, sub), :]
                + landed[chunk, 0, 0, sub].astype(F32)
                + landed[chunk, 1, 0, sub].astype(F32)
            )
            for side in range(2):
                where = pl.ds(place_of(chunk, side), quarter)
                out_ref[at, where] = residual[at, where].astype(F32) + sums[side]

    for t in range(last, 0, -1):
        reduce_step(0, t)

        @pl.loop((last - t) * groups // last, (last - t + 1) * groups // last)
        def _(g):
            combine(1, g)

    for t in range(last, 0, -1):
        reduce_step(1, t)
    settle(0)
    settle(1)

    for chunk in range(2):
        for way in range(2):
            for sub in range(2):
                for t in range(1, last + 1):
                    if used(way, t, sub):
                        hop(chunk, way, t, sub).wait_send()
        rings[chunk].finish()

        @pl.loop(1, ns)
        def _(j):
            go_copy(chunk, j).wait_send()
            back_copy(chunk, j).wait_send()

        @pl.loop(1, near_seats)
        def _(j):
            go_pair(chunk, j).wait_send()
            back_pair(chunk, j).wait_send()

        @pl.loop(DIRECT, groups)
        def _(g):
            swap_copy(chunk, g).wait_send()
            part_copy(chunk, g).wait_send()

    weights.finish()

    @pl.loop(1, ns)
    def _(j):
        for c in in_copies(j, toward(j), s):
            c.wait_send()

    @pl.loop(0, chips)
    def _(chip):
        @pl.when(owner(chip) != s)
        def _():
            out_copy(chip, s).wait_send()

    @pl.loop(0, nd)
    def _(index):
        sum_copy(index).wait_send()


def run_layer(docs, ids, gates, gain, score, qk, v, resid, out_weight, expert_weights, shared_weights, ns, nd):
    rows, width = v.shape
    length = rows * ns
    tokens = rows * nd
    half = width // 2
    quarter = half // 2
    slots = ns * nd * CAP
    groups = ns // GROUP
    near = DIRECT * GROUP * nd * CAP
    hidden = expert_weights[0].shape[1]
    shared_hidden = shared_weights[0].shape[0]
    dma = pltpu.SemaphoreType.DMA
    vmem = pl.BlockSpec(memory_space=pltpu.VMEM)
    anyspace = pl.BlockSpec(memory_space=pl.ANY)

    def buf(*shape):
        return pltpu.VMEM(shape, BF16)

    def wide(*shape):
        return pltpu.VMEM(shape, F32)

    ring = dma((2, nd // 2, 2))
    rings = dma((2, 2, nd // 2, 2))
    per_seat = dma((2, ns))
    per_group = dma((2, groups))
    per_near = dma((2, DIRECT * GROUP))
    return pl.pallas_call(
        functools.partial(layer_kernel, ns, nd),
        out_shape=jax.ShapeDtypeStruct((rows, width), F32),
        in_specs=[vmem] * 5 + [anyspace] * 10,
        out_specs=vmem,
        scratch_shapes=[buf(2, rows, width), buf(rows, width), buf(rows, width)]
        + [buf(hidden, width)] * 3
        + [buf(shared_hidden, width)] * 3
        + [wide(2, width), wide(length, HD)]
        + [wide(2 * TOPK, 2 * rows), wide(2 * TOPK, 2 * rows), wide(nd, 2 * TOPK, 2 * rows)]
        + [buf(length, HD)] * 4
        + [
            buf(rows * CORES, width // CORES),
            buf(nd, width // CORES, out_weight.shape[1]),
            wide(rows, width), wide(rows, width), wide(rows, width),
            buf(rows, width),
            buf(2, 2, rows, quarter),
            buf(2, 2, tokens, quarter),
            buf(slots, tokens), buf(slots, tokens),
            buf(2, slots, quarter), buf(2, slots, quarter), buf(2, slots, quarter),
            buf(slots, hidden),
            buf(2, slots, quarter), buf(2, slots, quarter),
            wide(slots, quarter),
            buf(2, slots, quarter), buf(2, slots, quarter),
            buf(2, near, quarter), buf(2, near, quarter),
            wide(2, 2, tokens, quarter),
            buf(2, 2, nd // 2, 2, 2, rows // 2, quarter),
            buf(2, 2, nd // 2, 2, 2, rows // 2, quarter),
            dma((10,)), dma((3,)), dma((3, ns)), dma((3, ns)), dma((ns // CORES,)),
            dma((ns // CORES,)), dma((nd,)), dma((nd,)), dma((nd,)), dma((nd,)),
            ring, ring, rings, rings,
            per_seat, per_seat, per_group, per_group, per_group, per_group, per_seat, per_seat,
            per_near, per_near, per_near, per_near, rings, rings,
        ],
        compiler_params=pltpu.CompilerParams(
            collective_id=1, has_side_effects=True, vmem_limit_bytes=67043328
        ),
        cost_estimate=pl.CostEstimate(
            flops=12 * slots * half * hidden, bytes_accessed=8 * slots * half, transcendentals=0
        ),
        name="layer",
    )(docs, ids, gates, gain, score, qk, v, resid, out_weight, *expert_weights, *shared_weights)


def body(
    resid,
    queries_keys,
    values,
    doc_ids,
    out_weight,
    norm_gain,
    expert_ids,
    gate_vals,
    expert_gate,
    expert_up,
    expert_down,
    shared_gate,
    shared_up,
    shared_down,
    shared_score,
):
    ns = lax.axis_size("seq")
    nd = lax.axis_size("dp")
    tokens = resid.shape[1]
    width = resid.shape[2]
    out = run_layer(
        doc_ids,
        expert_ids[0].T,
        gate_vals[0].T,
        norm_gain.reshape(-1, HD),
        shared_score.reshape(-1, HD),
        queries_keys.reshape(2, tokens, width),
        values[0],
        resid[0],
        out_weight,
        (expert_gate.transpose(0, 2, 1), expert_up.transpose(0, 2, 1), expert_down),
        (shared_gate.T, shared_up.T, shared_down),
        ns,
        nd,
    )
    return out.astype(BF16)[None]


def solution(mesh):
    placed = (
        P(("groups", "dp"), "seq", None),
        P(None, ("groups", "dp"), "seq", None),
        P(("groups", "dp"), "seq", None),
        P(("groups", "dp"), None),
        P(None, "dp"),
        P(),
        P(("groups", "dp"), "seq", None),
        P(("groups", "dp"), "seq", None),
        P(("seq", "dp"), None, None),
        P(("seq", "dp"), None, None),
        P(("seq", "dp"), None, None),
        P(None, "dp"),
        P(None, "dp"),
        P("dp", None),
        P(),
    )
    return jax.shard_map(
        body,
        mesh=mesh,
        in_specs=placed,
        out_specs=P(("groups", "dp"), "seq", None),
        check_vma=False,
    )
```

```python
import functools
import math

import jax
import jax.numpy as jnp
from jax import lax
from jax.experimental import pallas as pl
from jax.experimental.pallas import tpu as pltpu
from jax.sharding import PartitionSpec as P

HD = 128
TOPK = 4
SPLIT = 4
CAP = 10
GROUP = 2
CORES = 2
DIRECT = 1

norm_eps = 1e-06
MESH = pl.DeviceIdType.MESH
F32 = jnp.float32
BF16 = jnp.bfloat16


def ring_delta(j):
    return ((j + 1) // 2) * (2 * (j % 2) - 1)


class Ring:
    def __init__(self, nd, axis, source, place, send_sem, recv_sem):
        self.nd, self.axis, self.last = nd, axis, nd // 2
        self.source, self.place = source, place
        self.send_sem, self.recv_sem = send_sem, recv_sem
        self.me = lax.axis_index(axis)

    def behind(self, t, way):
        return lax.rem(self.me - (1 - 2 * way) * t + self.nd, self.nd)

    def hop(self, way, t, sub):
        index = self.behind(t - 1, way)
        src = self.source(sub) if t == 1 else self.place(index, sub)
        return pltpu.make_async_remote_copy(
            src, self.place(index, sub), self.send_sem.at[way, t - 1, sub],
            self.recv_sem.at[way, t - 1, sub],
            device_id={self.axis: self.behind(-1, way)}, device_id_type=MESH,
        )

    def hops(self, t):
        return [
            (way, t, sub)
            for sub in range(2)
            for way in range(2)
            if t < self.last or (t == self.last and sub == way)
        ]

    def start(self):
        for h in self.hops(1):
            self.hop(*h).start()

    def advance(self, t):
        following = self.hops(t + 1)
        for way, _, sub in self.hops(t):
            self.hop(way, t, sub).wait_recv()
            if (way, t + 1, sub) in following:
                self.hop(way, t + 1, sub).start()

    def arrived(self, t):
        return [self.behind(t, 0), self.behind(t, 1)] if t < self.last else [self.behind(t, 0)]

    def finish(self):
        for t in range(1, self.last + 1):
            for h in self.hops(t):
                self.hop(*h).wait_send()


def greet(axes):
    barrier = pltpu.get_barrier_semaphore()
    for axis, size in axes.items():
        me = lax.axis_index(axis)

        @pl.loop(1, size)
        def _(k):
            pl.semaphore_signal(
                barrier, inc=1, device_id={axis: lax.rem(me + k, size)}, device_id_type=MESH
            )

    pl.semaphore_wait(barrier, sum(axes.values()) - len(axes))


def layer_kernel(
    ns, nd, docs_ref, ids_ref, gates_ref, gain_ref, score_ref, qk_hbm, v_hbm, resid_hbm, w_hbm, eg_hbm, eu_hbm, ed_hbm,
    sg_hbm, su_hbm, sd_hbm, out_ref,
    qk, v, resid, wg, wu, wd, vg, vu, vd, vecs, dcol, spread, info, routes, qh, kh, vh, att, mixed, wall, own_sum,
    send_sum, got_sum, residual, normed, every, picks, mixes, send, own_in, pair_in, act, pair_out,
    pair_part, own_part, back, ret, send_pair, ret_pair, total, landed, passed,
    w_sem, local_sem, si_sem, ri_sem, so_sem, ro_sem, sd_sem, rd_sem, sp_sem, rp_sem, sw_sem, rw_sem,
    sg_sem, rg_sem, sy_sem, ry_sem, sx_sem, rx_sem, sq_sem, rq_sem, sr_sem, rr_sem, sf_sem, rf_sem, sb_sem, rb_sem,
    s2_sem, r2_sem,
):
    s = lax.axis_index("seq")
    d = lax.axis_index("dp")
    rows, width = v.shape
    length = rows * ns
    tokens = rows * nd
    core = lax.rem(s, CORES)
    chips = ns // CORES
    depth = width // CORES
    block = width // nd
    chip_rows = rows * CORES
    half = width // 2
    quarter = half // 2
    lanes = 2 * rows

    first = [
        pltpu.make_async_copy(src, dst, w_sem.at[i])
        for i, (src, dst) in enumerate(
            (
                (qk_hbm, qk), (v_hbm, v),
                (w_hbm.at[pl.ds(pl.multiple_of(core * depth, 16), depth)], wall.at[d]),
                (resid_hbm, resid),
            )
        )
    ]
    later = [
        pltpu.make_async_copy(src, dst, w_sem.at[4 + i])
        for i, (src, dst) in enumerate(
            (
                (sg_hbm, vg), (su_hbm, vu), (sd_hbm, vd),
                (eg_hbm.at[0], wg), (eu_hbm.at[0], wu), (ed_hbm.at[0], wd),
            )
        )
    ]
    for c in first:
        c.start()

    experts = ns * nd // SPLIT
    lane = lax.broadcasted_iota(jnp.int32, (1, lanes), 1)
    valid = (lane >= lax.rem(d, 2) * rows) & (lane < (lax.rem(d, 2) + 1) * rows)
    expert = lax.broadcasted_iota(jnp.int32, (experts, lanes), 0).astype(F32)
    spread[...] = jnp.zeros_like(spread)
    spread[0:TOPK, 0:rows] = ids_ref[...].astype(F32)
    spread[TOPK:, 0:rows] = gates_ref[...]
    odd = lax.rem(d, 2).astype(F32)
    both = spread[...] * (1.0 - odd) + pltpu.roll(spread[...], rows, 1) * odd
    chosen_ids = [jnp.where(valid, both[k : k + 1, :], -1.0) for k in range(TOPK)]
    named = [ids == expert for ids in chosen_ids]
    earlier = lax.broadcasted_iota(jnp.int32, (lanes, lanes), 0) < lax.broadcasted_iota(
        jnp.int32, (lanes, lanes), 1
    )
    counts = jnp.dot(
        jnp.where(functools.reduce(jnp.logical_or, named), 1.0, 0.0).astype(BF16),
        jnp.where(earlier, 1.0, 0.0).astype(BF16),
        preferred_element_type=F32,
    )
    for k in range(TOPK):
        rank = jnp.sum(jnp.where(named[k], counts, 0.0), axis=0, keepdims=True)
        info[k : k + 1, :] = jnp.where(valid, chosen_ids[k] * CAP + rank, 0.0)
    info[TOPK:, :] = both[TOPK:, :]
    score = score_ref[...].astype(F32)
    for i in range(width // HD):
        vecs[0:1, i * HD : (i + 1) * HD] = gain_ref[i : i + 1, :]
        vecs[1:2, i * HD : (i + 1) * HD] = score[i : i + 1, :]
    routes[d] = info[...]
    docs = docs_ref[...].astype(F32)
    for i in range(length // HD):
        tile = jnp.broadcast_to(docs[:, i * HD : (i + 1) * HD], (HD, HD))
        dcol[i * HD : (i + 1) * HD, :] = tile.T

    greet({"seq": ns, "dp": nd})
    first[0].wait()
    first[1].wait()

    def own_rows(ref, t):
        return ref.at[pl.ds(pl.multiple_of(t * rows, 16), rows)]

    def cols(t):
        return pl.ds(pl.multiple_of(t * HD, HD), HD)

    def info_copy(to, slot):
        return pltpu.make_async_remote_copy(
            info, routes.at[slot], sd_sem.at[to], rd_sem.at[slot],
            device_id={"dp": to}, device_id_type=MESH,
        )

    def pieces(t):
        return (
            (qk.at[0, :, cols(t)], qh),
            (qk.at[1, :, cols(t)], kh),
            (v.at[:, cols(t)], vh),
        )

    def in_copies(j, to, slot):
        return [
            pltpu.make_async_remote_copy(
                src, own_rows(dst, slot), si_sem.at[c, j], ri_sem.at[c, j],
                device_id={"seq": to}, device_id_type=MESH,
            )
            for c, (src, dst) in enumerate(pieces(to))
        ]

    def peer(j, sign):
        chip = lax.rem(s // CORES + sign * ring_delta(j // CORES) + chips, chips)
        return chip * CORES + lax.rem(core + j, CORES)

    def toward(j):
        return peer(j, -1)

    def origin(j):
        return peer(j, 1)

    @pl.loop(1, ns)
    def _(j):
        for c in in_copies(j, toward(j), s):
            c.start()

    w_part = depth // 2
    weights = Ring(
        nd, "dp",
        lambda sub: wall.at[d, pl.ds(sub * w_part, w_part)],
        lambda index, sub: wall.at[index, pl.ds(sub * w_part, w_part)],
        sw_sem, rw_sem,
    )
    first[2].wait()
    weights.start()

    @pl.loop(1, nd)
    def _(k):
        info_copy(lax.rem(d + k, nd), d).start()

    for c in later:
        c.start()
    local = [
        pltpu.make_async_copy(src, own_rows(dst, s), local_sem.at[c])
        for c, (src, dst) in enumerate(pieces(s))
    ]
    for c in local:
        c.start()
    for c in local:
        c.wait()

    def receive(j):
        frm = origin(j)
        for c in in_copies(j, frm, frm):
            c.wait_recv()

    @pl.loop(1, ns // 2)
    def _(j):
        receive(j)

    weights.advance(1)

    @pl.loop(ns // 2, ns)
    def _(j):
        receive(j)

    per_core = ns // CORES
    mate = s + 1 - 2 * core

    def owner(chip):
        return chip * CORES + s // per_core

    def out_copy(chip, head):
        return pltpu.make_async_remote_copy(
            att.at[pl.ds(pl.multiple_of(chip * chip_rows, 16), chip_rows)],
            mixed.at[:, cols(lax.rem(head, per_core))], so_sem.at[chip],
            ro_sem.at[lax.rem(head, per_core)],
            device_id={"seq": owner(chip)}, device_id_type=MESH,
        )

    scale = 1.0 / math.sqrt(HD)
    step_rows = 2 * chip_rows
    for i in range(length // step_rows):
        upto = (i + 1) * step_rows
        span = pl.ds(i * step_rows, step_rows)
        scores = lax.dot_general(
            qh[span, :], kh[0:upto, :], (((1,), (1,)), ((), ())), preferred_element_type=F32
        ) * scale
        at = lax.broadcasted_iota(jnp.int32, (step_rows, upto), 0) + i * step_rows
        key_at = lax.broadcasted_iota(jnp.int32, (step_rows, upto), 1)
        mine = jnp.concatenate([dcol[span, :]] * (upto // HD), axis=1)
        allowed = (key_at <= at) & (mine == docs[:, 0:upto])
        scores = jnp.where(allowed, scores, -1e30)
        lifted = jnp.exp(scores - jnp.max(scores, axis=-1, keepdims=True))
        probs = (lifted / jnp.sum(lifted, axis=-1, keepdims=True)).astype(BF16)
        att[span, :] = jnp.dot(probs, vh[0:upto, :], preferred_element_type=F32).astype(BF16)
        for chip in (2 * i, 2 * i + 1):

            @pl.when(owner(chip) != s)
            def _():
                out_copy(chip, s).start()

            @pl.when(owner(chip) == s)
            def _():
                mixed[:, cols(lax.rem(s, per_core))] = att[
                    pl.ds(chip * chip_rows, chip_rows), :
                ]

        if i == 1:
            weights.advance(2)

    slots = nd * CAP
    per_seq = nd // SPLIT
    first_expert = d // SPLIT

    @pl.loop(1, nd)
    def _(k):
        other = lax.rem(d + k, nd)
        info_copy(other, other).wait_send()
        info_copy(other, other).wait_recv()

    tiles = [routes[2 * m] + routes[2 * m + 1] for m in range(nd // 2)]
    code = jnp.concatenate([tile[:TOPK] for tile in tiles], axis=1)
    gates = jnp.concatenate([tile[TOPK:] for tile in tiles], axis=1)
    slot = lax.broadcasted_iota(jnp.int32, (slots, tokens), 0).astype(F32)
    token = lax.broadcasted_iota(jnp.int32, (slots, tokens), 1).astype(F32)
    slot_block = jnp.floor((slot + 0.5) * (1.0 / CAP))
    token_block = jnp.floor((token + 0.5) * (1.0 / rows))
    ranks = jnp.where(slot_block == token_block, slot - slot_block * CAP, -1e6)

    def seat(j):
        return pl.ds(pl.multiple_of(j * slots, 16), slots)

    @pl.loop(0, ns)
    def _(j):
        base = ((toward(j) * per_seq + first_expert) * CAP).astype(F32)
        hits = [code[k : k + 1, :] - base == ranks for k in range(TOPK)]
        hit = functools.reduce(jnp.logical_or, hits)
        picks[seat(j), :] = jnp.where(hit, 1.0, 0.0).astype(BF16)
        mixes[seat(j), :] = functools.reduce(
            jnp.add, [jnp.where(hits[k], gates[k : k + 1, :], 0.0) for k in range(TOPK)]
        ).astype(BF16)

    weights.advance(3)

    @pl.loop(0, per_core)
    def _(h):
        @pl.when(core * per_core + h != s)
        def _():
            out_copy(0, h).wait_recv()

    def sum_copy(index):
        at = pl.ds(pl.multiple_of(index * block, block), block)
        return pltpu.make_async_remote_copy(
            send_sum.at[:, at], got_sum.at[:, at], sp_sem.at[index], rp_sem.at[index],
            device_id={"seq": mate}, device_id_type=MESH,
        )

    def project(index):
        at = pl.ds(pl.multiple_of(index * block, block), block)
        theirs = mixed[pl.ds(pl.multiple_of((1 - core) * rows, 16), rows), :]
        mine = mixed[pl.ds(pl.multiple_of(core * rows, 16), rows), :]
        send_sum[:, at] = jnp.dot(theirs, wall[index], preferred_element_type=F32)
        own_sum[:, at] = jnp.dot(mine, wall[index], preferred_element_type=F32)
        sum_copy(index).start()

    project(d)
    for t in range(1, nd // 2 + 1):
        if t >= 4:
            weights.advance(t)
        for index in weights.arrived(t):
            project(index)

    @pl.loop(0, nd)
    def _(index):
        sum_copy(index).wait_recv()

    first[3].wait()
    projected = (own_sum[...] + got_sum[...]).astype(BF16)
    summed = (resid[...].astype(F32) + projected.astype(F32)).astype(BF16)
    residual[...] = summed
    stream = summed.astype(F32)
    scaled = (
        stream
        * lax.rsqrt(jnp.mean(stream * stream, axis=-1, keepdims=True) + norm_eps)
        * vecs[0:1, :]
    ).astype(BF16)

    def place_of(chunk, side):
        return side * half + chunk * quarter

    mine_at = pl.ds(pl.multiple_of(d * rows, 16), rows)
    for chunk in range(2):
        for side in range(2):
            at = place_of(chunk, side)
            normed[chunk, side] = scaled[:, at : at + quarter]
            every[chunk, side, mine_at, :] = scaled[:, at : at + quarter]
    part = rows // 2

    def gather(chunk):
        return Ring(
            nd, "dp",
            lambda sub: normed.at[chunk, :, pl.ds(sub * part, part)],
            lambda index, sub: every.at[
                chunk, :, pl.ds(pl.multiple_of(index * rows + sub * part, 16), part)
            ],
            sg_sem.at[chunk], rg_sem.at[chunk],
        )

    rings = [gather(0), gather(1)]

    par = lax.rem(d, 2)
    partner = d + 1 - 2 * par
    group_slots = GROUP * slots
    groups = ns // GROUP

    def span_of(g):
        return pl.ds(pl.multiple_of(g * group_slots, 16), group_slots)

    def go_copy(chunk, j):
        return pltpu.make_async_remote_copy(
            send.at[chunk, seat(j)], own_in.at[chunk, seat(j)], sy_sem.at[chunk, j],
            ry_sem.at[chunk, j], device_id={"seq": toward(j)}, device_id_type=MESH,
        )

    def swap_copy(chunk, g):
        return pltpu.make_async_remote_copy(
            own_in.at[chunk, span_of(g)], pair_in.at[chunk, span_of(g)], sx_sem.at[chunk, g],
            rx_sem.at[chunk, g], device_id={"dp": partner}, device_id_type=MESH,
        )

    def part_copy(chunk, g):
        return pltpu.make_async_remote_copy(
            pair_out.at[chunk, span_of(g)], pair_part.at[chunk, span_of(g)], sq_sem.at[chunk, g],
            rq_sem.at[chunk, g], device_id={"dp": partner}, device_id_type=MESH,
        )

    def back_copy(chunk, j):
        return pltpu.make_async_remote_copy(
            back.at[chunk, seat(j)], ret.at[chunk, seat(j)], sr_sem.at[chunk, j],
            rr_sem.at[chunk, j], device_id={"seq": origin(j)}, device_id_type=MESH,
        )

    def go_pair(chunk, j):
        return pltpu.make_async_remote_copy(
            send_pair.at[chunk, seat(j)], pair_in.at[chunk, seat(j)], sf_sem.at[chunk, j],
            rf_sem.at[chunk, j], device_id={"seq": toward(j)}, device_id_type=MESH,
        )

    def back_pair(chunk, j):
        return pltpu.make_async_remote_copy(
            pair_out.at[chunk, seat(j)], ret_pair.at[chunk, seat(j)], sb_sem.at[chunk, j],
            rb_sem.at[chunk, j], device_id={"seq": origin(j)}, device_id_type=MESH,
        )

    near_seats = DIRECT * GROUP

    def columns(chunk, side):
        return pl.ds(pl.multiple_of(side * half + chunk * quarter, quarter), quarter)

    batch = ns // 4

    def pick(chunk, q):
        at = pl.ds(q * batch * slots, batch * slots)
        got = jnp.dot(
            picks[at, :], every[chunk, par], preferred_element_type=F32
        ).astype(BF16)
        send[chunk, at, :] = got
        if q == 0:
            own_in[chunk, 0:slots, :] = got[0:slots]
            near = pl.ds(0, near_seats * slots)
            got = jnp.dot(
                picks[near, :], every[chunk, 1 - par], preferred_element_type=F32
            ).astype(BF16)
            send_pair[chunk, near, :] = got
            pair_in[chunk, 0:slots, :] = got[0:slots]

    def go(chunk, q):
        @pl.loop(max(1, q * batch), (q + 1) * batch)
        def _(j):
            go_copy(chunk, j).start()

        if q == 0:

            @pl.loop(1, near_seats)
            def _(j):
                go_pair(chunk, j).start()

    for ring in rings:
        ring.start()
    for t in range(1, nd // 2):
        for ring in rings:
            ring.advance(t)
    for chunk in range(2):
        rings[chunk].advance(nd // 2)
        for q in range(4):
            pick(chunk, q)
            if q:
                go(chunk, q - 1)
        go(chunk, 3)
    for c in later:
        c.wait()

    def nt(a, w):
        return lax.dot_general(a, w, (((1,), (1,)), ((), ())), preferred_element_type=F32)

    def silu(a):
        return a / (1.0 + jnp.exp(-a))

    def arrive(chunk, g):
        for i in range(GROUP):
            j = g * GROUP + i

            @pl.when(j > 0)
            def _():
                go_copy(chunk, j).wait_recv()

            @pl.when((j > 0) & (g < DIRECT))
            def _():
                go_pair(chunk, j).wait_recv()

        @pl.when(g >= DIRECT)
        def _():
            swap_copy(chunk, g).start()

    quads = [(chunk, side) for chunk in range(2) for side in range(2)]
    share = tokens // 4

    @pl.loop(0, groups)
    def _(g):
        arrive(0, g)

        @pl.when((g >= 1) & (g <= 4))
        def _():
            at = pl.ds(pl.multiple_of((g - 1) * share, share), share)
            gate_act = jnp.zeros((share, vg.shape[0]), F32)
            up_act = jnp.zeros((share, vg.shape[0]), F32)
            weight = jnp.zeros((share, 1), F32)
            for chunk, side in quads:
                a = every[chunk, side, at, :]
                where = pl.ds(place_of(chunk, side), quarter)
                gate_act += nt(a, vg[:, where])
                up_act += nt(a, vu[:, where])
                weight += jnp.sum(
                    a.astype(F32) * vecs[1:2, where], axis=-1, keepdims=True
                )
            hidden = (silu(gate_act) * up_act).astype(BF16)
            weight = 1.0 / (1.0 + jnp.exp(-weight))
            for chunk, side in quads:
                total[chunk, side, at, :] = weight * jnp.dot(
                    hidden, vd[:, pl.ds(place_of(chunk, side), quarter)],
                    preferred_element_type=F32,
                )

    def down(chunk, g):
        hidden = act[span_of(g), :]
        pair_out[chunk, span_of(g), :] = jnp.dot(
            hidden, wd[:, columns(chunk, 1 - par)], preferred_element_type=F32
        ).astype(BF16)
        own_part[span_of(g), :] = jnp.dot(
            hidden, wd[:, columns(chunk, par)], preferred_element_type=F32
        )

        @pl.when(g >= DIRECT)
        def _():
            part_copy(chunk, g).start()

    def join(chunk, g):
        @pl.when(g >= DIRECT)
        def _():
            part_copy(chunk, g).wait_recv()
            back[chunk, span_of(g), :] = (
                own_part[span_of(g), :] + pair_part[chunk, span_of(g), :].astype(F32)
            ).astype(BF16)

        @pl.when(g < DIRECT)
        def _():
            back[chunk, span_of(g), :] = own_part[span_of(g), :].astype(BF16)

    def leave(chunk, g):
        for i in range(GROUP):
            j = g * GROUP + i

            @pl.when(j > 0)
            def _():
                back_copy(chunk, j).start()

            @pl.when((j > 0) & (g < DIRECT))
            def _():
                back_pair(chunk, j).start()

            @pl.when(j == 0)
            def _():
                ret[chunk, 0:slots, :] = back[chunk, 0:slots, :]
                ret_pair[chunk, 0:slots, :] = pair_out[chunk, 0:slots, :]

    def combine(chunk, g):
        for i in range(GROUP):
            j = g * GROUP + i

            @pl.when(j > 0)
            def _():
                back_copy(chunk, j).wait_recv()

            @pl.when((j > 0) & (g < DIRECT))
            def _():
                back_pair(chunk, j).wait_recv()

        def mix(rows_in):
            return lax.dot_general(
                mixes[span_of(g), :], rows_in[chunk, span_of(g), :], (((0,), (0,)), ((), ())),
                preferred_element_type=F32,
            )

        total[chunk, par] += mix(ret)

        @pl.when(g < DIRECT)
        def _():
            total[chunk, 1 - par] += mix(ret_pair)

    @pl.loop(0, groups + 2)
    def _(step):
        @pl.when(step < groups)
        def _():
            arrive(1, step)

        @pl.when(step >= 2)
        def _():
            join(0, step - 2)

        @pl.when((step >= 1) & (step <= groups))
        def _():
            g = step - 1
            gate_act = jnp.zeros((group_slots, wg.shape[0]), F32)
            up_act = jnp.zeros((group_slots, wg.shape[0]), F32)
            for chunk in range(2):
                @pl.when(g >= DIRECT)
                def _():
                    swap_copy(chunk, g).wait_recv()

                for rows_in, side in ((own_in, par), (pair_in, 1 - par)):
                    a = rows_in[chunk, span_of(g), :]
                    gate_act += nt(a, wg[:, columns(chunk, side)])
                    up_act += nt(a, wu[:, columns(chunk, side)])
            act[span_of(g), :] = (silu(gate_act) * up_act).astype(BF16)
            down(0, g)

        @pl.when(step >= 2)
        def _():
            leave(0, step - 2)

    @pl.loop(0, groups)
    def _(g):
        down(1, g)

    @pl.loop(0, groups // 2)
    def _(g):
        join(1, g)
        leave(1, g)
        combine(0, 2 * g)
        combine(0, 2 * g + 1)

    last = nd // 2

    def own(index, sub):
        return pl.ds(pl.multiple_of(index * rows + sub * part, 16), part)

    def used(way, t, sub):
        return t < last or (t == last and sub == way)

    def hop(chunk, way, t, sub):
        sign = 1 - 2 * way
        return pltpu.make_async_remote_copy(
            passed.at[chunk, way, t - 1, sub], landed.at[chunk, way, t - 1, sub],
            s2_sem.at[chunk, way, t - 1, sub], r2_sem.at[chunk, way, t - 1, sub],
            device_id={"dp": lax.rem(d + sign + nd, nd)}, device_id_type=MESH,
        )

    def target(way, t):
        return lax.rem(d + (1 - 2 * way) * t + nd, nd)

    def reduce_step(chunk, t):
        for sub in range(2):
            for way in range(2):
                if not used(way, t, sub):
                    continue
                term = total[chunk, :, own(target(way, t), sub), :]
                if used(way, t + 1, sub):
                    hop(chunk, way, t + 1, sub).wait_recv()
                    term = term + landed[chunk, way, t, sub].astype(F32)
                passed[chunk, way, t - 1, sub] = term.astype(BF16)
                hop(chunk, way, t, sub).start()

    def settle(chunk):
        for sub in range(2):
            for way in range(2):
                hop(chunk, way, 1, sub).wait_recv()
            at = pl.ds(sub * part, part)
            sums = (
                total[chunk, :, own(d, sub), :]
                + landed[chunk, 0, 0, sub].astype(F32)
                + landed[chunk, 1, 0, sub].astype(F32)
            )
            for side in range(2):
                where = pl.ds(place_of(chunk, side), quarter)
                out_ref[at, where] = residual[at, where].astype(F32) + sums[side]

    for t in range(last, 0, -1):
        reduce_step(0, t)

        @pl.loop(
            groups // 2 + (last - t) * groups // (2 * last),
            groups // 2 + (last - t + 1) * groups // (2 * last),
        )
        def _(g):
            join(1, g)
            leave(1, g)

    @pl.loop(0, groups)
    def _(g):
        combine(1, g)

    for t in range(last, 0, -1):
        reduce_step(1, t)
    settle(0)
    settle(1)

    for chunk in range(2):
        for way in range(2):
            for sub in range(2):
                for t in range(1, last + 1):
                    if used(way, t, sub):
                        hop(chunk, way, t, sub).wait_send()
        rings[chunk].finish()

        @pl.loop(1, ns)
        def _(j):
            go_copy(chunk, j).wait_send()
            back_copy(chunk, j).wait_send()

        @pl.loop(1, near_seats)
        def _(j):
            go_pair(chunk, j).wait_send()
            back_pair(chunk, j).wait_send()

        @pl.loop(DIRECT, groups)
        def _(g):
            swap_copy(chunk, g).wait_send()
            part_copy(chunk, g).wait_send()

    weights.finish()

    @pl.loop(1, ns)
    def _(j):
        for c in in_copies(j, toward(j), s):
            c.wait_send()

    @pl.loop(0, chips)
    def _(chip):
        @pl.when(owner(chip) != s)
        def _():
            out_copy(chip, s).wait_send()

    @pl.loop(0, nd)
    def _(index):
        sum_copy(index).wait_send()


def run_layer(docs, ids, gates, gain, score, qk, v, resid, out_weight, expert_weights, shared_weights, ns, nd):
    rows, width = v.shape
    length = rows * ns
    tokens = rows * nd
    half = width // 2
    quarter = half // 2
    slots = ns * nd * CAP
    groups = ns // GROUP
    near = DIRECT * GROUP * nd * CAP
    hidden = expert_weights[0].shape[1]
    shared_hidden = shared_weights[0].shape[0]
    dma = pltpu.SemaphoreType.DMA
    vmem = pl.BlockSpec(memory_space=pltpu.VMEM)
    anyspace = pl.BlockSpec(memory_space=pl.ANY)

    def buf(*shape):
        return pltpu.VMEM(shape, BF16)

    def wide(*shape):
        return pltpu.VMEM(shape, F32)

    ring = dma((2, nd // 2, 2))
    rings = dma((2, 2, nd // 2, 2))
    per_seat = dma((2, ns))
    per_group = dma((2, groups))
    per_near = dma((2, DIRECT * GROUP))
    return pl.pallas_call(
        functools.partial(layer_kernel, ns, nd),
        out_shape=jax.ShapeDtypeStruct((rows, width), F32),
        in_specs=[vmem] * 5 + [anyspace] * 10,
        out_specs=vmem,
        scratch_shapes=[buf(2, rows, width), buf(rows, width), buf(rows, width)]
        + [buf(hidden, width)] * 3
        + [buf(shared_hidden, width)] * 3
        + [wide(2, width), wide(length, HD)]
        + [wide(2 * TOPK, 2 * rows), wide(2 * TOPK, 2 * rows), wide(nd, 2 * TOPK, 2 * rows)]
        + [buf(length, HD)] * 4
        + [
            buf(rows * CORES, width // CORES),
            buf(nd, width // CORES, out_weight.shape[1]),
            wide(rows, width), wide(rows, width), wide(rows, width),
            buf(rows, width),
            buf(2, 2, rows, quarter),
            buf(2, 2, tokens, quarter),
            buf(slots, tokens), buf(slots, tokens),
            buf(2, slots, quarter), buf(2, slots, quarter), buf(2, slots, quarter),
            buf(slots, hidden),
            buf(2, slots, quarter), buf(2, slots, quarter),
            wide(slots, quarter),
            buf(2, slots, quarter), buf(2, slots, quarter),
            buf(2, near, quarter), buf(2, near, quarter),
            wide(2, 2, tokens, quarter),
            buf(2, 2, nd // 2, 2, 2, rows // 2, quarter),
            buf(2, 2, nd // 2, 2, 2, rows // 2, quarter),
            dma((10,)), dma((3,)), dma((3, ns)), dma((3, ns)), dma((ns // CORES,)),
            dma((ns // CORES,)), dma((nd,)), dma((nd,)), dma((nd,)), dma((nd,)),
            ring, ring, rings, rings,
            per_seat, per_seat, per_group, per_group, per_group, per_group, per_seat, per_seat,
            per_near, per_near, per_near, per_near, rings, rings,
        ],
        compiler_params=pltpu.CompilerParams(
            collective_id=1, has_side_effects=True, vmem_limit_bytes=67043328
        ),
        cost_estimate=pl.CostEstimate(
            flops=12 * slots * half * hidden, bytes_accessed=8 * slots * half, transcendentals=0
        ),
        name="layer",
    )(docs, ids, gates, gain, score, qk, v, resid, out_weight, *expert_weights, *shared_weights)


def body(
    resid,
    queries_keys,
    values,
    doc_ids,
    out_weight,
    norm_gain,
    expert_ids,
    gate_vals,
    expert_gate,
    expert_up,
    expert_down,
    shared_gate,
    shared_up,
    shared_down,
    shared_score,
):
    ns = lax.axis_size("seq")
    nd = lax.axis_size("dp")
    tokens = resid.shape[1]
    width = resid.shape[2]
    out = run_layer(
        doc_ids,
        expert_ids[0].T,
        gate_vals[0].T,
        norm_gain.reshape(-1, HD),
        shared_score.reshape(-1, HD),
        queries_keys.reshape(2, tokens, width),
        values[0],
        resid[0],
        out_weight,
        (expert_gate.transpose(0, 2, 1), expert_up.transpose(0, 2, 1), expert_down),
        (shared_gate.T, shared_up.T, shared_down),
        ns,
        nd,
    )
    return out.astype(BF16)[None]


def solution(mesh):
    placed = (
        P(("groups", "dp"), "seq", None),
        P(None, ("groups", "dp"), "seq", None),
        P(("groups", "dp"), "seq", None),
        P(("groups", "dp"), None),
        P(None, "dp"),
        P(),
        P(("groups", "dp"), "seq", None),
        P(("groups", "dp"), "seq", None),
        P(("seq", "dp"), None, None),
        P(("seq", "dp"), None, None),
        P(("seq", "dp"), None, None),
        P(None, "dp"),
        P(None, "dp"),
        P("dp", None),
        P(),
    )
    return jax.shard_map(
        body,
        mesh=mesh,
        in_specs=placed,
        out_specs=P(("groups", "dp"), "seq", None),
        check_vma=False,
    )
```

```python
import functools
import math

import jax
import jax.numpy as jnp
from jax import lax
from jax.experimental import pallas as pl
from jax.experimental.pallas import tpu as pltpu
from jax.sharding import PartitionSpec as P

HD = 128
TOPK = 4
SPLIT = 4
CAP = 10
GROUP = 2
CORES = 2
DIRECT = (1, 2)

norm_eps = 1e-06
MESH = pl.DeviceIdType.MESH
F32 = jnp.float32
BF16 = jnp.bfloat16


def ring_delta(j):
    return ((j + 1) // 2) * (2 * (j % 2) - 1)


class Ring:
    def __init__(self, nd, axis, source, place, send_sem, recv_sem):
        self.nd, self.axis, self.last = nd, axis, nd // 2
        self.source, self.place = source, place
        self.send_sem, self.recv_sem = send_sem, recv_sem
        self.me = lax.axis_index(axis)

    def behind(self, t, way):
        return lax.rem(self.me - (1 - 2 * way) * t + self.nd, self.nd)

    def hop(self, way, t, sub):
        index = self.behind(t - 1, way)
        src = self.source(sub) if t == 1 else self.place(index, sub)
        return pltpu.make_async_remote_copy(
            src, self.place(index, sub), self.send_sem.at[way, t - 1, sub],
            self.recv_sem.at[way, t - 1, sub],
            device_id={self.axis: self.behind(-1, way)}, device_id_type=MESH,
        )

    def hops(self, t):
        return [
            (way, t, sub)
            for sub in range(2)
            for way in range(2)
            if t < self.last or (t == self.last and sub == way)
        ]

    def start(self):
        for h in self.hops(1):
            self.hop(*h).start()

    def advance(self, t):
        following = self.hops(t + 1)
        for way, _, sub in self.hops(t):
            self.hop(way, t, sub).wait_recv()
            if (way, t + 1, sub) in following:
                self.hop(way, t + 1, sub).start()

    def arrived(self, t):
        return [self.behind(t, 0), self.behind(t, 1)] if t < self.last else [self.behind(t, 0)]

    def finish(self):
        for t in range(1, self.last + 1):
            for h in self.hops(t):
                self.hop(*h).wait_send()


def greet(axes):
    barrier = pltpu.get_barrier_semaphore()
    for axis, size in axes.items():
        me = lax.axis_index(axis)

        @pl.loop(1, size)
        def _(k):
            pl.semaphore_signal(
                barrier, inc=1, device_id={axis: lax.rem(me + k, size)}, device_id_type=MESH
            )

    pl.semaphore_wait(barrier, sum(axes.values()) - len(axes))


def layer_kernel(
    ns, nd, docs_ref, ids_ref, gates_ref, gain_ref, score_ref, qk_hbm, v_hbm, resid_hbm, w_hbm, eg_hbm, eu_hbm, ed_hbm,
    sg_hbm, su_hbm, sd_hbm, out_ref,
    qk, v, resid, wg, wu, wd, vg, vu, vd, vecs, dcol, spread, info, routes, qh, kh, vh, att, mixed, wall, own_sum,
    send_sum, got_sum, residual, normed, every, picks, mixes, send, own_in, pair_in, act, pair_out,
    pair_part, own_part, back, ret, send_pair, ret_pair, total, landed, passed,
    w_sem, local_sem, si_sem, ri_sem, so_sem, ro_sem, sd_sem, rd_sem, sp_sem, rp_sem, sw_sem, rw_sem,
    sg_sem, rg_sem, sy_sem, ry_sem, sx_sem, rx_sem, sq_sem, rq_sem, sr_sem, rr_sem, sf_sem, rf_sem, sb_sem, rb_sem,
    s2_sem, r2_sem,
):
    s = lax.axis_index("seq")
    d = lax.axis_index("dp")
    rows, width = v.shape
    length = rows * ns
    tokens = rows * nd
    core = lax.rem(s, CORES)
    chips = ns // CORES
    depth = width // CORES
    block = width // nd
    chip_rows = rows * CORES
    half = width // 2
    quarter = half // 2
    lanes = 2 * rows

    first = [
        pltpu.make_async_copy(src, dst, w_sem.at[i])
        for i, (src, dst) in enumerate(
            (
                (qk_hbm, qk), (v_hbm, v),
                (w_hbm.at[pl.ds(pl.multiple_of(core * depth, 16), depth)], wall.at[d]),
                (resid_hbm, resid),
            )
        )
    ]
    later = [
        pltpu.make_async_copy(src, dst, w_sem.at[4 + i])
        for i, (src, dst) in enumerate(
            (
                (sg_hbm, vg), (su_hbm, vu), (sd_hbm, vd),
                (eg_hbm.at[0], wg), (eu_hbm.at[0], wu), (ed_hbm.at[0], wd),
            )
        )
    ]
    for c in first:
        c.start()

    experts = ns * nd // SPLIT
    lane = lax.broadcasted_iota(jnp.int32, (1, lanes), 1)
    valid = (lane >= lax.rem(d, 2) * rows) & (lane < (lax.rem(d, 2) + 1) * rows)
    expert = lax.broadcasted_iota(jnp.int32, (experts, lanes), 0).astype(F32)
    spread[...] = jnp.zeros_like(spread)
    spread[0:TOPK, 0:rows] = ids_ref[...].astype(F32)
    spread[TOPK:, 0:rows] = gates_ref[...]
    odd = lax.rem(d, 2).astype(F32)
    both = spread[...] * (1.0 - odd) + pltpu.roll(spread[...], rows, 1) * odd
    chosen_ids = [jnp.where(valid, both[k : k + 1, :], -1.0) for k in range(TOPK)]
    named = [ids == expert for ids in chosen_ids]
    earlier = lax.broadcasted_iota(jnp.int32, (lanes, lanes), 0) < lax.broadcasted_iota(
        jnp.int32, (lanes, lanes), 1
    )
    counts = jnp.dot(
        jnp.where(functools.reduce(jnp.logical_or, named), 1.0, 0.0).astype(BF16),
        jnp.where(earlier, 1.0, 0.0).astype(BF16),
        preferred_element_type=F32,
    )
    for k in range(TOPK):
        rank = jnp.sum(jnp.where(named[k], counts, 0.0), axis=0, keepdims=True)
        info[k : k + 1, :] = jnp.where(valid, chosen_ids[k] * CAP + rank, 0.0)
    info[TOPK:, :] = both[TOPK:, :]
    score = score_ref[...].astype(F32)
    for i in range(width // HD):
        vecs[0:1, i * HD : (i + 1) * HD] = gain_ref[i : i + 1, :]
        vecs[1:2, i * HD : (i + 1) * HD] = score[i : i + 1, :]
    routes[d] = info[...]
    docs = docs_ref[...].astype(F32)
    for i in range(length // HD):
        tile = jnp.broadcast_to(docs[:, i * HD : (i + 1) * HD], (HD, HD))
        dcol[i * HD : (i + 1) * HD, :] = tile.T

    greet({"seq": ns, "dp": nd})
    first[0].wait()
    first[1].wait()

    def own_rows(ref, t):
        return ref.at[pl.ds(pl.multiple_of(t * rows, 16), rows)]

    def cols(t):
        return pl.ds(pl.multiple_of(t * HD, HD), HD)

    def info_copy(to, slot):
        return pltpu.make_async_remote_copy(
            info, routes.at[slot], sd_sem.at[to], rd_sem.at[slot],
            device_id={"dp": to}, device_id_type=MESH,
        )

    def pieces(t):
        return (
            (qk.at[0, :, cols(t)], qh),
            (qk.at[1, :, cols(t)], kh),
            (v.at[:, cols(t)], vh),
        )

    def in_copies(j, to, slot):
        return [
            pltpu.make_async_remote_copy(
                src, own_rows(dst, slot), si_sem.at[c, j], ri_sem.at[c, j],
                device_id={"seq": to}, device_id_type=MESH,
            )
            for c, (src, dst) in enumerate(pieces(to))
        ]

    def peer(j, sign):
        chip = lax.rem(s // CORES + sign * ring_delta(j // CORES) + chips, chips)
        return chip * CORES + lax.rem(core + j, CORES)

    def toward(j):
        return peer(j, -1)

    def origin(j):
        return peer(j, 1)

    @pl.loop(1, ns)
    def _(j):
        for c in in_copies(j, toward(j), s):
            c.start()

    w_part = depth // 2
    weights = Ring(
        nd, "dp",
        lambda sub: wall.at[d, pl.ds(sub * w_part, w_part)],
        lambda index, sub: wall.at[index, pl.ds(sub * w_part, w_part)],
        sw_sem, rw_sem,
    )
    first[2].wait()
    weights.start()

    @pl.loop(1, nd)
    def _(k):
        info_copy(lax.rem(d + k, nd), d).start()

    for c in later:
        c.start()
    local = [
        pltpu.make_async_copy(src, own_rows(dst, s), local_sem.at[c])
        for c, (src, dst) in enumerate(pieces(s))
    ]
    for c in local:
        c.start()
    for c in local:
        c.wait()

    def receive(j):
        frm = origin(j)
        for c in in_copies(j, frm, frm):
            c.wait_recv()

    @pl.loop(1, ns // 2)
    def _(j):
        receive(j)

    weights.advance(1)

    @pl.loop(ns // 2, ns)
    def _(j):
        receive(j)

    per_core = ns // CORES
    mate = s + 1 - 2 * core

    def owner(chip):
        return chip * CORES + s // per_core

    def out_copy(chip, head):
        return pltpu.make_async_remote_copy(
            att.at[pl.ds(pl.multiple_of(chip * chip_rows, 16), chip_rows)],
            mixed.at[:, cols(lax.rem(head, per_core))], so_sem.at[chip],
            ro_sem.at[lax.rem(head, per_core)],
            device_id={"seq": owner(chip)}, device_id_type=MESH,
        )

    scale = 1.0 / math.sqrt(HD)
    step_rows = 2 * chip_rows
    for i in range(length // step_rows):
        upto = (i + 1) * step_rows
        span = pl.ds(i * step_rows, step_rows)
        scores = lax.dot_general(
            qh[span, :], kh[0:upto, :], (((1,), (1,)), ((), ())), preferred_element_type=F32
        ) * scale
        at = lax.broadcasted_iota(jnp.int32, (step_rows, upto), 0) + i * step_rows
        key_at = lax.broadcasted_iota(jnp.int32, (step_rows, upto), 1)
        mine = jnp.concatenate([dcol[span, :]] * (upto // HD), axis=1)
        allowed = (key_at <= at) & (mine == docs[:, 0:upto])
        scores = jnp.where(allowed, scores, -1e30)
        lifted = jnp.exp(scores - jnp.max(scores, axis=-1, keepdims=True))
        probs = (lifted / jnp.sum(lifted, axis=-1, keepdims=True)).astype(BF16)
        att[span, :] = jnp.dot(probs, vh[0:upto, :], preferred_element_type=F32).astype(BF16)
        for chip in (2 * i, 2 * i + 1):

            @pl.when(owner(chip) != s)
            def _():
                out_copy(chip, s).start()

            @pl.when(owner(chip) == s)
            def _():
                mixed[:, cols(lax.rem(s, per_core))] = att[
                    pl.ds(chip * chip_rows, chip_rows), :
                ]

        if i == 1:
            weights.advance(2)

    slots = nd * CAP
    per_seq = nd // SPLIT
    first_expert = d // SPLIT

    @pl.loop(1, nd)
    def _(k):
        other = lax.rem(d + k, nd)
        info_copy(other, other).wait_send()
        info_copy(other, other).wait_recv()

    tiles = [routes[2 * m] + routes[2 * m + 1] for m in range(nd // 2)]
    code = jnp.concatenate([tile[:TOPK] for tile in tiles], axis=1)
    gates = jnp.concatenate([tile[TOPK:] for tile in tiles], axis=1)
    slot = lax.broadcasted_iota(jnp.int32, (slots, tokens), 0).astype(F32)
    token = lax.broadcasted_iota(jnp.int32, (slots, tokens), 1).astype(F32)
    slot_block = jnp.floor((slot + 0.5) * (1.0 / CAP))
    token_block = jnp.floor((token + 0.5) * (1.0 / rows))
    ranks = jnp.where(slot_block == token_block, slot - slot_block * CAP, -1e6)

    def seat(j):
        return pl.ds(pl.multiple_of(j * slots, 16), slots)

    @pl.loop(0, ns)
    def _(j):
        base = ((toward(j) * per_seq + first_expert) * CAP).astype(F32)
        hits = [code[k : k + 1, :] - base == ranks for k in range(TOPK)]
        hit = functools.reduce(jnp.logical_or, hits)
        picks[seat(j), :] = jnp.where(hit, 1.0, 0.0).astype(BF16)
        mixes[seat(j), :] = functools.reduce(
            jnp.add, [jnp.where(hits[k], gates[k : k + 1, :], 0.0) for k in range(TOPK)]
        ).astype(BF16)

    weights.advance(3)

    @pl.loop(0, per_core)
    def _(h):
        @pl.when(core * per_core + h != s)
        def _():
            out_copy(0, h).wait_recv()

    def sum_copy(index):
        at = pl.ds(pl.multiple_of(index * block, block), block)
        return pltpu.make_async_remote_copy(
            send_sum.at[:, at], got_sum.at[:, at], sp_sem.at[index], rp_sem.at[index],
            device_id={"seq": mate}, device_id_type=MESH,
        )

    def project(index):
        at = pl.ds(pl.multiple_of(index * block, block), block)
        theirs = mixed[pl.ds(pl.multiple_of((1 - core) * rows, 16), rows), :]
        mine = mixed[pl.ds(pl.multiple_of(core * rows, 16), rows), :]
        send_sum[:, at] = jnp.dot(theirs, wall[index], preferred_element_type=F32)
        own_sum[:, at] = jnp.dot(mine, wall[index], preferred_element_type=F32)
        sum_copy(index).start()

    project(d)
    for t in range(1, nd // 2 + 1):
        if t >= 4:
            weights.advance(t)
        for index in weights.arrived(t):
            project(index)

    @pl.loop(0, nd)
    def _(index):
        sum_copy(index).wait_recv()

    first[3].wait()
    projected = (own_sum[...] + got_sum[...]).astype(BF16)
    summed = (resid[...].astype(F32) + projected.astype(F32)).astype(BF16)
    residual[...] = summed
    stream = summed.astype(F32)
    scaled = (
        stream
        * lax.rsqrt(jnp.mean(stream * stream, axis=-1, keepdims=True) + norm_eps)
        * vecs[0:1, :]
    ).astype(BF16)

    def place_of(chunk, side):
        return side * half + chunk * quarter

    mine_at = pl.ds(pl.multiple_of(d * rows, 16), rows)
    for chunk in range(2):
        for side in range(2):
            at = place_of(chunk, side)
            normed[chunk, side] = scaled[:, at : at + quarter]
            every[chunk, side, mine_at, :] = scaled[:, at : at + quarter]
    part = rows // 2

    def gather(chunk):
        return Ring(
            nd, "dp",
            lambda sub: normed.at[chunk, :, pl.ds(sub * part, part)],
            lambda index, sub: every.at[
                chunk, :, pl.ds(pl.multiple_of(index * rows + sub * part, 16), part)
            ],
            sg_sem.at[chunk], rg_sem.at[chunk],
        )

    rings = [gather(0), gather(1)]

    par = lax.rem(d, 2)
    partner = d + 1 - 2 * par
    group_slots = GROUP * slots
    groups = ns // GROUP

    def span_of(g):
        return pl.ds(pl.multiple_of(g * group_slots, 16), group_slots)

    def go_copy(chunk, j):
        return pltpu.make_async_remote_copy(
            send.at[chunk, seat(j)], own_in.at[chunk, seat(j)], sy_sem.at[chunk, j],
            ry_sem.at[chunk, j], device_id={"seq": toward(j)}, device_id_type=MESH,
        )

    def swap_copy(chunk, g):
        return pltpu.make_async_remote_copy(
            own_in.at[chunk, span_of(g)], pair_in.at[chunk, span_of(g)], sx_sem.at[chunk, g],
            rx_sem.at[chunk, g], device_id={"dp": partner}, device_id_type=MESH,
        )

    def part_copy(chunk, g):
        return pltpu.make_async_remote_copy(
            pair_out.at[chunk, span_of(g)], pair_part.at[chunk, span_of(g)], sq_sem.at[chunk, g],
            rq_sem.at[chunk, g], device_id={"dp": partner}, device_id_type=MESH,
        )

    def back_copy(chunk, j):
        return pltpu.make_async_remote_copy(
            back.at[chunk, seat(j)], ret.at[chunk, seat(j)], sr_sem.at[chunk, j],
            rr_sem.at[chunk, j], device_id={"seq": origin(j)}, device_id_type=MESH,
        )

    def go_pair(chunk, j):
        return pltpu.make_async_remote_copy(
            send_pair.at[chunk, seat(j)], pair_in.at[chunk, seat(j)], sf_sem.at[chunk, j],
            rf_sem.at[chunk, j], device_id={"seq": toward(j)}, device_id_type=MESH,
        )

    def back_pair(chunk, j):
        return pltpu.make_async_remote_copy(
            pair_out.at[chunk, seat(j)], ret_pair.at[chunk, seat(j)], sb_sem.at[chunk, j],
            rb_sem.at[chunk, j], device_id={"seq": origin(j)}, device_id_type=MESH,
        )

    near_seats = [count * GROUP for count in DIRECT]

    def columns(chunk, side):
        return pl.ds(pl.multiple_of(side * half + chunk * quarter, quarter), quarter)

    batch = ns // 4

    def pick(chunk, q):
        at = pl.ds(q * batch * slots, batch * slots)
        got = jnp.dot(
            picks[at, :], every[chunk, par], preferred_element_type=F32
        ).astype(BF16)
        send[chunk, at, :] = got
        if q == 0:
            own_in[chunk, 0:slots, :] = got[0:slots]
            near = pl.ds(0, near_seats[chunk] * slots)
            got = jnp.dot(
                picks[near, :], every[chunk, 1 - par], preferred_element_type=F32
            ).astype(BF16)
            send_pair[chunk, near, :] = got
            pair_in[chunk, 0:slots, :] = got[0:slots]

    def go(chunk, q):
        @pl.loop(max(1, q * batch), (q + 1) * batch)
        def _(j):
            go_copy(chunk, j).start()

        if q == 0:

            @pl.loop(1, near_seats[chunk])
            def _(j):
                go_pair(chunk, j).start()

    for ring in rings:
        ring.start()
    for t in range(1, nd // 2):
        for ring in rings:
            ring.advance(t)
    for chunk in range(2):
        rings[chunk].advance(nd // 2)
        for q in range(4):
            pick(chunk, q)
            if q:
                go(chunk, q - 1)
        go(chunk, 3)
    for c in later:
        c.wait()

    def nt(a, w):
        return lax.dot_general(a, w, (((1,), (1,)), ((), ())), preferred_element_type=F32)

    def silu(a):
        return a / (1.0 + jnp.exp(-a))

    def arrive(chunk, g):
        for i in range(GROUP):
            j = g * GROUP + i

            @pl.when(j > 0)
            def _():
                go_copy(chunk, j).wait_recv()

            @pl.when((j > 0) & (g < DIRECT[chunk]))
            def _():
                go_pair(chunk, j).wait_recv()

        @pl.when(g >= DIRECT[chunk])
        def _():
            swap_copy(chunk, g).start()

    quads = [(chunk, side) for chunk in range(2) for side in range(2)]
    share = tokens // 4

    @pl.loop(0, groups)
    def _(g):
        arrive(0, g)

        @pl.when((g >= 1) & (g <= 4))
        def _():
            at = pl.ds(pl.multiple_of((g - 1) * share, share), share)
            gate_act = jnp.zeros((share, vg.shape[0]), F32)
            up_act = jnp.zeros((share, vg.shape[0]), F32)
            weight = jnp.zeros((share, 1), F32)
            for chunk, side in quads:
                a = every[chunk, side, at, :]
                where = pl.ds(place_of(chunk, side), quarter)
                gate_act += nt(a, vg[:, where])
                up_act += nt(a, vu[:, where])
                weight += jnp.sum(
                    a.astype(F32) * vecs[1:2, where], axis=-1, keepdims=True
                )
            hidden = (silu(gate_act) * up_act).astype(BF16)
            weight = 1.0 / (1.0 + jnp.exp(-weight))
            for chunk, side in quads:
                total[chunk, side, at, :] = weight * jnp.dot(
                    hidden, vd[:, pl.ds(place_of(chunk, side), quarter)],
                    preferred_element_type=F32,
                )

    def down(chunk, g):
        hidden = act[span_of(g), :]
        pair_out[chunk, span_of(g), :] = jnp.dot(
            hidden, wd[:, columns(chunk, 1 - par)], preferred_element_type=F32
        ).astype(BF16)
        own_part[span_of(g), :] = jnp.dot(
            hidden, wd[:, columns(chunk, par)], preferred_element_type=F32
        )

        @pl.when(g >= DIRECT[chunk])
        def _():
            part_copy(chunk, g).start()

    def join(chunk, g):
        @pl.when(g >= DIRECT[chunk])
        def _():
            part_copy(chunk, g).wait_recv()
            back[chunk, span_of(g), :] = (
                own_part[span_of(g), :] + pair_part[chunk, span_of(g), :].astype(F32)
            ).astype(BF16)

        @pl.when(g < DIRECT[chunk])
        def _():
            back[chunk, span_of(g), :] = own_part[span_of(g), :].astype(BF16)

    def leave(chunk, g):
        for i in range(GROUP):
            j = g * GROUP + i

            @pl.when(j > 0)
            def _():
                back_copy(chunk, j).start()

            @pl.when((j > 0) & (g < DIRECT[chunk]))
            def _():
                back_pair(chunk, j).start()

            @pl.when(j == 0)
            def _():
                ret[chunk, 0:slots, :] = back[chunk, 0:slots, :]
                ret_pair[chunk, 0:slots, :] = pair_out[chunk, 0:slots, :]

    def combine(chunk, g):
        for i in range(GROUP):
            j = g * GROUP + i

            @pl.when(j > 0)
            def _():
                back_copy(chunk, j).wait_recv()

            @pl.when((j > 0) & (g < DIRECT[chunk]))
            def _():
                back_pair(chunk, j).wait_recv()

        def mix(rows_in):
            return lax.dot_general(
                mixes[span_of(g), :], rows_in[chunk, span_of(g), :], (((0,), (0,)), ((), ())),
                preferred_element_type=F32,
            )

        total[chunk, par] += mix(ret)

        @pl.when(g < DIRECT[chunk])
        def _():
            total[chunk, 1 - par] += mix(ret_pair)

    @pl.loop(0, groups + 2)
    def _(step):
        @pl.when(step < groups)
        def _():
            arrive(1, step)

        @pl.when(step >= 2)
        def _():
            join(0, step - 2)

        @pl.when((step >= 1) & (step <= groups))
        def _():
            g = step - 1
            gate_act = jnp.zeros((group_slots, wg.shape[0]), F32)
            up_act = jnp.zeros((group_slots, wg.shape[0]), F32)
            for chunk in range(2):
                @pl.when(g >= DIRECT[chunk])
                def _():
                    swap_copy(chunk, g).wait_recv()

                for rows_in, side in ((own_in, par), (pair_in, 1 - par)):
                    a = rows_in[chunk, span_of(g), :]
                    gate_act += nt(a, wg[:, columns(chunk, side)])
                    up_act += nt(a, wu[:, columns(chunk, side)])
            act[span_of(g), :] = (silu(gate_act) * up_act).astype(BF16)
            down(0, g)

        @pl.when(step >= 2)
        def _():
            leave(0, step - 2)

    @pl.loop(0, groups)
    def _(g):
        down(1, g)

    @pl.loop(0, groups)
    def _(g):
        join(1, g)
        leave(1, g)
        combine(0, g)

    last = nd // 2

    def own(index, sub):
        return pl.ds(pl.multiple_of(index * rows + sub * part, 16), part)

    def used(way, t, sub):
        return t < last or (t == last and sub == way)

    def hop(chunk, way, t, sub):
        sign = 1 - 2 * way
        return pltpu.make_async_remote_copy(
            passed.at[chunk, way, t - 1, sub], landed.at[chunk, way, t - 1, sub],
            s2_sem.at[chunk, way, t - 1, sub], r2_sem.at[chunk, way, t - 1, sub],
            device_id={"dp": lax.rem(d + sign + nd, nd)}, device_id_type=MESH,
        )

    def target(way, t):
        return lax.rem(d + (1 - 2 * way) * t + nd, nd)

    def reduce_step(chunk, t):
        for sub in range(2):
            for way in range(2):
                if not used(way, t, sub):
                    continue
                term = total[chunk, :, own(target(way, t), sub), :]
                if used(way, t + 1, sub):
                    hop(chunk, way, t + 1, sub).wait_recv()
                    term = term + landed[chunk, way, t, sub].astype(F32)
                passed[chunk, way, t - 1, sub] = term.astype(BF16)
                hop(chunk, way, t, sub).start()

    def settle(chunk):
        for sub in range(2):
            for way in range(2):
                hop(chunk, way, 1, sub).wait_recv()
            at = pl.ds(sub * part, part)
            sums = (
                total[chunk, :, own(d, sub), :]
                + landed[chunk, 0, 0, sub].astype(F32)
                + landed[chunk, 1, 0, sub].astype(F32)
            )
            for side in range(2):
                where = pl.ds(place_of(chunk, side), quarter)
                out_ref[at, where] = residual[at, where].astype(F32) + sums[side]

    reduce_step(0, last)
    reduce_step(0, last - 1)

    @pl.loop(0, groups)
    def _(g):
        combine(1, g)

    for t in range(last, 0, -1):
        reduce_step(1, t)
        if t > 2:
            reduce_step(0, t - 2)
    settle(0)
    settle(1)

    for chunk in range(2):
        for way in range(2):
            for sub in range(2):
                for t in range(1, last + 1):
                    if used(way, t, sub):
                        hop(chunk, way, t, sub).wait_send()
        rings[chunk].finish()

        @pl.loop(1, ns)
        def _(j):
            go_copy(chunk, j).wait_send()
            back_copy(chunk, j).wait_send()

        @pl.loop(1, near_seats[chunk])
        def _(j):
            go_pair(chunk, j).wait_send()
            back_pair(chunk, j).wait_send()

        @pl.loop(DIRECT[chunk], groups)
        def _(g):
            swap_copy(chunk, g).wait_send()
            part_copy(chunk, g).wait_send()

    weights.finish()

    @pl.loop(1, ns)
    def _(j):
        for c in in_copies(j, toward(j), s):
            c.wait_send()

    @pl.loop(0, chips)
    def _(chip):
        @pl.when(owner(chip) != s)
        def _():
            out_copy(chip, s).wait_send()

    @pl.loop(0, nd)
    def _(index):
        sum_copy(index).wait_send()


def run_layer(docs, ids, gates, gain, score, qk, v, resid, out_weight, expert_weights, shared_weights, ns, nd):
    rows, width = v.shape
    length = rows * ns
    tokens = rows * nd
    half = width // 2
    quarter = half // 2
    slots = ns * nd * CAP
    groups = ns // GROUP
    near = max(DIRECT) * GROUP * nd * CAP
    hidden = expert_weights[0].shape[1]
    shared_hidden = shared_weights[0].shape[0]
    dma = pltpu.SemaphoreType.DMA
    vmem = pl.BlockSpec(memory_space=pltpu.VMEM)
    anyspace = pl.BlockSpec(memory_space=pl.ANY)

    def buf(*shape):
        return pltpu.VMEM(shape, BF16)

    def wide(*shape):
        return pltpu.VMEM(shape, F32)

    ring = dma((2, nd // 2, 2))
    rings = dma((2, 2, nd // 2, 2))
    per_seat = dma((2, ns))
    per_group = dma((2, groups))
    per_near = dma((2, max(DIRECT) * GROUP))
    return pl.pallas_call(
        functools.partial(layer_kernel, ns, nd),
        out_shape=jax.ShapeDtypeStruct((rows, width), F32),
        in_specs=[vmem] * 5 + [anyspace] * 10,
        out_specs=vmem,
        scratch_shapes=[buf(2, rows, width), buf(rows, width), buf(rows, width)]
        + [buf(hidden, width)] * 3
        + [buf(shared_hidden, width)] * 3
        + [wide(2, width), wide(length, HD)]
        + [wide(2 * TOPK, 2 * rows), wide(2 * TOPK, 2 * rows), wide(nd, 2 * TOPK, 2 * rows)]
        + [buf(length, HD)] * 4
        + [
            buf(rows * CORES, width // CORES),
            buf(nd, width // CORES, out_weight.shape[1]),
            wide(rows, width), wide(rows, width), wide(rows, width),
            buf(rows, width),
            buf(2, 2, rows, quarter),
            buf(2, 2, tokens, quarter),
            buf(slots, tokens), buf(slots, tokens),
            buf(2, slots, quarter), buf(2, slots, quarter), buf(2, slots, quarter),
            buf(slots, hidden),
            buf(2, slots, quarter), buf(2, slots, quarter),
            wide(slots, quarter),
            buf(2, slots, quarter), buf(2, slots, quarter),
            buf(2, near, quarter), buf(2, near, quarter),
            wide(2, 2, tokens, quarter),
            buf(2, 2, nd // 2, 2, 2, rows // 2, quarter),
            buf(2, 2, nd // 2, 2, 2, rows // 2, quarter),
            dma((10,)), dma((3,)), dma((3, ns)), dma((3, ns)), dma((ns // CORES,)),
            dma((ns // CORES,)), dma((nd,)), dma((nd,)), dma((nd,)), dma((nd,)),
            ring, ring, rings, rings,
            per_seat, per_seat, per_group, per_group, per_group, per_group, per_seat, per_seat,
            per_near, per_near, per_near, per_near, rings, rings,
        ],
        compiler_params=pltpu.CompilerParams(
            collective_id=1, has_side_effects=True, vmem_limit_bytes=67043328
        ),
        cost_estimate=pl.CostEstimate(
            flops=12 * slots * half * hidden, bytes_accessed=8 * slots * half, transcendentals=0
        ),
        name="layer",
    )(docs, ids, gates, gain, score, qk, v, resid, out_weight, *expert_weights, *shared_weights)


def body(
    resid,
    queries_keys,
    values,
    doc_ids,
    out_weight,
    norm_gain,
    expert_ids,
    gate_vals,
    expert_gate,
    expert_up,
    expert_down,
    shared_gate,
    shared_up,
    shared_down,
    shared_score,
):
    ns = lax.axis_size("seq")
    nd = lax.axis_size("dp")
    tokens = resid.shape[1]
    width = resid.shape[2]
    out = run_layer(
        doc_ids,
        expert_ids[0].T,
        gate_vals[0].T,
        norm_gain.reshape(-1, HD),
        shared_score.reshape(-1, HD),
        queries_keys.reshape(2, tokens, width),
        values[0],
        resid[0],
        out_weight,
        (expert_gate.transpose(0, 2, 1), expert_up.transpose(0, 2, 1), expert_down),
        (shared_gate.T, shared_up.T, shared_down),
        ns,
        nd,
    )
    return out.astype(BF16)[None]


def solution(mesh):
    placed = (
        P(("groups", "dp"), "seq", None),
        P(None, ("groups", "dp"), "seq", None),
        P(("groups", "dp"), "seq", None),
        P(("groups", "dp"), None),
        P(None, "dp"),
        P(),
        P(("groups", "dp"), "seq", None),
        P(("groups", "dp"), "seq", None),
        P(("seq", "dp"), None, None),
        P(("seq", "dp"), None, None),
        P(("seq", "dp"), None, None),
        P(None, "dp"),
        P(None, "dp"),
        P("dp", None),
        P(),
    )
    return jax.shard_map(
        body,
        mesh=mesh,
        in_specs=placed,
        out_specs=P(("groups", "dp"), "seq", None),
        check_vma=False,
    )
```

```python
import functools
import math

import jax
import jax.numpy as jnp
from jax import lax
from jax.experimental import pallas as pl
from jax.experimental.pallas import tpu as pltpu
from jax.sharding import PartitionSpec as P

HD = 128
TOPK = 4
SPLIT = 4
CAP = 10
GROUP = 2
CORES = 2
DIRECT = 1

norm_eps = 1e-06
MESH = pl.DeviceIdType.MESH
F32 = jnp.float32
BF16 = jnp.bfloat16


def ring_delta(j):
    return ((j + 1) // 2) * (2 * (j % 2) - 1)


class Ring:
    def __init__(self, nd, axis, source, place, send_sem, recv_sem):
        self.nd, self.axis, self.last = nd, axis, nd // 2
        self.source, self.place = source, place
        self.send_sem, self.recv_sem = send_sem, recv_sem
        self.me = lax.axis_index(axis)

    def behind(self, t, way):
        return lax.rem(self.me - (1 - 2 * way) * t + self.nd, self.nd)

    def hop(self, way, t, sub):
        index = self.behind(t - 1, way)
        src = self.source(sub) if t == 1 else self.place(index, sub)
        return pltpu.make_async_remote_copy(
            src, self.place(index, sub), self.send_sem.at[way, t - 1, sub],
            self.recv_sem.at[way, t - 1, sub],
            device_id={self.axis: self.behind(-1, way)}, device_id_type=MESH,
        )

    def hops(self, t):
        return [
            (way, t, sub)
            for sub in range(2)
            for way in range(2)
            if t < self.last or (t == self.last and sub == way)
        ]

    def start(self):
        for h in self.hops(1):
            self.hop(*h).start()

    def advance(self, t):
        following = self.hops(t + 1)
        for way, _, sub in self.hops(t):
            self.hop(way, t, sub).wait_recv()
            if (way, t + 1, sub) in following:
                self.hop(way, t + 1, sub).start()

    def arrived(self, t):
        return [self.behind(t, 0), self.behind(t, 1)] if t < self.last else [self.behind(t, 0)]

    def finish(self):
        for t in range(1, self.last + 1):
            for h in self.hops(t):
                self.hop(*h).wait_send()


def greet(axes):
    barrier = pltpu.get_barrier_semaphore()
    for axis, size in axes.items():
        me = lax.axis_index(axis)

        @pl.loop(1, size)
        def _(k):
            pl.semaphore_signal(
                barrier, inc=1, device_id={axis: lax.rem(me + k, size)}, device_id_type=MESH
            )

    pl.semaphore_wait(barrier, sum(axes.values()) - len(axes))


def layer_kernel(
    ns, nd, docs_ref, ids_ref, gates_ref, gain_ref, score_ref, qk_hbm, v_hbm, resid_hbm, w_hbm, eg_hbm, eu_hbm, ed_hbm,
    sg_hbm, su_hbm, sd_hbm, out_ref,
    qk, v, resid, wg, wu, wd, vg, vu, vd, vecs, dcol, spread, info, routes, qh, kh, vh, att, mixed, wall, own_sum,
    send_sum, got_sum, residual, normed, every, picks, mixes, send, own_in, pair_in, act, pair_out,
    pair_part, own_part, back, ret, send_pair, ret_pair, total, landed, passed,
    w_sem, local_sem, si_sem, ri_sem, so_sem, ro_sem, sd_sem, rd_sem, sp_sem, rp_sem, sw_sem, rw_sem,
    sg_sem, rg_sem, sy_sem, ry_sem, sx_sem, rx_sem, sq_sem, rq_sem, sr_sem, rr_sem, sf_sem, rf_sem, sb_sem, rb_sem,
    s2_sem, r2_sem,
):
    s = lax.axis_index("seq")
    d = lax.axis_index("dp")
    rows, width = v.shape
    length = rows * ns
    tokens = rows * nd
    core = lax.rem(s, CORES)
    chips = ns // CORES
    depth = width // CORES
    block = width // nd
    chip_rows = rows * CORES
    half = width // 2
    quarter = half // 2
    lanes = 2 * rows

    first = [
        pltpu.make_async_copy(src, dst, w_sem.at[i])
        for i, (src, dst) in enumerate(
            (
                (qk_hbm, qk), (v_hbm, v),
                (w_hbm.at[pl.ds(pl.multiple_of(core * depth, 16), depth)], wall.at[d]),
                (resid_hbm, resid),
            )
        )
    ]
    later = [
        pltpu.make_async_copy(src, dst, w_sem.at[4 + i])
        for i, (src, dst) in enumerate(
            (
                (sg_hbm, vg), (su_hbm, vu), (sd_hbm, vd),
                (eg_hbm.at[0], wg), (eu_hbm.at[0], wu), (ed_hbm.at[0], wd),
            )
        )
    ]
    for c in first:
        c.start()

    experts = ns * nd // SPLIT
    lane = lax.broadcasted_iota(jnp.int32, (1, lanes), 1)
    valid = (lane >= lax.rem(d, 2) * rows) & (lane < (lax.rem(d, 2) + 1) * rows)
    expert = lax.broadcasted_iota(jnp.int32, (experts, lanes), 0).astype(F32)
    spread[...] = jnp.zeros_like(spread)
    spread[0:TOPK, 0:rows] = ids_ref[...].astype(F32)
    spread[TOPK:, 0:rows] = gates_ref[...]
    odd = lax.rem(d, 2).astype(F32)
    both = spread[...] * (1.0 - odd) + pltpu.roll(spread[...], rows, 1) * odd
    chosen_ids = [jnp.where(valid, both[k : k + 1, :], -1.0) for k in range(TOPK)]
    named = [ids == expert for ids in chosen_ids]
    earlier = lax.broadcasted_iota(jnp.int32, (lanes, lanes), 0) < lax.broadcasted_iota(
        jnp.int32, (lanes, lanes), 1
    )
    counts = jnp.dot(
        jnp.where(functools.reduce(jnp.logical_or, named), 1.0, 0.0).astype(BF16),
        jnp.where(earlier, 1.0, 0.0).astype(BF16),
        preferred_element_type=F32,
    )
    for k in range(TOPK):
        rank = jnp.sum(jnp.where(named[k], counts, 0.0), axis=0, keepdims=True)
        info[k : k + 1, :] = jnp.where(valid, chosen_ids[k] * CAP + rank, 0.0)
    info[TOPK:, :] = both[TOPK:, :]
    score = score_ref[...].astype(F32)
    for i in range(width // HD):
        vecs[0:1, i * HD : (i + 1) * HD] = gain_ref[i : i + 1, :]
        vecs[1:2, i * HD : (i + 1) * HD] = score[i : i + 1, :]
    routes[d] = info[...]
    docs = docs_ref[...].astype(F32)
    for i in range(length // HD):
        tile = jnp.broadcast_to(docs[:, i * HD : (i + 1) * HD], (HD, HD))
        dcol[i * HD : (i + 1) * HD, :] = tile.T

    greet({"seq": ns, "dp": nd})
    first[0].wait()
    first[1].wait()

    def own_rows(ref, t):
        return ref.at[pl.ds(pl.multiple_of(t * rows, 16), rows)]

    def cols(t):
        return pl.ds(pl.multiple_of(t * HD, HD), HD)

    def info_copy(to, slot):
        return pltpu.make_async_remote_copy(
            info, routes.at[slot], sd_sem.at[to], rd_sem.at[slot],
            device_id={"dp": to}, device_id_type=MESH,
        )

    def pieces(t):
        return (
            (qk.at[0, :, cols(t)], qh),
            (qk.at[1, :, cols(t)], kh),
            (v.at[:, cols(t)], vh),
        )

    def in_copies(j, to, slot):
        return [
            pltpu.make_async_remote_copy(
                src, own_rows(dst, slot), si_sem.at[c, j], ri_sem.at[c, j],
                device_id={"seq": to}, device_id_type=MESH,
            )
            for c, (src, dst) in enumerate(pieces(to))
        ]

    def peer(j, sign):
        chip = lax.rem(s // CORES + sign * ring_delta(j // CORES) + chips, chips)
        return chip * CORES + lax.rem(core + j, CORES)

    def toward(j):
        return peer(j, -1)

    def origin(j):
        return peer(j, 1)

    @pl.loop(1, ns)
    def _(j):
        for c in in_copies(j, toward(j), s):
            c.start()

    w_part = depth // 2
    weights = Ring(
        nd, "dp",
        lambda sub: wall.at[d, pl.ds(sub * w_part, w_part)],
        lambda index, sub: wall.at[index, pl.ds(sub * w_part, w_part)],
        sw_sem, rw_sem,
    )
    first[2].wait()
    weights.start()

    @pl.loop(1, nd)
    def _(k):
        info_copy(lax.rem(d + k, nd), d).start()

    for c in later:
        c.start()
    local = [
        pltpu.make_async_copy(src, own_rows(dst, s), local_sem.at[c])
        for c, (src, dst) in enumerate(pieces(s))
    ]
    for c in local:
        c.start()
    for c in local:
        c.wait()

    def receive(j):
        frm = origin(j)
        for c in in_copies(j, frm, frm):
            c.wait_recv()

    @pl.loop(1, ns // 2)
    def _(j):
        receive(j)

    weights.advance(1)

    @pl.loop(ns // 2, ns)
    def _(j):
        receive(j)

    per_core = ns // CORES
    mate = s + 1 - 2 * core

    def owner(chip):
        return chip * CORES + s // per_core

    def out_copy(chip, head):
        return pltpu.make_async_remote_copy(
            att.at[pl.ds(pl.multiple_of(chip * chip_rows, 16), chip_rows)],
            mixed.at[:, cols(lax.rem(head, per_core))], so_sem.at[chip],
            ro_sem.at[lax.rem(head, per_core)],
            device_id={"seq": owner(chip)}, device_id_type=MESH,
        )

    scale = 1.0 / math.sqrt(HD)
    step_rows = 2 * chip_rows
    for i in range(length // step_rows):
        upto = (i + 1) * step_rows
        span = pl.ds(i * step_rows, step_rows)
        scores = lax.dot_general(
            qh[span, :], kh[0:upto, :], (((1,), (1,)), ((), ())), preferred_element_type=F32
        ) * scale
        at = lax.broadcasted_iota(jnp.int32, (step_rows, upto), 0) + i * step_rows
        key_at = lax.broadcasted_iota(jnp.int32, (step_rows, upto), 1)
        mine = jnp.concatenate([dcol[span, :]] * (upto // HD), axis=1)
        allowed = (key_at <= at) & (mine == docs[:, 0:upto])
        scores = jnp.where(allowed, scores, -1e30)
        lifted = jnp.exp(scores - jnp.max(scores, axis=-1, keepdims=True))
        probs = (lifted / jnp.sum(lifted, axis=-1, keepdims=True)).astype(BF16)
        att[span, :] = jnp.dot(probs, vh[0:upto, :], preferred_element_type=F32).astype(BF16)
        for chip in (2 * i, 2 * i + 1):

            @pl.when(owner(chip) != s)
            def _():
                out_copy(chip, s).start()

            @pl.when(owner(chip) == s)
            def _():
                mixed[:, cols(lax.rem(s, per_core))] = att[
                    pl.ds(chip * chip_rows, chip_rows), :
                ]

        if i == 1:
            weights.advance(2)

    slots = nd * CAP
    per_seq = nd // SPLIT
    first_expert = d // SPLIT

    @pl.loop(1, nd)
    def _(k):
        other = lax.rem(d + k, nd)
        info_copy(other, other).wait_send()
        info_copy(other, other).wait_recv()

    tiles = [routes[2 * m] + routes[2 * m + 1] for m in range(nd // 2)]
    code = jnp.concatenate([tile[:TOPK] for tile in tiles], axis=1)
    gates = jnp.concatenate([tile[TOPK:] for tile in tiles], axis=1)
    slot = lax.broadcasted_iota(jnp.int32, (slots, tokens), 0).astype(F32)
    token = lax.broadcasted_iota(jnp.int32, (slots, tokens), 1).astype(F32)
    slot_block = jnp.floor((slot + 0.5) * (1.0 / CAP))
    token_block = jnp.floor((token + 0.5) * (1.0 / rows))
    ranks = jnp.where(slot_block == token_block, slot - slot_block * CAP, -1e6)

    def seat(j):
        return pl.ds(pl.multiple_of(j * slots, 16), slots)

    @pl.loop(0, ns)
    def _(j):
        base = ((toward(j) * per_seq + first_expert) * CAP).astype(F32)
        hits = [code[k : k + 1, :] - base == ranks for k in range(TOPK)]
        hit = functools.reduce(jnp.logical_or, hits)
        picks[seat(j), :] = jnp.where(hit, 1.0, 0.0).astype(BF16)
        mixes[seat(j), :] = functools.reduce(
            jnp.add, [jnp.where(hits[k], gates[k : k + 1, :], 0.0) for k in range(TOPK)]
        ).astype(BF16)

    weights.advance(3)

    @pl.loop(0, per_core)
    def _(h):
        @pl.when(core * per_core + h != s)
        def _():
            out_copy(0, h).wait_recv()

    def sum_copy(index):
        at = pl.ds(pl.multiple_of(index * block, block), block)
        return pltpu.make_async_remote_copy(
            send_sum.at[:, at], got_sum.at[:, at], sp_sem.at[index], rp_sem.at[index],
            device_id={"seq": mate}, device_id_type=MESH,
        )

    def project(index):
        at = pl.ds(pl.multiple_of(index * block, block), block)
        theirs = mixed[pl.ds(pl.multiple_of((1 - core) * rows, 16), rows), :]
        mine = mixed[pl.ds(pl.multiple_of(core * rows, 16), rows), :]
        send_sum[:, at] = jnp.dot(theirs, wall[index], preferred_element_type=F32)
        own_sum[:, at] = jnp.dot(mine, wall[index], preferred_element_type=F32)
        sum_copy(index).start()

    project(d)
    for t in range(1, nd // 2 + 1):
        if t >= 4:
            weights.advance(t)
        for index in weights.arrived(t):
            project(index)

    @pl.loop(0, nd)
    def _(index):
        sum_copy(index).wait_recv()

    first[3].wait()
    projected = (own_sum[...] + got_sum[...]).astype(BF16)
    summed = (resid[...].astype(F32) + projected.astype(F32)).astype(BF16)
    residual[...] = summed
    stream = summed.astype(F32)
    scaled = (
        stream
        * lax.rsqrt(jnp.mean(stream * stream, axis=-1, keepdims=True) + norm_eps)
        * vecs[0:1, :]
    ).astype(BF16)

    def place_of(chunk, side):
        return side * half + chunk * quarter

    mine_at = pl.ds(pl.multiple_of(d * rows, 16), rows)
    for chunk in range(2):
        for side in range(2):
            at = place_of(chunk, side)
            normed[chunk, side] = scaled[:, at : at + quarter]
            every[chunk, side, mine_at, :] = scaled[:, at : at + quarter]
    part = rows // 2

    def gather(chunk):
        return Ring(
            nd, "dp",
            lambda sub: normed.at[chunk, :, pl.ds(sub * part, part)],
            lambda index, sub: every.at[
                chunk, :, pl.ds(pl.multiple_of(index * rows + sub * part, 16), part)
            ],
            sg_sem.at[chunk], rg_sem.at[chunk],
        )

    rings = [gather(0), gather(1)]

    par = lax.rem(d, 2)
    partner = d + 1 - 2 * par
    group_slots = GROUP * slots
    groups = ns // GROUP

    def span_of(g):
        return pl.ds(pl.multiple_of(g * group_slots, 16), group_slots)

    def go_copy(chunk, j):
        return pltpu.make_async_remote_copy(
            send.at[chunk, seat(j)], own_in.at[chunk, seat(j)], sy_sem.at[chunk, j],
            ry_sem.at[chunk, j], device_id={"seq": toward(j)}, device_id_type=MESH,
        )

    def swap_copy(chunk, g):
        return pltpu.make_async_remote_copy(
            own_in.at[chunk, span_of(g)], pair_in.at[chunk, span_of(g)], sx_sem.at[chunk, g],
            rx_sem.at[chunk, g], device_id={"dp": partner}, device_id_type=MESH,
        )

    def part_copy(chunk, g):
        return pltpu.make_async_remote_copy(
            pair_out.at[chunk, span_of(g)], pair_part.at[chunk, span_of(g)], sq_sem.at[chunk, g],
            rq_sem.at[chunk, g], device_id={"dp": partner}, device_id_type=MESH,
        )

    def back_copy(chunk, j):
        return pltpu.make_async_remote_copy(
            back.at[chunk, seat(j)], ret.at[chunk, seat(j)], sr_sem.at[chunk, j],
            rr_sem.at[chunk, j], device_id={"seq": origin(j)}, device_id_type=MESH,
        )

    def go_pair(chunk, j):
        return pltpu.make_async_remote_copy(
            send_pair.at[chunk, seat(j)], pair_in.at[chunk, seat(j)], sf_sem.at[chunk, j],
            rf_sem.at[chunk, j], device_id={"seq": toward(j)}, device_id_type=MESH,
        )

    def back_pair(chunk, j):
        return pltpu.make_async_remote_copy(
            pair_out.at[chunk, seat(j)], ret_pair.at[chunk, seat(j)], sb_sem.at[chunk, j],
            rb_sem.at[chunk, j], device_id={"seq": origin(j)}, device_id_type=MESH,
        )

    near_seats = DIRECT * GROUP

    def columns(chunk, side):
        return pl.ds(pl.multiple_of(side * half + chunk * quarter, quarter), quarter)

    batch = ns // 4

    def pick(chunk, q):
        at = pl.ds(q * batch * slots, batch * slots)
        got = jnp.dot(
            picks[at, :], every[chunk, par], preferred_element_type=F32
        ).astype(BF16)
        send[chunk, at, :] = got
        if q == 0:
            own_in[chunk, 0:slots, :] = got[0:slots]
            near = pl.ds(0, near_seats * slots)
            got = jnp.dot(
                picks[near, :], every[chunk, 1 - par], preferred_element_type=F32
            ).astype(BF16)
            send_pair[chunk, near, :] = got
            pair_in[chunk, 0:slots, :] = got[0:slots]

    def go(chunk, q):
        @pl.loop(max(1, q * batch), (q + 1) * batch)
        def _(j):
            go_copy(chunk, j).start()

        if q == 0:

            @pl.loop(1, near_seats)
            def _(j):
                go_pair(chunk, j).start()

    for ring in rings:
        ring.start()
    for t in range(1, nd // 2):
        for ring in rings:
            ring.advance(t)
    for chunk in range(2):
        rings[chunk].advance(nd // 2)
        for q in range(4):
            pick(chunk, q)
            if q:
                go(chunk, q - 1)
        go(chunk, 3)
    for c in later:
        c.wait()

    def nt(a, w):
        return lax.dot_general(a, w, (((1,), (1,)), ((), ())), preferred_element_type=F32)

    def silu(a):
        return a / (1.0 + jnp.exp(-a))

    def arrive(chunk, g):
        for i in range(GROUP):
            j = g * GROUP + i

            @pl.when(j > 0)
            def _():
                go_copy(chunk, j).wait_recv()

            @pl.when((j > 0) & (g < DIRECT))
            def _():
                go_pair(chunk, j).wait_recv()

        @pl.when(g >= DIRECT)
        def _():
            swap_copy(chunk, g).start()

    quads = [(chunk, side) for chunk in range(2) for side in range(2)]
    share = tokens // 4

    @pl.loop(0, groups)
    def _(g):
        arrive(0, g)

        @pl.when((g >= 1) & (g <= 4))
        def _():
            at = pl.ds(pl.multiple_of((g - 1) * share, share), share)
            gate_act = jnp.zeros((share, vg.shape[0]), F32)
            up_act = jnp.zeros((share, vg.shape[0]), F32)
            weight = jnp.zeros((share, 1), F32)
            for chunk, side in quads:
                a = every[chunk, side, at, :]
                where = pl.ds(place_of(chunk, side), quarter)
                gate_act += nt(a, vg[:, where])
                up_act += nt(a, vu[:, where])
                weight += jnp.sum(
                    a.astype(F32) * vecs[1:2, where], axis=-1, keepdims=True
                )
            hidden = (silu(gate_act) * up_act).astype(BF16)
            weight = 1.0 / (1.0 + jnp.exp(-weight))
            for chunk, side in quads:
                total[chunk, side, at, :] = weight * jnp.dot(
                    hidden, vd[:, pl.ds(place_of(chunk, side), quarter)],
                    preferred_element_type=F32,
                )

    def down(chunk, g):
        hidden = act[span_of(g), :]
        pair_out[chunk, span_of(g), :] = jnp.dot(
            hidden, wd[:, columns(chunk, 1 - par)], preferred_element_type=F32
        ).astype(BF16)
        own_part[span_of(g), :] = jnp.dot(
            hidden, wd[:, columns(chunk, par)], preferred_element_type=F32
        )

        @pl.when(g >= DIRECT)
        def _():
            part_copy(chunk, g).start()

    def join(chunk, g):
        @pl.when(g >= DIRECT)
        def _():
            part_copy(chunk, g).wait_recv()
            back[chunk, span_of(g), :] = (
                own_part[span_of(g), :] + pair_part[chunk, span_of(g), :].astype(F32)
            ).astype(BF16)

        @pl.when(g < DIRECT)
        def _():
            back[chunk, span_of(g), :] = own_part[span_of(g), :].astype(BF16)

    def leave(chunk, g):
        for i in range(GROUP):
            j = g * GROUP + i

            @pl.when(j > 0)
            def _():
                back_copy(chunk, j).start()

            @pl.when((j > 0) & (g < DIRECT))
            def _():
                back_pair(chunk, j).start()

            @pl.when(j == 0)
            def _():
                ret[chunk, 0:slots, :] = back[chunk, 0:slots, :]
                ret_pair[chunk, 0:slots, :] = pair_out[chunk, 0:slots, :]

    def combine(chunk, g):
        for i in range(GROUP):
            j = g * GROUP + i

            @pl.when(j > 0)
            def _():
                back_copy(chunk, j).wait_recv()

            @pl.when((j > 0) & (g < DIRECT))
            def _():
                back_pair(chunk, j).wait_recv()

        def mix(rows_in):
            return lax.dot_general(
                mixes[span_of(g), :], rows_in[chunk, span_of(g), :], (((0,), (0,)), ((), ())),
                preferred_element_type=F32,
            )

        total[chunk, par] += mix(ret)

        @pl.when(g < DIRECT)
        def _():
            total[chunk, 1 - par] += mix(ret_pair)

    @pl.loop(0, groups + 2)
    def _(step):
        @pl.when(step < groups)
        def _():
            arrive(1, step)

        @pl.when(step >= 2)
        def _():
            join(0, step - 2)

        @pl.when((step >= 1) & (step <= groups))
        def _():
            g = step - 1
            gate_act = jnp.zeros((group_slots, wg.shape[0]), F32)
            up_act = jnp.zeros((group_slots, wg.shape[0]), F32)
            for chunk in range(2):
                @pl.when(g >= DIRECT)
                def _():
                    swap_copy(chunk, g).wait_recv()

                for rows_in, side in ((own_in, par), (pair_in, 1 - par)):
                    a = rows_in[chunk, span_of(g), :]
                    gate_act += nt(a, wg[:, columns(chunk, side)])
                    up_act += nt(a, wu[:, columns(chunk, side)])
            act[span_of(g), :] = (silu(gate_act) * up_act).astype(BF16)
            down(0, g)

        @pl.when(step >= 2)
        def _():
            leave(0, step - 2)

    @pl.loop(0, groups)
    def _(g):
        down(1, groups - 1 - g)

    @pl.loop(0, groups)
    def _(g):
        join(1, groups - 1 - g)
        leave(1, groups - 1 - g)
        combine(0, g)

    last = nd // 2

    def own(index, sub):
        return pl.ds(pl.multiple_of(index * rows + sub * part, 16), part)

    def used(way, t, sub):
        return t < last or (t == last and sub == way)

    def hop(chunk, way, t, sub):
        sign = 1 - 2 * way
        return pltpu.make_async_remote_copy(
            passed.at[chunk, way, t - 1, sub], landed.at[chunk, way, t - 1, sub],
            s2_sem.at[chunk, way, t - 1, sub], r2_sem.at[chunk, way, t - 1, sub],
            device_id={"dp": lax.rem(d + sign + nd, nd)}, device_id_type=MESH,
        )

    def target(way, t):
        return lax.rem(d + (1 - 2 * way) * t + nd, nd)

    def reduce_step(chunk, t):
        for sub in range(2):
            for way in range(2):
                if not used(way, t, sub):
                    continue
                term = total[chunk, :, own(target(way, t), sub), :]
                if used(way, t + 1, sub):
                    hop(chunk, way, t + 1, sub).wait_recv()
                    term = term + landed[chunk, way, t, sub].astype(F32)
                passed[chunk, way, t - 1, sub] = term.astype(BF16)
                hop(chunk, way, t, sub).start()

    def settle(chunk):
        for sub in range(2):
            for way in range(2):
                hop(chunk, way, 1, sub).wait_recv()
            at = pl.ds(sub * part, part)
            sums = (
                total[chunk, :, own(d, sub), :]
                + landed[chunk, 0, 0, sub].astype(F32)
                + landed[chunk, 1, 0, sub].astype(F32)
            )
            for side in range(2):
                where = pl.ds(place_of(chunk, side), quarter)
                out_ref[at, where] = residual[at, where].astype(F32) + sums[side]

    for t in range(last, 0, -1):
        reduce_step(0, t)

        @pl.loop((last - t) * groups // last, (last - t + 1) * groups // last)
        def _(g):
            combine(1, groups - 1 - g)

    for t in range(last, 0, -1):
        reduce_step(1, t)
    settle(0)
    settle(1)

    for chunk in range(2):
        for way in range(2):
            for sub in range(2):
                for t in range(1, last + 1):
                    if used(way, t, sub):
                        hop(chunk, way, t, sub).wait_send()
        rings[chunk].finish()

        @pl.loop(1, ns)
        def _(j):
            go_copy(chunk, j).wait_send()
            back_copy(chunk, j).wait_send()

        @pl.loop(1, near_seats)
        def _(j):
            go_pair(chunk, j).wait_send()
            back_pair(chunk, j).wait_send()

        @pl.loop(DIRECT, groups)
        def _(g):
            swap_copy(chunk, g).wait_send()
            part_copy(chunk, g).wait_send()

    weights.finish()

    @pl.loop(1, ns)
    def _(j):
        for c in in_copies(j, toward(j), s):
            c.wait_send()

    @pl.loop(0, chips)
    def _(chip):
        @pl.when(owner(chip) != s)
        def _():
            out_copy(chip, s).wait_send()

    @pl.loop(0, nd)
    def _(index):
        sum_copy(index).wait_send()


def run_layer(docs, ids, gates, gain, score, qk, v, resid, out_weight, expert_weights, shared_weights, ns, nd):
    rows, width = v.shape
    length = rows * ns
    tokens = rows * nd
    half = width // 2
    quarter = half // 2
    slots = ns * nd * CAP
    groups = ns // GROUP
    near = DIRECT * GROUP * nd * CAP
    hidden = expert_weights[0].shape[1]
    shared_hidden = shared_weights[0].shape[0]
    dma = pltpu.SemaphoreType.DMA
    vmem = pl.BlockSpec(memory_space=pltpu.VMEM)
    anyspace = pl.BlockSpec(memory_space=pl.ANY)

    def buf(*shape):
        return pltpu.VMEM(shape, BF16)

    def wide(*shape):
        return pltpu.VMEM(shape, F32)

    ring = dma((2, nd // 2, 2))
    rings = dma((2, 2, nd // 2, 2))
    per_seat = dma((2, ns))
    per_group = dma((2, groups))
    per_near = dma((2, DIRECT * GROUP))
    return pl.pallas_call(
        functools.partial(layer_kernel, ns, nd),
        out_shape=jax.ShapeDtypeStruct((rows, width), F32),
        in_specs=[vmem] * 5 + [anyspace] * 10,
        out_specs=vmem,
        scratch_shapes=[buf(2, rows, width), buf(rows, width), buf(rows, width)]
        + [buf(hidden, width)] * 3
        + [buf(shared_hidden, width)] * 3
        + [wide(2, width), wide(length, HD)]
        + [wide(2 * TOPK, 2 * rows), wide(2 * TOPK, 2 * rows), wide(nd, 2 * TOPK, 2 * rows)]
        + [buf(length, HD)] * 4
        + [
            buf(rows * CORES, width // CORES),
            buf(nd, width // CORES, out_weight.shape[1]),
            wide(rows, width), wide(rows, width), wide(rows, width),
            buf(rows, width),
            buf(2, 2, rows, quarter),
            buf(2, 2, tokens, quarter),
            buf(slots, tokens), buf(slots, tokens),
            buf(2, slots, quarter), buf(2, slots, quarter), buf(2, slots, quarter),
            buf(slots, hidden),
            buf(2, slots, quarter), buf(2, slots, quarter),
            wide(slots, quarter),
            buf(2, slots, quarter), buf(2, slots, quarter),
            buf(2, near, quarter), buf(2, near, quarter),
            wide(2, 2, tokens, quarter),
            buf(2, 2, nd // 2, 2, 2, rows // 2, quarter),
            buf(2, 2, nd // 2, 2, 2, rows // 2, quarter),
            dma((10,)), dma((3,)), dma((3, ns)), dma((3, ns)), dma((ns // CORES,)),
            dma((ns // CORES,)), dma((nd,)), dma((nd,)), dma((nd,)), dma((nd,)),
            ring, ring, rings, rings,
            per_seat, per_seat, per_group, per_group, per_group, per_group, per_seat, per_seat,
            per_near, per_near, per_near, per_near, rings, rings,
        ],
        compiler_params=pltpu.CompilerParams(
            collective_id=1, has_side_effects=True, vmem_limit_bytes=67043328
        ),
        cost_estimate=pl.CostEstimate(
            flops=12 * slots * half * hidden, bytes_accessed=8 * slots * half, transcendentals=0
        ),
        name="layer",
    )(docs, ids, gates, gain, score, qk, v, resid, out_weight, *expert_weights, *shared_weights)


def body(
    resid,
    queries_keys,
    values,
    doc_ids,
    out_weight,
    norm_gain,
    expert_ids,
    gate_vals,
    expert_gate,
    expert_up,
    expert_down,
    shared_gate,
    shared_up,
    shared_down,
    shared_score,
):
    ns = lax.axis_size("seq")
    nd = lax.axis_size("dp")
    tokens = resid.shape[1]
    width = resid.shape[2]
    out = run_layer(
        doc_ids,
        expert_ids[0].T,
        gate_vals[0].T,
        norm_gain.reshape(-1, HD),
        shared_score.reshape(-1, HD),
        queries_keys.reshape(2, tokens, width),
        values[0],
        resid[0],
        out_weight,
        (expert_gate.transpose(0, 2, 1), expert_up.transpose(0, 2, 1), expert_down),
        (shared_gate.T, shared_up.T, shared_down),
        ns,
        nd,
    )
    return out.astype(BF16)[None]


def solution(mesh):
    placed = (
        P(("groups", "dp"), "seq", None),
        P(None, ("groups", "dp"), "seq", None),
        P(("groups", "dp"), "seq", None),
        P(("groups", "dp"), None),
        P(None, "dp"),
        P(),
        P(("groups", "dp"), "seq", None),
        P(("groups", "dp"), "seq", None),
        P(("seq", "dp"), None, None),
        P(("seq", "dp"), None, None),
        P(("seq", "dp"), None, None),
        P(None, "dp"),
        P(None, "dp"),
        P("dp", None),
        P(),
    )
    return jax.shard_map(
        body,
        mesh=mesh,
        in_specs=placed,
        out_specs=P(("groups", "dp"), "seq", None),
        check_vma=False,
    )
```
